256 devices in a mesh: group: 2 (over y_hi), gx: 8 (over z), gy: 16 (over x, y_lo, core).
Axes of the slice: x: 4, y: 4 (y_hi: 2, y_lo: 2; y = y_hi * 2 + y_lo), z: 8, core: 2. Of those that a mesh axis runs over, the one named last changes fastest.
Arguments:
- displacement: float32 [2, 3, 64, 256, 128], P('group', None, 'gx', 'gy'), may hold values from -6 to 6
- velocity: float32 [2, 3, 64, 256, 128], P('group', None, 'gx', 'gy'), may hold values from -6 to 6
- modulus: float32 [2, 64, 256, 128], P('group', 'gx', 'gy'), may hold values from 1 to 4
- bond_words: int32 [2, 64, 256, 128], P(None, 'gx', 'gy'), may hold values from 0 to 2147483647, as said below
- coupling_map: int32 [3, 64, 256], P(None, 'gx', 'gy'), may hold values from 0 to 2
Outputs:
- new_displacement: float32 [2, 3, 64, 256, 128], P('group', None, 'gx', 'gy')
- new_velocity: float32 [2, 3, 64, 256, 128], P('group', None, 'gx', 'gy')
The draws below stay inside these ranges and needn't reach their ends.
Inputs may be any that keep to these rules, and one draw needn't show every extreme that they name: `bond_words`: bonds to positions outside the zone are 0; bit 30 of word 1 is 0.
All inputs are finite; a program needn't handle non-finite values.
Results may differ from the reference program's by a relative error of at most 0.0001.
Values sent between devices are 32-bit elements; how exact they have to be, the bound alone decides.
A program may use at most 64 MiB of HBM per device.

```python
import math
import jax
import jax.numpy as jnp
import numpy as np
from jax import lax

NZ = 128
OV = 3
STEPS = 1
NX = 64
NY = 256


def half_offsets_drawn():
    table = []
    for delta_x in range(-3, 4):
        for delta_y in range(-3, 4):
            for delta_z in range(-3, 4):
                radius = delta_x * delta_x + delta_y * delta_y + delta_z * delta_z
                if 0 < radius <= 9 and (delta_x, delta_y, delta_z) > (0, 0, 0):
                    table.append((delta_x, delta_y, delta_z))
    return table


def draw_bond_words(key, part):
    grid_x = jnp.arange(NX)[:, None, None]
    grid_y = jnp.arange(NY)[None, :, None]
    grid_z = jnp.arange(NZ)[None, None, :]
    packed = [jnp.zeros((NX, NY, NZ), jnp.int32), jnp.zeros((NX, NY, NZ), jnp.int32)]
    for number, offset in enumerate(half_offsets_drawn()):
        delta_x, delta_y, delta_z = offset
        intact = jax.random.randint(jax.random.fold_in(key, number), (NX, NY, NZ), 0, 4) > 0
        inside = (grid_x + delta_x >= 0) & (grid_x + delta_x < NX) & (grid_y + delta_y >= 0) & (grid_y + delta_y < NY) & (grid_z + delta_z >= 0) & (grid_z + delta_z < NZ)
        crack = (grid_x < NX // 2) & (grid_x + delta_x >= NX // 2) & (grid_y < NY // 2)
        flagged = (intact & inside & ~crack).astype(jnp.int32)
        packed[number // 31] = packed[number // 31] + flagged * (1 << number % 31)
    return jnp.stack(packed)


def touch_ends(values, stream_key, least, largest):
    place = [jax.random.randint(jax.random.fold_in(stream_key, axis), (), 0, length) for axis, length in enumerate(values.shape)]
    widest = values.shape.index(max(values.shape))
    beside = place[:widest] + [(place[widest] + 1) % values.shape[widest]] + place[widest + 1:]
    return values.at[tuple(place)].set(least).at[tuple(beside)].set(largest)


def steps_of(rng, extent, split, low, top_value):
    def one(position, blocks):
        draws = jax.random.uniform(jax.random.fold_in(jax.random.fold_in(rng, 6), position), (blocks,), jnp.float32, low / len(split), top_value / len(split))
        return jnp.repeat(jnp.exp(draws), extent[position] // blocks).reshape((-1,) + (1,) * (len(extent) - position - 1))

    loudness = one(*split[0])
    for cut in split[1:]:
        loudness = loudness * one(*cut)
    return loudness


def noise(key, dims, scale, most, cuts=(), kind=jnp.bfloat16):
    values = scale * jax.random.normal(key, dims, jnp.float32)
    if cuts:
        values = values * steps_of(key, dims, cuts, -0.22, 0.18)
    return jnp.clip(values, -most, most).astype(kind)


def setup_inputs(seed: int = 0) -> dict:
    seeds = jax.random.split(jax.random.key(seed), 6)
    return {
        "displacement": noise(seeds[0], (2, 3, NX, NY, NZ), 1.0, 6.0, ((0, 2), (2, 8), (3, 16)), jnp.float32),
        "velocity": noise(seeds[1], (2, 3, NX, NY, NZ), 1.0, 6.0, ((0, 2), (2, 8), (3, 16)), jnp.float32),
        "modulus": jnp.clip(jnp.exp(math.log(4.0) - 1.3862944 * jax.random.uniform(seeds[2], (2, NX, NY, NZ), jnp.float32) ** steps_of(seeds[2], (2, NX, NY, NZ), ((0, 2), (1, 8), (2, 16)), -0.2, 0.2)), 1.0, 4.0),
        "bond_words": draw_bond_words(jax.random.fold_in(seeds[5], 71), 0),
        "coupling_map": touch_ends(jax.random.randint(seeds[4], (OV, NX, NY), 0, OV), jax.random.fold_in(seeds[4], 1), 0, OV - 1).astype(jnp.int32),
    }


time_step = 0.1
bond_scale = 1.0

def half_offsets():
    table = []
    for delta_x in range(-3, 4):
        for delta_y in range(-3, 4):
            for delta_z in range(-3, 4):
                radius = delta_x * delta_x + delta_y * delta_y + delta_z * delta_z
                if 0 < radius <= 9 and (delta_x, delta_y, delta_z) > (0, 0, 0):
                    table.append((delta_x, delta_y, delta_z))
    return table

def hex_stiffness():
    poisson = 0.3
    lame_first = poisson / ((1.0 + poisson) * (1.0 - 2.0 * poisson))
    shear_modulus = 0.5 / (1.0 + poisson)
    elastic = np.zeros((6, 6))
    elastic[:3, :3] = lame_first
    for axis_id in range(3):
        elastic[axis_id, axis_id] += 2.0 * shear_modulus
        elastic[3 + axis_id, 3 + axis_id] = shear_modulus
    points = [0.5 - 0.5 / math.sqrt(3.0), 0.5 + 0.5 / math.sqrt(3.0)]
    result = np.zeros((24, 24))
    shear_pairs = ((0, 1), (1, 2), (0, 2))
    for along_x in points:
        for along_y in points:
            for along_z in points:
                coords = (along_x, along_y, along_z)
                gradients = np.zeros((3, 8))
                for corner in range(8):
                    corner_bits = (corner >> 2 & 1, corner >> 1 & 1, corner & 1)
                    factors = [coords[axis_id] if corner_bits[axis_id] else 1.0 - coords[axis_id] for axis_id in range(3)]
                    slopes = [1.0 if corner_bits[axis_id] else -1.0 for axis_id in range(3)]
                    gradients[0, corner] = slopes[0] * factors[1] * factors[2]
                    gradients[1, corner] = factors[0] * slopes[1] * factors[2]
                    gradients[2, corner] = factors[0] * factors[1] * slopes[2]
                strain = np.zeros((6, 24))
                for axis_id in range(3):
                    strain[axis_id, axis_id * 8:axis_id * 8 + 8] = gradients[axis_id]
                for shear_row, pair in enumerate(shear_pairs):
                    left_axis, right_axis = pair
                    strain[3 + shear_row, left_axis * 8:left_axis * 8 + 8] = gradients[right_axis]
                    strain[3 + shear_row, right_axis * 8:right_axis * 8 + 8] = gradients[left_axis]
                result += strain.T @ elastic @ strain / 8.0
    return result

def bond_sum(field_pad, words_pad, modulus_pad, size_x, size_y, size_z):

    def window(array, delta_x, delta_y, delta_z):
        return array[..., 3 + delta_x:3 + delta_x + size_x, 3 + delta_y:3 + delta_y + size_y, 3 + delta_z:3 + delta_z + size_z]
    centre = window(field_pad, 0, 0, 0)
    centre_modulus = window(modulus_pad, 0, 0, 0)
    centre_words = window(words_pad, 0, 0, 0)
    summed = jnp.zeros_like(centre)
    for number, offset in enumerate(half_offsets()):
        delta_x, delta_y, delta_z = offset
        word_id = number // 31
        bit_id = number % 31
        factor = 0.5 * bond_scale / float(delta_x * delta_x + delta_y * delta_y + delta_z * delta_z) ** 1.5
        ahead_diff = window(field_pad, delta_x, delta_y, delta_z) - centre
        behind_diff = window(field_pad, -delta_x, -delta_y, -delta_z) - centre
        ahead_proj = delta_x * ahead_diff[0] + delta_y * ahead_diff[1] + delta_z * ahead_diff[2]
        behind_proj = delta_x * behind_diff[0] + delta_y * behind_diff[1] + delta_z * behind_diff[2]
        ahead_flag = (centre_words[word_id] >> bit_id & 1).astype(jnp.float32)
        behind_flag = (window(words_pad[word_id], -delta_x, -delta_y, -delta_z) >> bit_id & 1).astype(jnp.float32)
        strength = ahead_flag * (centre_modulus + window(modulus_pad, delta_x, delta_y, delta_z)) * ahead_proj
        strength = strength + behind_flag * (centre_modulus + window(modulus_pad, -delta_x, -delta_y, -delta_z)) * behind_proj
        strength = factor * strength
        summed = summed + jnp.stack([delta_x * strength, delta_y * strength, delta_z * strength])
    return summed

def couple(below_top, map_layers):
    coupled = jnp.zeros_like(below_top)
    for layer_id in range(below_top.shape[3]):
        coupled = coupled + jnp.where(map_layers[None] == layer_id, below_top[..., layer_id:layer_id + 1], 0.0)
    return coupled

def spread(reaction, map_layers):
    columns = []
    for layer_id in range(reaction.shape[3]):
        columns.append(lax.optimization_barrier(jnp.sum(jnp.where(map_layers[None] == layer_id, reaction, 0.0), axis=3)))
    return jnp.stack(columns, axis=3)

def slab_forces(field_now, modulus_slab):
    size_x, size_y, size_z = (field_now.shape[1], field_now.shape[2], field_now.shape[3])
    stiffness = jnp.asarray(hex_stiffness(), dtype=jnp.float32)
    field_pad = jnp.pad(field_now, ((0, 0), (0, 1), (0, 1), (0, 1)))
    pieces = []
    for component in range(3):
        for corner in range(8):
            corner_x, corner_y, corner_z = (corner >> 2 & 1, corner >> 1 & 1, corner & 1)
            pieces.append(field_pad[component, corner_x:corner_x + size_x, corner_y:corner_y + size_y, corner_z:corner_z + size_z])
    gathered = jnp.stack(pieces).reshape(24, -1)
    inside = ((jnp.arange(size_x) < size_x - 1)[:, None, None] & (jnp.arange(size_y) < size_y - 1)[None, :, None] & (jnp.arange(size_z) < size_z - 1)[None, None, :]).astype(jnp.float32)
    result = jnp.dot(stiffness, gathered, precision=lax.Precision.HIGHEST, preferred_element_type=jnp.float32)
    result = result.reshape(24, size_x, size_y, size_z) * (modulus_slab * inside)[None]
    result_pad = jnp.pad(result, ((0, 0), (1, 0), (1, 0), (1, 0)))
    forces = []
    for component in range(3):
        summed = jnp.zeros((size_x, size_y, size_z), jnp.float32)
        for corner in range(8):
            corner_x, corner_y, corner_z = (corner >> 2 & 1, corner >> 1 & 1, corner & 1)
            summed = summed - result_pad[component * 8 + corner, 1 - corner_x:1 - corner_x + size_x, 1 - corner_y:1 - corner_y + size_y, 1 - corner_z:1 - corner_z + size_z]
        forces.append(summed)
    return jnp.stack(forces)

def reference(displacement, velocity, modulus, bond_words, coupling_map):
    zone_field, slab_field = (displacement[0], displacement[1])
    zone_speed, slab_speed = (velocity[0], velocity[1])
    map_layers = jnp.transpose(coupling_map, (1, 2, 0))
    layer_ids = jnp.arange(NZ)
    moving = (layer_ids >= OV)[None, None, None, :]
    unclamped = (layer_ids > 0)[None, None, None, :]
    count_x = (jnp.arange(NX) > 0).astype(jnp.float32) + (jnp.arange(NX) < NX - 1).astype(jnp.float32)
    count_y = (jnp.arange(NY) > 0).astype(jnp.float32) + (jnp.arange(NY) < NY - 1).astype(jnp.float32)
    count_z = (layer_ids > 0).astype(jnp.float32) + (layer_ids < NZ - 1).astype(jnp.float32)
    lumped_mass = count_x[:, None, None] * count_y[None, :, None] * count_z[None, None, :] / 8.0
    words_pad = jnp.pad(bond_words, ((0, 0), (3, 3), (3, 3), (3, 3)))
    modulus_pad = jnp.pad(modulus[0], ((3, 3), (3, 3), (3, 3)))
    for step_count in range(STEPS):
        coupled = couple(slab_field[..., NZ - OV:], map_layers)
        zone_field = jnp.concatenate([coupled, zone_field[..., OV:]], axis=3)
        field_pad = jnp.pad(zone_field, ((0, 0), (3, 3), (3, 3), (3, 3)))
        zone_force = bond_sum(field_pad, words_pad, modulus_pad, NX, NY, NZ)
        interface = jnp.pad(spread(zone_force[..., :OV], map_layers), ((0, 0), (0, 0), (0, 0), (NZ - OV, 0)))
        slab_force = slab_forces(slab_field, modulus[1]) + interface
        zone_speed = jnp.where(moving, zone_speed + time_step * zone_force, zone_speed)
        zone_field = jnp.where(moving, zone_field + time_step * zone_speed, zone_field)
        slab_speed = jnp.where(unclamped, slab_speed + time_step * slab_force / lumped_mass, 0.0)
        slab_field = jnp.where(unclamped, slab_field + time_step * slab_speed, 0.0)
    return (jnp.stack([zone_field, slab_field]), jnp.stack([zone_speed, slab_speed]))
```

```python
import math

import jax
import jax.numpy as jnp
import numpy as np
from jax import lax
from jax.experimental import pallas as pl
from jax.experimental.pallas import tpu as pltpu
from jax.sharding import PartitionSpec as P

time_step = 0.1
bond_scale = 1.0
rim = 3
low = 8
MESH = pl.DeviceIdType.MESH
directions = [(1, 0), (-1, 0), (0, 1), (0, -1), (1, 1), (1, -1), (-1, 1), (-1, -1)]
shifts = [1, -1, 2, -2]


def half_offsets():
    table = []
    for delta_x in range(-3, 4):
        for delta_y in range(-3, 4):
            for delta_z in range(-3, 4):
                radius = delta_x * delta_x + delta_y * delta_y + delta_z * delta_z
                if 0 < radius <= 9 and (delta_x, delta_y, delta_z) > (0, 0, 0):
                    table.append((delta_x, delta_y, delta_z))
    return table


def hex_stiffness():
    poisson = 0.3
    lame_first = poisson / ((1.0 + poisson) * (1.0 - 2.0 * poisson))
    shear_modulus = 0.5 / (1.0 + poisson)
    elastic = np.zeros((6, 6))
    elastic[:3, :3] = lame_first
    for axis_id in range(3):
        elastic[axis_id, axis_id] += 2.0 * shear_modulus
        elastic[3 + axis_id, 3 + axis_id] = shear_modulus
    points = [0.5 - 0.5 / math.sqrt(3.0), 0.5 + 0.5 / math.sqrt(3.0)]
    result = np.zeros((24, 24))
    shear_pairs = ((0, 1), (1, 2), (0, 2))
    for along_x in points:
        for along_y in points:
            for along_z in points:
                coords = (along_x, along_y, along_z)
                gradients = np.zeros((3, 8))
                for corner in range(8):
                    corner_bits = (corner >> 2 & 1, corner >> 1 & 1, corner & 1)
                    factors = [
                        coords[axis_id] if corner_bits[axis_id] else 1.0 - coords[axis_id]
                        for axis_id in range(3)
                    ]
                    slopes = [1.0 if corner_bits[axis_id] else -1.0 for axis_id in range(3)]
                    gradients[0, corner] = slopes[0] * factors[1] * factors[2]
                    gradients[1, corner] = factors[0] * slopes[1] * factors[2]
                    gradients[2, corner] = factors[0] * factors[1] * slopes[2]
                strain = np.zeros((6, 24))
                for axis_id in range(3):
                    strain[axis_id, axis_id * 8 : axis_id * 8 + 8] = gradients[axis_id]
                for shear_row, pair in enumerate(shear_pairs):
                    left_axis, right_axis = pair
                    strain[3 + shear_row, left_axis * 8 : left_axis * 8 + 8] = gradients[right_axis]
                    strain[3 + shear_row, right_axis * 8 : right_axis * 8 + 8] = gradients[
                        left_axis
                    ]
                result += strain.T @ elastic @ strain / 8.0
    return result


def modal_stiffness():
    one = np.array([[1.0, -1.0], [1.0, 1.0]])
    corners = np.kron(np.kron(one, one), one)
    basis = np.kron(np.eye(3), corners)
    modal = basis.T @ hex_stiffness() @ basis / 64.0
    modal[np.abs(modal) < 1e-12] = 0.0
    return modal


offsets = half_offsets()
numbers = {offset: number for number, offset in enumerate(offsets)}


def scaled(coefficient, value):
    return value if coefficient == 1 else coefficient * value


def combine(terms):
    total = None
    negative = None
    for coefficient, value in terms:
        if coefficient == 0:
            continue
        if coefficient < 0 and total is None:
            negative = scaled(-coefficient, value) if negative is None else (
                negative + scaled(-coefficient, value)
            )
        elif total is None:
            total = scaled(coefficient, value)
            if negative is not None:
                total = total - negative
                negative = None
        elif coefficient > 0:
            total = total + scaled(coefficient, value)
        else:
            total = total - scaled(-coefficient, value)
    if negative is not None:
        total = -negative
    return total


def turn(value, by):
    return pltpu.roll(value, (-by) % 128, value.ndim - 1)


def kernel(
    disp, vel, mod, words, cmap,
    out_u, out_v,
    B, W, V, CM,
    YS, YSW, YR, YRW, CS, CSW, CR, CRW,
    PS, PX, PY, RS, RR,
    R, R3, WR, WR3, SL, SH,
    load_sem, fs, fr, ws, wr, ps, pr, link_s, link_r,
):
    group = lax.axis_index("group")
    gx = lax.axis_index("gx")
    gy = lax.axis_index("gy")
    size_x = lax.axis_size("gx")
    size_y = lax.axis_size("gy")
    is_zone = group == 0
    is_slab = group == 1
    rows_x, rows_y, depth = V.shape[1], V.shape[2], V.shape[3]
    own_x = slice(rim, rim + rows_x)
    own_y = slice(low, low + rows_y)

    def at(step_x, step_y):
        return (group, gx + step_x, gy + step_y)

    def both(first, second):
        if first is None:
            return second
        return first if second is None else jnp.logical_and(first, second)

    def exists(step_x, step_y):
        test = None
        if step_x:
            test = gx + step_x < size_x if step_x > 0 else gx > 0
        if step_y:
            test = both(test, gy + step_y < size_y if step_y > 0 else gy > 0)
        return test

    loads = [
        pltpu.make_async_copy(disp.at[0], B.at[0:3, own_x, own_y, :], load_sem.at[0]),
        pltpu.make_async_copy(mod.at[0], B.at[3, own_x, own_y, :], load_sem.at[1]),
        pltpu.make_async_copy(words, W.at[:, own_x, own_y, :], load_sem.at[2]),
        pltpu.make_async_copy(cmap, CM, load_sem.at[3]),
        pltpu.make_async_copy(vel.at[0], V, load_sem.at[4]),
    ]
    for load in loads:
        load.start()

    barrier = pltpu.get_barrier_semaphore()
    pl.semaphore_signal(barrier, inc=1, device_id=(1 - group, gx, gy), device_id_type=MESH)
    expected = jnp.int32(1)
    for step_x, step_y in directions:
        present = exists(step_x, step_y)
        expected = expected + present.astype(jnp.int32)

        @pl.when(present)
        def _():
            pl.semaphore_signal(
                barrier, inc=1, device_id=at(step_x, step_y), device_id_type=MESH
            )

    def clear(ref):
        ref[...] = jnp.zeros(ref.shape, ref.dtype)

    @pl.when(gx == 0)
    def _():
        clear(B.at[:, 0:rim])
        clear(W.at[:, 0:rim])
        clear(PX.at[0])
        for side in range(2):
            clear(PY.at[side, 0])

    @pl.when(gx == size_x - 1)
    def _():
        clear(B.at[:, rim + rows_x :])
        clear(PX.at[2])
        for side in range(2):
            clear(PY.at[side, 2])

    for side, edge in ((0, gy == 0), (1, gy == size_y - 1)):

        @pl.when(edge)
        def _():
            clear(YR.at[side])
            clear(YRW.at[side])
            for index in range(3):
                clear(PY.at[side, index])

    for index, (step_x, step_y) in enumerate(directions[4:]):

        @pl.when(jnp.logical_not(exists(-step_x, -step_y)))
        def _():
            clear(CR.at[index])
            if step_x > 0:
                clear(CRW.at[index])

    for load in loads[:3]:
        load.wait()

    def rows_for(step_y):
        return slice(low + rows_y - rim, low + rows_y) if step_y > 0 else slice(low, low + rim)

    for step_y in (1, -1):
        side = 0 if step_y > 0 else 1
        for x in range(rows_x):
            for field in range(4):
                YS[side, field, rim * x : rim * x + rim, :] = B[
                    field, rim + x, rows_for(step_y), :
                ]

        @pl.when(is_zone)
        def _():
            for x in range(rows_x):
                for word in range(2):
                    YSW[side, word, rim * x : rim * x + rim, :] = W[
                        word, rim + x, rows_for(step_y), :
                    ]

    for index, (step_x, step_y) in enumerate(directions[4:]):
        for count in range(2):
            x = rim + (rows_x - 2 + count if step_x > 0 else count)
            for field in range(4):
                CS[index, field, rim * count : rim * count + rim, :] = B[
                    field, x, rows_for(step_y), :
                ]
        if step_x > 0:

            @pl.when(is_zone)
            def _():
                for count in range(2):
                    x = rim + rows_x - 2 + count
                    for word in range(2):
                        CSW[index, word, rim * count : rim * count + rim, :] = W[
                            word, x, rows_for(step_y), :
                        ]

    lanes = lax.broadcasted_iota(jnp.int32, (8, depth), 1)
    wide_lanes = lax.broadcasted_iota(jnp.int32, (rows_y, depth), 1)
    wide_layer = lax.rem(wide_lanes, 3)
    loads[3].wait()

    def packed_map():
        source = lax.broadcasted_iota(jnp.int32, (3 * rows_x, depth), 0)
        target = lax.broadcasted_iota(jnp.int32, (3 * rows_x, depth), 1)
        chosen = jnp.logical_and(
            lax.div(source, rows_x) == lax.rem(target, 3),
            lax.rem(source, rows_x) == lax.rem(lax.div(target, 3), rows_x),
        )
        values = CM[...].reshape(3 * rows_x, rows_y).astype(jnp.float32)
        spread = lax.dot_general(
            values,
            chosen.astype(jnp.float32),
            (((0,), (0,)), ((), ())),
            preferred_element_type=jnp.float32,
        )
        return (spread + 0.5).astype(jnp.int32)

    @pl.when(is_slab)
    def _():
        for tile in range(2):
            rows = slice(low + 8 * tile, low + 8 * tile + 8)
            top = jnp.zeros((8, depth), jnp.float32)
            for c in range(3):
                for x in range(rows_x):
                    place = 3 * (rows_x * c + x)
                    moved = turn(B[c, rim + x, rows, :], depth - 3 - place)
                    top = jnp.where(
                        jnp.logical_and(lanes >= place, lanes < place + 3), moved, top
                    )
            RS[8 * tile : 8 * tile + 8, :] = top
        top = RS[...]
        away = packed_map() - wide_layer
        coupled = jnp.zeros((rows_y, depth), jnp.float32)
        for by in range(-2, 3):
            coupled = jnp.where(away == by, turn(top, by), coupled)
        PS[...] = coupled

    pl.semaphore_wait(barrier, expected)

    def message(source, target, sends, recvs, index, device):
        return pltpu.make_async_remote_copy(
            src_ref=source, dst_ref=target,
            send_sem=sends.at[index], recv_sem=recvs.at[index],
            device_id=device, device_id_type=MESH,
        )

    def field_parts(index):
        step_x, step_y = directions[index]
        if step_y == 0:
            if step_x > 0:
                return B.at[:, rows_x : rows_x + rim, own_y, :], B.at[:, 0:rim, own_y, :]
            return (
                B.at[:, rim : 2 * rim, own_y, :],
                B.at[:, rim + rows_x : 2 * rim + rows_x, own_y, :],
            )
        if step_x == 0:
            side = 0 if step_y > 0 else 1
            return YS.at[side], YR.at[side]
        return CS.at[index - 4], CR.at[index - 4]

    def word_parts(index):
        step_x, step_y = directions[index]
        if step_y == 0:
            return W.at[:, rows_x : rows_x + rim, own_y, :], W.at[:, 0:rim, own_y, :]
        if step_x == 0:
            side = 0 if step_y > 0 else 1
            return YSW.at[side], YRW.at[side]
        return CSW.at[index - 4], CRW.at[index - 4]

    def coupled_parts(index):
        step_x, step_y = directions[index]
        if step_y == 0:
            return PX.at[1], PX.at[1 - step_x]
        if step_y > 0:
            return PX.at[1, 8:16, :], PY.at[0, 1 - step_x]
        return PX.at[1, 0:8, :], PY.at[1, 1 - step_x]

    def send(parts, sends, recvs, index):
        source, target = parts(index)
        return message(source, target, sends, recvs, index, at(*directions[index]))

    has_words = [index for index, (step_x, _) in enumerate(directions) if step_x >= 0]
    order = [0, 1, 4, 5, 6, 7, 2, 3]

    link_up = message(PS, PX.at[1], link_s, link_r, 0, (1 - group, gx, gy))
    link_down = message(RS, RR, link_s, link_r, 1, (1 - group, gx, gy))

    @pl.when(is_slab)
    def _():
        link_up.start()

    for index in order:

        @pl.when(exists(*directions[index]))
        def _():
            send(field_parts, fs, fr, index).start()

    @pl.when(is_zone)
    def _():
        for index in order:
            if index in has_words:

                @pl.when(exists(*directions[index]))
                def _():
                    send(word_parts, ws, wr, index).start()

        link_up.wait_recv()
        for index in order:

            @pl.when(exists(*directions[index]))
            def _():
                send(coupled_parts, ps, pr, index).start()

    loads[4].wait()

    def arrived(index):
        step_x, step_y = directions[index]
        return exists(-step_x, -step_y)

    for index in range(8):

        @pl.when(arrived(index))
        def _():
            send(field_parts, fs, fr, index).wait_recv()

    for side in range(2):
        rows = slice(low - rim, low) if side == 0 else slice(low + rows_y, low + rows_y + rim)
        for x in range(rows_x):
            for field in range(4):
                B[field, rim + x, rows, :] = YR[side, field, rim * x : rim * x + rim, :]
    for index, (step_x, step_y) in enumerate(directions[4:]):
        rows = slice(low - rim, low) if step_y > 0 else slice(low + rows_y, low + rows_y + rim)
        for count in range(2):
            x = 1 + count if step_x > 0 else rim + rows_x + count
            for field in range(4):
                B[field, x, rows, :] = CR[index, field, rim * count : rim * count + rim, :]

    @pl.when(is_zone)
    def _():
        for index in has_words:

            @pl.when(arrived(index))
            def _():
                send(word_parts, ws, wr, index).wait_recv()

        for side in range(2):
            rows = slice(low - rim, low) if side == 0 else slice(low + rows_y, low + rows_y + rim)
            for x in range(rows_x):
                for word in range(2):
                    W[word, rim + x, rows, :] = YRW[side, word, rim * x : rim * x + rim, :]
        for index, (step_x, step_y) in enumerate(directions[4:]):
            if step_x < 0:
                continue
            rows = slice(low - rim, low) if step_y > 0 else slice(low + rows_y, low + rows_y + rim)
            for count in range(2):
                for word in range(2):
                    W[word, 1 + count, rows, :] = CRW[
                        index, word, rim * count : rim * count + rim, :
                    ]

        tiles = [slice(8 * tile, 8 * tile + 8) for tile in range(4)]

        def turn_words(x, carry):
            for word in range(2):
                for rows in tiles:
                    value = W[word, x, rows, :]
                    for place, by in enumerate(shifts):
                        WR[place, word, x, rows, :] = turn(value, by)
            return carry

        lax.fori_loop(1, rim + rows_x, turn_words, 0)

        def turn_modulus(x, carry):
            for rows in tiles:
                value = B[3, x, rows, :]
                for place, by in enumerate(shifts):
                    R[place, 3, x, rows, :] = turn(value, by)
            return carry

        lax.fori_loop(1, 2 * rim + rows_x - 1, turn_modulus, 0)

        for index in range(8):

            @pl.when(arrived(index))
            def _():
                send(coupled_parts, ps, pr, index).wait_recv()

        def turn_fields(x, carry):
            beside = jnp.where(x < rim, 0, jnp.where(x < rim + rows_x, 1, 2))
            inner = lax.rem(x + rows_x - rim, rows_x)
            for tile, rows in enumerate(tiles):
                if tile == 0:
                    packed = PY[0, beside]
                elif tile == 3:
                    packed = PY[1, beside]
                else:
                    packed = PX[beside, 8 * tile - 8 : 8 * tile, :]
                for c in range(3):
                    place = 3 * (rows_x * c + inner)
                    moved = pltpu.roll(packed, lax.rem(depth - place, depth), 1)
                    value = jnp.where(lanes < 3, moved, B[c, x, rows, :])
                    R[4, c, x, rows, :] = value
                    for spot, by in enumerate(shifts):
                        R[spot, c, x, rows, :] = scaled(by if c == 2 else 1, turn(value, by))
            return carry

        lax.fori_loop(0, 2 * rim + rows_x, turn_fields, 0)

        def turn_far(x, carry):
            for rows in tiles[1:3]:
                where = slice(rows.start - low, rows.stop - low)
                for spot, by in enumerate((3, -3)):
                    R3[spot, 0, x, where, :] = turn(B[3, rim + x, rows, :], by)
                    R3[spot, 1, x, where, :] = by * turn(R[4, 2, rim + x, rows, :], by)
                WR3[x, where, :] = turn(W[0, rim + x, rows, :], -3)
            return carry

        lax.fori_loop(0, rows_x, turn_far, 0)

        classes = sorted({tuple(abs(delta) for delta in offset) for offset in offsets})

        def zone_row(x, carry):
            for tile in range(2):
                here = slice(8 * tile, 8 * tile + 8)

                def load(field, delta):
                    delta_x, delta_y, delta_z = delta
                    if abs(delta_z) == 3:
                        return R3[0 if delta_z > 0 else 1, {3: 0, 2: 1}[field], x, here, :]
                    first = low + 8 * tile + delta_y
                    rows = slice(first, first + 8)
                    if delta_z == 0:
                        source = B.at[3] if field == 3 else R.at[4, field]
                        return source[x + rim + delta_x, rows, :]
                    return R[shifts.index(delta_z), field, x + rim + delta_x, rows, :]

                def load_word(word, delta):
                    delta_x, delta_y, delta_z = delta
                    if delta_z == -3:
                        return WR3[x, here, :]
                    first = low + 8 * tile + delta_y
                    rows = slice(first, first + 8)
                    if delta_z == 0:
                        return W[word, x + rim + delta_x, rows, :]
                    return WR[shifts.index(delta_z), word, x + rim + delta_x, rows, :]

                centre = [load(field, (0, 0, 0)) for field in range(4)]
                centre_words = [load_word(word, (0, 0, 0)) for word in range(2)]
                force = [jnp.zeros((8, depth), jnp.float32) for _ in range(3)]
                for kind in classes:
                    weight = (
                        0.5
                        * bond_scale
                        / float(kind[0] ** 2 + kind[1] ** 2 + kind[2] ** 2) ** 1.5
                    )
                    sums = [None, None, None]
                    signs = [(1, -1) if size else (1,) for size in kind]
                    for sign_x in signs[0]:
                        for sign_y in signs[1]:
                            parts = {}
                            for sign_z in signs[2]:
                                delta = (sign_x * kind[0], sign_y * kind[1], sign_z * kind[2])
                                ahead = delta > (0, 0, 0)
                                number = numbers[
                                    delta if ahead else tuple(-value for value in delta)
                                ]
                                word = number // 31
                                flags = (
                                    centre_words[word] if ahead else load_word(word, delta)
                                )
                                intact = (flags & (1 << number % 31)) != 0
                                there = []
                                for c in range(3):
                                    if delta[c]:
                                        coefficient = delta[c]
                                        if c == 2:
                                            coefficient = 1
                                        there.append((coefficient, load(c, delta)))
                                along = combine(there)
                                base = combine(
                                    [(delta[c], centre[c]) for c in range(3) if delta[c]]
                                )
                                strength = (centre[3] + load(3, delta)) * (along - base)
                                parts[sign_z] = jnp.where(intact, strength, 0.0)
                            if kind[2]:
                                plain = parts[1] + parts[-1]
                                tilted = parts[1] - parts[-1]
                            else:
                                plain = parts[1]
                                tilted = None
                            for c, value in enumerate(
                                (plain if kind[0] else None, plain if kind[1] else None, tilted)
                            ):
                                if value is None:
                                    continue
                                sign = (sign_x, sign_y, 1)[c]
                                if sums[c] is None:
                                    sums[c] = value if sign > 0 else -value
                                elif sign > 0:
                                    sums[c] = sums[c] + value
                                else:
                                    sums[c] = sums[c] - value
                    for c in range(3):
                        if sums[c] is not None:
                            force[c] = force[c] + (weight * kind[c]) * sums[c]
                moving = lanes >= 3
                for c in range(3):
                    old = V[c, x, here, :]
                    speed = jnp.where(moving, old + time_step * force[c], old)
                    out_v[0, c, x, here, :] = speed
                    out_u[0, c, x, here, :] = jnp.where(
                        moving, centre[c] + time_step * speed, centre[c]
                    )
                    place = 3 * (rows_x * c + x)
                    moved = pltpu.roll(force[c], place, 1)
                    RS[here, :] = jnp.where(
                        jnp.logical_and(lanes >= place, lanes < place + 3), moved, RS[here, :]
                    )
            return carry

        RS[...] = jnp.zeros(RS.shape, RS.dtype)
        lax.fori_loop(0, rows_x, zone_row, 0)
        link_down.start()

    @pl.when(is_slab)
    def _():
        modal = modal_stiffness()
        last_x = gx == size_x - 1
        last_y = gy == size_y - 1
        row_ids = lax.broadcasted_iota(jnp.int32, (8, depth), 0)
        for tile in range(3):
            rows = slice(8 * tile, 8 * tile + 8)
            next_rows = slice(8 * tile + 1, 8 * tile + 9)
            solid = lanes < depth - 1
            if tile == 2:
                solid = jnp.logical_and(
                    solid, jnp.logical_or(row_ids < 7, jnp.logical_not(last_y))
                )

            def nodes(x):
                result = []
                for c in range(3):
                    here, there = B[c, x, rows, :], B[c, x, next_rows, :]
                    for value in (here + there, there - here):
                        above = turn(value, 1)
                        result += [value + above, above - value]
                return result

            below = nodes(rim - 1)
            carried = None
            for element in range(rows_x + 1):
                above = nodes(rim + element)
                modes = {}
                for c in range(3):
                    for pair in range(4):
                        first, second = below[4 * c + pair], above[4 * c + pair]
                        if pair:
                            modes[8 * c + pair] = first + second
                        modes[8 * c + 4 + pair] = second - first
                below = above
                inside = solid
                if element == rows_x:
                    inside = jnp.logical_and(inside, jnp.logical_not(last_x))
                stiff = jnp.where(inside, B[3, rim - 1 + element, rows, :], 0.0)
                loads_of = {}
                for i in range(24):
                    total = None
                    for j in range(24):
                        if modal[i, j]:
                            term = float(modal[i, j]) * modes[j]
                            total = term if total is None else total + term
                    if total is not None:
                        loads_of[i] = total * stiff
                lows, highs = [], []
                for c in range(3):
                    for pair in range(4):
                        flat, steep = loads_of.get(8 * c + pair), loads_of[8 * c + 4 + pair]
                        lows.append(-steep if flat is None else flat - steep)
                        highs.append(steep if flat is None else flat + steep)
                if element:
                    for c in range(3):
                        halves = []
                        for pair in range(2):
                            flat = lows[4 * c + 2 * pair] + carried[4 * c + 2 * pair]
                            steep = lows[4 * c + 2 * pair + 1] + carried[4 * c + 2 * pair + 1]
                            halves.append((flat - steep) + turn(flat + steep, -1))
                        SL[c, element - 1, rows, :] = halves[0] - halves[1]
                        SH[c, element - 1, rows, :] = halves[0] + halves[1]
                carried = highs

        def inverse_mass(x, tile):
            spread = jnp.where(jnp.logical_or(lanes == 0, lanes == depth - 1), 2.0, 1.0)
            ends_y = jnp.logical_or(
                jnp.logical_and(gy == 0, row_ids + 8 * tile == 0),
                jnp.logical_and(last_y, row_ids + 8 * tile == rows_y - 1),
            )
            spread = spread * jnp.where(ends_y, 2.0, 1.0)
            if x == 0:
                spread = spread * jnp.where(gx == 0, 2.0, 1.0)
            if x == rows_x - 1:
                spread = spread * jnp.where(last_x, 2.0, 1.0)
            return spread

        for x in range(rows_x):
            for tile in range(2):
                here = slice(8 * tile, 8 * tile + 8)
                factor = time_step * inverse_mass(x, tile)
                for c in range(3):
                    force = (
                        SL[c, x, low + 8 * tile : low + 8 * tile + 8, :]
                        + SH[c, x, low + 8 * tile - 1 : low + 8 * tile + 7, :]
                    )
                    out_v[0, c, x, here, :] = V[c, x, here, :] - factor * force

        mapped = packed_map()
        link_down.wait_recv()
        reaction = RR[...]
        shared = jnp.zeros((rows_y, depth), jnp.float32)
        for by in range(-2, 3):
            source_layer = wide_layer + by
            fits = jnp.logical_and(source_layer >= 0, source_layer < 3)
            chosen = jnp.logical_and(fits, turn(mapped, by) == wide_layer)
            shared = shared + jnp.where(chosen, turn(reaction, by), 0.0)
        unclamped = lanes > 0
        for tile in range(2):
            here = slice(8 * tile, 8 * tile + 8)
            part = shared[here, :]
            for x in range(rows_x):
                factor = jnp.where(lanes >= depth - 3, time_step * inverse_mass(x, tile), 0.0)
                for c in range(3):
                    place = 3 * (rows_x * c + x)
                    moved = turn(part, place + 3 - depth)
                    speed = jnp.where(unclamped, out_v[0, c, x, here, :] + factor * moved, 0.0)
                    out_v[0, c, x, here, :] = speed
                    out_u[0, c, x, here, :] = jnp.where(
                        unclamped,
                        B[c, rim + x, low + 8 * tile : low + 8 * tile + 8, :] + time_step * speed,
                        0.0,
                    )

    for index in range(8):

        @pl.when(exists(*directions[index]))
        def _():
            send(field_parts, fs, fr, index).wait_send()

            @pl.when(is_zone)
            def _():
                if index in has_words:
                    send(word_parts, ws, wr, index).wait_send()
                send(coupled_parts, ps, pr, index).wait_send()

    @pl.when(is_slab)
    def _():
        link_up.wait_send()

    @pl.when(is_zone)
    def _():
        link_down.wait_send()


def per_device(displacement, velocity, modulus, bond_words, coupling_map):
    _, _, rows_x, rows_y, depth = displacement.shape
    f32, i32 = jnp.float32, jnp.int32
    wide_x, wide_y = rows_x + 2 * rim, rows_y + 16
    packed = rim * rows_x
    dma = pltpu.SemaphoreType.DMA
    return pl.pallas_call(
        kernel,
        out_shape=(
            jax.ShapeDtypeStruct(displacement.shape, f32),
            jax.ShapeDtypeStruct(velocity.shape, f32),
        ),
        in_specs=[pl.BlockSpec(memory_space=pl.ANY)] * 5,
        out_specs=(pl.BlockSpec(memory_space=pltpu.VMEM),) * 2,
        scratch_shapes=[
            pltpu.VMEM((4, wide_x, wide_y, depth), f32),
            pltpu.VMEM((2, rim + rows_x, wide_y, depth), i32),
            pltpu.VMEM((3, rows_x, rows_y, depth), f32),
            pltpu.VMEM(coupling_map.shape, i32),
            pltpu.VMEM((2, 4, packed, depth), f32),
            pltpu.VMEM((2, 2, packed, depth), i32),
            pltpu.VMEM((2, 4, packed, depth), f32),
            pltpu.VMEM((2, 2, packed, depth), i32),
            pltpu.VMEM((4, 4, 8, depth), f32),
            pltpu.VMEM((2, 2, 8, depth), i32),
            pltpu.VMEM((4, 4, 8, depth), f32),
            pltpu.VMEM((2, 2, 8, depth), i32),
            pltpu.VMEM((rows_y, depth), f32),
            pltpu.VMEM((3, rows_y, depth), f32),
            pltpu.VMEM((2, 3, 8, depth), f32),
            pltpu.VMEM((rows_y, depth), f32),
            pltpu.VMEM((rows_y, depth), f32),
            pltpu.VMEM((5, 4, wide_x, wide_y, depth), f32),
            pltpu.VMEM((2, 2, rows_x, rows_y, depth), f32),
            pltpu.VMEM((4, 2, rim + rows_x, wide_y, depth), i32),
            pltpu.VMEM((rows_x, rows_y, depth), i32),
            pltpu.VMEM((3, rows_x, rows_y + 8, depth), f32),
            pltpu.VMEM((3, rows_x, rows_y + 8, depth), f32),
            dma((5,)), dma((8,)), dma((8,)), dma((8,)), dma((8,)), dma((8,)), dma((8,)),
            dma((2,)), dma((2,)),
        ],
        compiler_params=pltpu.CompilerParams(
            collective_id=0, has_side_effects=True, vmem_limit_bytes=56 * 1024 * 1024
        ),
    )(displacement, velocity, modulus, bond_words, coupling_map)


def solution(mesh):
    return jax.shard_map(
        per_device,
        mesh=mesh,
        in_specs=(
            P("group", None, "gx", "gy", None),
            P("group", None, "gx", "gy", None),
            P("group", "gx", "gy", None),
            P(None, "gx", "gy", None),
            P(None, "gx", "gy"),
        ),
        out_specs=(P("group", None, "gx", "gy", None), P("group", None, "gx", "gy", None)),
        check_vma=False,
    )
```

```python
import math

import jax
import jax.numpy as jnp
import numpy as np
from jax import lax
from jax.experimental import pallas as pl
from jax.experimental.pallas import tpu as pltpu
from jax.sharding import PartitionSpec as P

time_step = 0.1
bond_scale = 1.0
rim = 3
low = 8
MESH = pl.DeviceIdType.MESH
directions = [(1, 0), (-1, 0), (0, 1), (0, -1), (1, 1), (1, -1), (-1, 1), (-1, -1)]
shifts = [1, -1, 2, -2]


def half_offsets():
    table = []
    for delta_x in range(-3, 4):
        for delta_y in range(-3, 4):
            for delta_z in range(-3, 4):
                radius = delta_x * delta_x + delta_y * delta_y + delta_z * delta_z
                if 0 < radius <= 9 and (delta_x, delta_y, delta_z) > (0, 0, 0):
                    table.append((delta_x, delta_y, delta_z))
    return table


def hex_stiffness():
    poisson = 0.3
    lame_first = poisson / ((1.0 + poisson) * (1.0 - 2.0 * poisson))
    shear_modulus = 0.5 / (1.0 + poisson)
    elastic = np.zeros((6, 6))
    elastic[:3, :3] = lame_first
    for axis_id in range(3):
        elastic[axis_id, axis_id] += 2.0 * shear_modulus
        elastic[3 + axis_id, 3 + axis_id] = shear_modulus
    points = [0.5 - 0.5 / math.sqrt(3.0), 0.5 + 0.5 / math.sqrt(3.0)]
    result = np.zeros((24, 24))
    shear_pairs = ((0, 1), (1, 2), (0, 2))
    for along_x in points:
        for along_y in points:
            for along_z in points:
                coords = (along_x, along_y, along_z)
                gradients = np.zeros((3, 8))
                for corner in range(8):
                    corner_bits = (corner >> 2 & 1, corner >> 1 & 1, corner & 1)
                    factors = [
                        coords[axis_id] if corner_bits[axis_id] else 1.0 - coords[axis_id]
                        for axis_id in range(3)
                    ]
                    slopes = [1.0 if corner_bits[axis_id] else -1.0 for axis_id in range(3)]
                    gradients[0, corner] = slopes[0] * factors[1] * factors[2]
                    gradients[1, corner] = factors[0] * slopes[1] * factors[2]
                    gradients[2, corner] = factors[0] * factors[1] * slopes[2]
                strain = np.zeros((6, 24))
                for axis_id in range(3):
                    strain[axis_id, axis_id * 8 : axis_id * 8 + 8] = gradients[axis_id]
                for shear_row, pair in enumerate(shear_pairs):
                    left_axis, right_axis = pair
                    strain[3 + shear_row, left_axis * 8 : left_axis * 8 + 8] = gradients[right_axis]
                    strain[3 + shear_row, right_axis * 8 : right_axis * 8 + 8] = gradients[
                        left_axis
                    ]
                result += strain.T @ elastic @ strain / 8.0
    return result


def modal_stiffness():
    one = np.array([[1.0, -1.0], [1.0, 1.0]])
    corners = np.kron(np.kron(one, one), one)
    basis = np.kron(np.eye(3), corners)
    modal = basis.T @ hex_stiffness() @ basis / 64.0
    modal[np.abs(modal) < 1e-12] = 0.0
    return modal


offsets = half_offsets()
numbers = {offset: number for number, offset in enumerate(offsets)}
bonds = offsets + [tuple(-delta for delta in offset) for offset in offsets]


def scaled(coefficient, value):
    return value if coefficient == 1 else coefficient * value


def combine(terms):
    total = None
    negative = None
    for coefficient, value in terms:
        if coefficient == 0:
            continue
        if coefficient < 0 and total is None:
            negative = scaled(-coefficient, value) if negative is None else (
                negative + scaled(-coefficient, value)
            )
        elif total is None:
            total = scaled(coefficient, value)
            if negative is not None:
                total = total - negative
                negative = None
        elif coefficient > 0:
            total = total + scaled(coefficient, value)
        else:
            total = total - scaled(-coefficient, value)
    if negative is not None:
        total = 0.0 - negative
    return total


def turn(value, by):
    return pltpu.roll(value, (-by) % 128, value.ndim - 1)


def kernel(
    disp, vel, mod, words, cmap,
    out_u, out_v,
    B, W, V, CM,
    YS, YSW, YR, YRW, CS, CSW, CR, CRW,
    PS, PX, PY, RS, RR,
    R, R3, WR, WR3, K, SL, SH,
    load_sem, fs, fr, ms, mr, ws, wr, ps, pr, link_s, link_r,
):
    group = lax.axis_index("group")
    gx = lax.axis_index("gx")
    gy = lax.axis_index("gy")
    size_x = lax.axis_size("gx")
    size_y = lax.axis_size("gy")
    is_zone = group == 0
    is_slab = group == 1
    rows_x, rows_y, depth = V.shape[1], V.shape[2], V.shape[3]
    own_x = slice(rim, rim + rows_x)
    own_y = slice(low, low + rows_y)

    def at(step_x, step_y):
        return (group, gx + step_x, gy + step_y)

    def both(first, second):
        if first is None:
            return second
        return first if second is None else jnp.logical_and(first, second)

    def exists(step_x, step_y):
        test = None
        if step_x:
            test = gx + step_x < size_x if step_x > 0 else gx > 0
        if step_y:
            test = both(test, gy + step_y < size_y if step_y > 0 else gy > 0)
        return test

    loads = [
        pltpu.make_async_copy(disp.at[0], B.at[0:3, own_x, own_y, :], load_sem.at[0]),
        pltpu.make_async_copy(mod.at[0], B.at[3, own_x, own_y, :], load_sem.at[1]),
        pltpu.make_async_copy(words, W.at[:, own_x, own_y, :], load_sem.at[2]),
        pltpu.make_async_copy(cmap, CM, load_sem.at[3]),
        pltpu.make_async_copy(vel.at[0], V, load_sem.at[4]),
    ]
    for load in loads:
        load.start()

    barrier = pltpu.get_barrier_semaphore()
    pl.semaphore_signal(barrier, inc=1, device_id=(1 - group, gx, gy), device_id_type=MESH)
    expected = jnp.int32(1)
    for step_x, step_y in directions:
        present = exists(step_x, step_y)
        expected = expected + jnp.where(is_slab, 2, 1) * present.astype(jnp.int32)

        @pl.when(present)
        def _():
            pl.semaphore_signal(
                barrier, inc=1, device_id=at(step_x, step_y), device_id_type=MESH
            )

            @pl.when(is_zone)
            def _():
                pl.semaphore_signal(
                    barrier,
                    inc=1,
                    device_id=(1 - group, gx + step_x, gy + step_y),
                    device_id_type=MESH,
                )

    def clear(ref):
        ref[...] = jnp.zeros(ref.shape, ref.dtype)

    @pl.when(gx == 0)
    def _():
        clear(B.at[:, 0:rim])
        clear(W.at[:, 0:rim])
        clear(PX.at[0])
        for side in range(2):
            clear(PY.at[side, 0])

    @pl.when(gx == size_x - 1)
    def _():
        clear(B.at[:, rim + rows_x :])
        clear(PX.at[2])
        for side in range(2):
            clear(PY.at[side, 2])

    for side, edge in ((0, gy == 0), (1, gy == size_y - 1)):

        @pl.when(edge)
        def _():
            clear(YR.at[side])
            clear(YRW.at[side])
            for index in range(3):
                clear(PY.at[side, index])

    for index, (step_x, step_y) in enumerate(directions[4:]):

        @pl.when(jnp.logical_not(exists(-step_x, -step_y)))
        def _():
            clear(CR.at[index])
            if step_x > 0:
                clear(CRW.at[index])

    for load in loads[:3]:
        load.wait()

    def rows_for(step_y):
        return slice(low + rows_y - rim, low + rows_y) if step_y > 0 else slice(low, low + rim)

    for step_y in (1, -1):
        side = 0 if step_y > 0 else 1
        for x in range(rows_x):
            for field in range(4):
                YS[side, field, rim * x : rim * x + rim, :] = B[
                    field, rim + x, rows_for(step_y), :
                ]

        @pl.when(is_zone)
        def _():
            for x in range(rows_x):
                for word in range(2):
                    YSW[side, word, rim * x : rim * x + rim, :] = W[
                        word, rim + x, rows_for(step_y), :
                    ]

    for index, (step_x, step_y) in enumerate(directions[4:]):
        for count in range(2):
            x = rim + (rows_x - 2 + count if step_x > 0 else count)
            for field in range(4):
                CS[index, field, rim * count : rim * count + rim, :] = B[
                    field, x, rows_for(step_y), :
                ]
        if step_x > 0:

            @pl.when(is_zone)
            def _():
                for count in range(2):
                    x = rim + rows_x - 2 + count
                    for word in range(2):
                        CSW[index, word, rim * count : rim * count + rim, :] = W[
                            word, x, rows_for(step_y), :
                        ]

    lanes = lax.broadcasted_iota(jnp.int32, (8, depth), 1)
    wide_lanes = lax.broadcasted_iota(jnp.int32, (rows_y, depth), 1)
    wide_layer = lax.rem(wide_lanes, 3)
    loads[3].wait()

    def packed_map():
        source = lax.broadcasted_iota(jnp.int32, (3 * rows_x, depth), 0)
        target = lax.broadcasted_iota(jnp.int32, (3 * rows_x, depth), 1)
        chosen = jnp.logical_and(
            lax.div(source, rows_x) == lax.rem(target, 3),
            lax.rem(source, rows_x) == lax.rem(lax.div(target, 3), rows_x),
        )
        values = CM[...].reshape(3 * rows_x, rows_y).astype(jnp.float32)
        spread = lax.dot_general(
            values,
            chosen.astype(jnp.float32),
            (((0,), (0,)), ((), ())),
            preferred_element_type=jnp.float32,
        )
        return (spread + 0.5).astype(jnp.int32)

    @pl.when(is_slab)
    def _():
        for tile in range(2):
            rows = slice(low + 8 * tile, low + 8 * tile + 8)
            top = jnp.zeros((8, depth), jnp.float32)
            for c in range(3):
                for x in range(rows_x):
                    place = 3 * (rows_x * c + x)
                    moved = turn(B[c, rim + x, rows, :], depth - 3 - place)
                    top = jnp.where(
                        jnp.logical_and(lanes >= place, lanes < place + 3), moved, top
                    )
            RS[8 * tile : 8 * tile + 8, :] = top
        top = RS[...]
        away = packed_map() - wide_layer
        coupled = jnp.zeros((rows_y, depth), jnp.float32)
        for by in range(-2, 3):
            coupled = jnp.where(away == by, turn(top, by), coupled)
        PS[...] = coupled

    pl.semaphore_wait(barrier, expected)

    def message(source, target, sends, recvs, index, device):
        return pltpu.make_async_remote_copy(
            src_ref=source, dst_ref=target,
            send_sem=sends.at[index], recv_sem=recvs.at[index],
            device_id=device, device_id_type=MESH,
        )

    def field_parts(index, fields=slice(0, 3)):
        step_x, step_y = directions[index]
        if step_y == 0:
            if step_x > 0:
                return B.at[fields, rows_x : rows_x + rim, own_y, :], B.at[fields, 0:rim, own_y, :]
            return (
                B.at[fields, rim : 2 * rim, own_y, :],
                B.at[fields, rim + rows_x : 2 * rim + rows_x, own_y, :],
            )
        if step_x == 0:
            side = 0 if step_y > 0 else 1
            return YS.at[side, fields], YR.at[side, fields]
        return CS.at[index - 4, fields], CR.at[index - 4, fields]

    def modulus_parts(index):
        return field_parts(index, 3)

    def word_parts(index):
        step_x, step_y = directions[index]
        if step_y == 0:
            return W.at[:, rows_x : rows_x + rim, own_y, :], W.at[:, 0:rim, own_y, :]
        if step_x == 0:
            side = 0 if step_y > 0 else 1
            return YSW.at[side], YRW.at[side]
        return CSW.at[index - 4], CRW.at[index - 4]

    def coupled_parts(index):
        if index == 8:
            return PS, PX.at[1]
        step_x, step_y = directions[index]
        if step_y == 0:
            return PS, PX.at[1 - step_x]
        if step_y > 0:
            return PS.at[8:16, :], PY.at[0, 1 - step_x]
        return PS.at[0:8, :], PY.at[1, 1 - step_x]

    def send(parts, sends, recvs, index):
        source, target = parts(index)
        return message(source, target, sends, recvs, index, at(*directions[index]))

    def send_coupled(index):
        source, target = coupled_parts(index)
        step_x, step_y = directions[index] if index < 8 else (0, 0)
        device = (1 - group, gx + step_x, gy + step_y)
        return message(source, target, ps, pr, index, device)

    has_words = [index for index, (step_x, _) in enumerate(directions) if step_x >= 0]
    order = [0, 1, 4, 5, 6, 7, 2, 3]

    link_down = message(RS, RR, link_s, link_r, 0, (1 - group, gx, gy))

    @pl.when(is_slab)
    def _():
        send_coupled(8).start()
        for index in order:

            @pl.when(exists(*directions[index]))
            def _():
                send_coupled(index).start()

    for index in order:

        @pl.when(exists(*directions[index]))
        def _():
            send(modulus_parts, ms, mr, index).start()
            if index in has_words:

                @pl.when(is_zone)
                def _():
                    send(word_parts, ws, wr, index).start()

    for index in order:

        @pl.when(exists(*directions[index]))
        def _():
            send(field_parts, fs, fr, index).start()

    loads[4].wait()

    def arrived(index):
        step_x, step_y = directions[index]
        return exists(-step_x, -step_y)

    def receive_fields(parts, recvs, fields):
        for index in range(8):

            @pl.when(arrived(index))
            def _():
                send(parts, fs, recvs, index).wait_recv()

        for side in range(2):
            rows = slice(low - rim, low) if side == 0 else slice(low + rows_y, low + rows_y + rim)
            for x in range(rows_x):
                for field in fields:
                    B[field, rim + x, rows, :] = YR[side, field, rim * x : rim * x + rim, :]
        for index, (step_x, step_y) in enumerate(directions[4:]):
            rows = slice(low - rim, low) if step_y > 0 else slice(low + rows_y, low + rows_y + rim)
            for count in range(2):
                x = 1 + count if step_x > 0 else rim + rows_x + count
                for field in fields:
                    B[field, x, rows, :] = CR[index, field, rim * count : rim * count + rim, :]

    @pl.when(is_zone)
    def _():
        tiles = [slice(8 * tile, 8 * tile + 8) for tile in range(4)]
        beside_x = (1, 2, rim + rows_x, rim + rows_x + 1)

        def turn_words(x, chosen):
            for word in range(2):
                for rows in chosen:
                    value = W[word, x, rows, :]
                    for place, by in enumerate(shifts):
                        WR[place, word, x, rows, :] = turn(value, by)

        def turn_fields(x, chosen, fields):
            for field in fields:
                for rows in chosen:
                    value = B[field, x, rows, :]
                    for place, by in enumerate(shifts):
                        R[place, field, x, rows, :] = scaled(
                            by if field == 2 else 1, turn(value, by)
                        )

        def turn_own(x, carry):
            turn_words(rim + x, tiles[1:3])
            turn_fields(rim + x, tiles[1:3], range(4))
            for rows in tiles[1:3]:
                where = slice(rows.start - low, rows.stop - low)
                for spot, by in enumerate((3, -3)):
                    R3[spot, 0, x, where, :] = turn(B[3, rim + x, rows, :], by)
                    R3[spot, 1, x, where, :] = by * turn(B[2, rim + x, rows, :], by)
                WR3[x, where, :] = turn(W[0, rim + x, rows, :], -3)
            return carry

        lax.fori_loop(0, rows_x, turn_own, 0)

        receive_fields(modulus_parts, mr, (3,))
        for index in has_words:

            @pl.when(arrived(index))
            def _():
                send(word_parts, ws, wr, index).wait_recv()

        for side in range(2):
            rows = slice(low - rim, low) if side == 0 else slice(low + rows_y, low + rows_y + rim)
            for x in range(rows_x):
                for word in range(2):
                    W[word, rim + x, rows, :] = YRW[side, word, rim * x : rim * x + rim, :]
        for index, (step_x, step_y) in enumerate(directions[4:]):
            if step_x < 0:
                continue
            rows = slice(low - rim, low) if step_y > 0 else slice(low + rows_y, low + rows_y + rim)
            for count in range(2):
                for word in range(2):
                    W[word, 1 + count, rows, :] = CRW[
                        index, word, rim * count : rim * count + rim, :
                    ]

        def turn_beside(x, carry):
            turn_words(rim + x, (tiles[0], tiles[3]))
            turn_fields(rim + x, (tiles[0], tiles[3]), (3,))
            return carry

        lax.fori_loop(0, rows_x, turn_beside, 0)
        for x in beside_x:
            turn_fields(x, tiles, (3,))
            if x < rim:
                turn_words(x, tiles)

        def factor_row(x, carry):
            for tile in range(2):
                here = slice(8 * tile, 8 * tile + 8)

                def there(delta):
                    first = low + 8 * tile + delta[1]
                    return x + rim + delta[0], slice(first, first + 8)

                def load_modulus(delta):
                    if abs(delta[2]) == 3:
                        return R3[0 if delta[2] > 0 else 1, 0, x, here, :]
                    at_x, rows = there(delta)
                    if delta[2] == 0:
                        return B[3, at_x, rows, :]
                    return R[shifts.index(delta[2]), 3, at_x, rows, :]

                def load_word(word, delta):
                    if delta[2] == -3:
                        return WR3[x, here, :]
                    at_x, rows = there(delta)
                    if delta[2] == 0:
                        return W[word, at_x, rows, :]
                    return WR[shifts.index(delta[2]), word, at_x, rows, :]

                centre = load_modulus((0, 0, 0))
                centre_words = [load_word(word, (0, 0, 0)) for word in range(2)]
                for index, delta in enumerate(bonds):
                    radius = sum(value * value for value in delta)
                    weight = 0.5 * bond_scale / float(radius) ** 1.5
                    ahead = delta > (0, 0, 0)
                    number = numbers[delta if ahead else tuple(-value for value in delta)]
                    word = number // 31
                    flags = centre_words[word] if ahead else load_word(word, delta)
                    intact = (flags & (1 << number % 31)) != 0
                    K[index, x, here, :] = jnp.where(
                        intact, weight * (centre + load_modulus(delta)), 0.0
                    )
            return carry

        lax.fori_loop(0, rows_x, factor_row, 0)

        receive_fields(field_parts, fr, range(3))

        def turn_around(x, carry):
            turn_fields(rim + x, (tiles[0], tiles[3]), range(3))
            return carry

        lax.fori_loop(0, rows_x, turn_around, 0)
        for x in beside_x:
            turn_fields(x, tiles, range(3))

        send_coupled(8).wait_recv()
        for index in range(8):

            @pl.when(arrived(index))
            def _():
                send_coupled(index).wait_recv()

        def merge(x, inner, beside, outer):
            for tile, rows in enumerate(tiles):
                if tile == 0:
                    packed = PY[0, beside]
                elif tile == 3:
                    packed = PY[1, beside]
                else:
                    packed = PX[beside, 8 * tile - 8 : 8 * tile, :]
                for c in range(3):
                    place = 3 * (rows_x * c + inner)

                    def moved(by):
                        return pltpu.roll(packed, lax.rem(2 * depth - place - by, depth), 1)

                    R[4, c, x, rows, :] = jnp.where(lanes < 3, moved(0), B[c, x, rows, :])
                    if outer:
                        continue
                    for spot, by in enumerate(shifts):
                        inside = lanes < 3 - by
                        if by < 0:
                            inside = jnp.logical_and(inside, lanes >= -by)
                        R[spot, c, x, rows, :] = jnp.where(
                            inside, scaled(by if c == 2 else 1, moved(by)), R[spot, c, x, rows, :]
                        )
                    if c == 2 and beside == 1 and tile in (1, 2):
                        where = slice(rows.start - low, rows.stop - low)
                        inside = jnp.logical_and(lanes >= 3, lanes < 6)
                        R3[1, 1, inner, where, :] = jnp.where(
                            inside, -3 * moved(-3), R3[1, 1, inner, where, :]
                        )

        def merge_own(x, carry):
            merge(rim + x, x, 1, False)
            return carry

        lax.fori_loop(0, rows_x, merge_own, 0)
        for x in range(rim):
            merge(x, rows_x - rim + x, 0, x == 0)
            merge(rim + rows_x + x, x, 2, x == rim - 1)

        group_of = 4

        def zone_rows(step, carry):
            start = step * group_of
            for tile in range(2):
                here = slice(8 * tile, 8 * tile + 8)

                def load(field, move_x, delta_y, delta_z):
                    if abs(delta_z) == 3:
                        return R3[0 if delta_z > 0 else 1, 1, start + move_x, here, :]
                    first = low + 8 * tile + delta_y
                    place = 4 if delta_z == 0 else shifts.index(delta_z)
                    return R[place, field, start + rim + move_x, slice(first, first + 8), :]

                def added(total, sign, value):
                    if total is None:
                        return value if sign > 0 else -value
                    return total + value if sign > 0 else total - value

                centre = [
                    [load(c, member, 0, 0) for c in range(3)] for member in range(group_of)
                ]
                along_x = [[None] * 4 for _ in range(group_of)]
                along_z = [[None] * 4 for _ in range(group_of)]
                along_y = [None] * group_of
                for delta_y in range(-3, 4):
                    sheet = [None] * group_of
                    for delta_z in range(-3, 4):
                        left = 9 - delta_y * delta_y - delta_z * delta_z
                        if left < 0:
                            continue
                        reach = math.isqrt(left)
                        base = [
                            combine([(delta_y, centre[member][1]), (delta_z, centre[member][2])])
                            for member in range(group_of)
                        ]
                        line = [None] * group_of
                        for move_x in range(-reach, group_of + reach):
                            members = [
                                member
                                for member in range(group_of)
                                if abs(move_x - member) <= reach
                                and (move_x - member, delta_y, delta_z) != (0, 0, 0)
                            ]
                            if not members:
                                continue
                            if any(move_x != member for member in members):
                                away = load(0, move_x, delta_y, delta_z)
                            side = combine(
                                [
                                    (delta_y, load(1, move_x, delta_y, delta_z) if delta_y else None),
                                    (
                                        1 if delta_z else 0,
                                        load(2, move_x, delta_y, delta_z) if delta_z else None,
                                    ),
                                ]
                            )
                            for member in members:
                                delta_x = move_x - member
                                stretch = None
                                if side is not None:
                                    stretch = side - base[member]
                                if delta_x:
                                    gap = away - centre[member][0]
                                    if stretch is None:
                                        stretch = scaled(delta_x, gap)
                                    elif abs(delta_x) == 1:
                                        stretch = added(stretch, delta_x, gap)
                                    else:
                                        stretch = stretch + delta_x * gap
                                index = bonds.index((delta_x, delta_y, delta_z))
                                pull = K[index, start + member, here, :] * stretch
                                line[member] = added(line[member], 1, pull)
                                if delta_x:
                                    along_x[member][abs(delta_x)] = added(
                                        along_x[member][abs(delta_x)], delta_x, pull
                                    )
                        for member in range(group_of):
                            sheet[member] = added(sheet[member], 1, line[member])
                            if delta_z:
                                along_z[member][abs(delta_z)] = added(
                                    along_z[member][abs(delta_z)], delta_z, line[member]
                                )
                    if delta_y:
                        for member in range(group_of):
                            term = scaled(abs(delta_y), sheet[member])
                            along_y[member] = added(along_y[member], delta_y, term)

                moving = lanes >= 3
                for member in range(group_of):
                    x = start + member
                    force = [
                        combine([(size, along_x[member][size]) for size in (1, 2, 3)]),
                        along_y[member],
                        combine([(size, along_z[member][size]) for size in (1, 2, 3)]),
                    ]
                    for c in range(3):
                        old = V[c, x, here, :]
                        speed = jnp.where(moving, old + time_step * force[c], old)
                        out_v[0, c, x, here, :] = speed
                        out_u[0, c, x, here, :] = jnp.where(
                            moving, centre[member][c] + time_step * speed, centre[member][c]
                        )
                        place = 3 * (rows_x * c + x)
                        moved = pltpu.roll(force[c], place, 1)
                        RS[here, :] = jnp.where(
                            jnp.logical_and(lanes >= place, lanes < place + 3), moved, RS[here, :]
                        )
            return carry

        RS[...] = jnp.zeros(RS.shape, RS.dtype)
        lax.fori_loop(0, rows_x // group_of, zone_rows, 0)
        link_down.start()

    @pl.when(is_slab)
    def _():
        receive_fields(modulus_parts, mr, (3,))
        receive_fields(field_parts, fr, range(3))
        modal = modal_stiffness()
        last_x = gx == size_x - 1
        last_y = gy == size_y - 1
        row_ids = lax.broadcasted_iota(jnp.int32, (8, depth), 0)
        for tile in range(3):
            rows = slice(8 * tile, 8 * tile + 8)
            next_rows = slice(8 * tile + 1, 8 * tile + 9)
            solid = lanes < depth - 1
            if tile == 2:
                solid = jnp.logical_and(
                    solid, jnp.logical_or(row_ids < 7, jnp.logical_not(last_y))
                )

            def nodes(x):
                result = []
                for c in range(3):
                    here, there = B[c, x, rows, :], B[c, x, next_rows, :]
                    for value in (here + there, there - here):
                        above = turn(value, 1)
                        result += [value + above, above - value]
                return result

            below = nodes(rim - 1)
            carried = None
            for element in range(rows_x + 1):
                above = nodes(rim + element)
                modes = {}
                for c in range(3):
                    for pair in range(4):
                        first, second = below[4 * c + pair], above[4 * c + pair]
                        if pair:
                            modes[8 * c + pair] = first + second
                        modes[8 * c + 4 + pair] = second - first
                below = above
                inside = solid
                if element == rows_x:
                    inside = jnp.logical_and(inside, jnp.logical_not(last_x))
                stiff = jnp.where(inside, B[3, rim - 1 + element, rows, :], 0.0)
                loads_of = {}
                for i in range(24):
                    total = None
                    for j in range(24):
                        if modal[i, j]:
                            term = float(modal[i, j]) * modes[j]
                            total = term if total is None else total + term
                    if total is not None:
                        loads_of[i] = total * stiff
                lows, highs = [], []
                for c in range(3):
                    for pair in range(4):
                        flat, steep = loads_of.get(8 * c + pair), loads_of[8 * c + 4 + pair]
                        lows.append(-steep if flat is None else flat - steep)
                        highs.append(steep if flat is None else flat + steep)
                if element:
                    for c in range(3):
                        halves = []
                        for pair in range(2):
                            flat = lows[4 * c + 2 * pair] + carried[4 * c + 2 * pair]
                            steep = lows[4 * c + 2 * pair + 1] + carried[4 * c + 2 * pair + 1]
                            halves.append((flat - steep) + turn(flat + steep, -1))
                        SL[c, element - 1, rows, :] = halves[0] - halves[1]
                        SH[c, element - 1, rows, :] = halves[0] + halves[1]
                carried = highs

        def inverse_mass(x, tile):
            spread = jnp.where(jnp.logical_or(lanes == 0, lanes == depth - 1), 2.0, 1.0)
            ends_y = jnp.logical_or(
                jnp.logical_and(gy == 0, row_ids + 8 * tile == 0),
                jnp.logical_and(last_y, row_ids + 8 * tile == rows_y - 1),
            )
            spread = spread * jnp.where(ends_y, 2.0, 1.0)
            if x == 0:
                spread = spread * jnp.where(gx == 0, 2.0, 1.0)
            if x == rows_x - 1:
                spread = spread * jnp.where(last_x, 2.0, 1.0)
            return spread

        for x in range(rows_x):
            for tile in range(2):
                here = slice(8 * tile, 8 * tile + 8)
                factor = time_step * inverse_mass(x, tile)
                for c in range(3):
                    force = (
                        SL[c, x, low + 8 * tile : low + 8 * tile + 8, :]
                        + SH[c, x, low + 8 * tile - 1 : low + 8 * tile + 7, :]
                    )
                    out_v[0, c, x, here, :] = V[c, x, here, :] - factor * force

        mapped = packed_map()
        link_down.wait_recv()
        reaction = RR[...]
        shared = jnp.zeros((rows_y, depth), jnp.float32)
        for by in range(-2, 3):
            source_layer = wide_layer + by
            fits = jnp.logical_and(source_layer >= 0, source_layer < 3)
            chosen = jnp.logical_and(fits, turn(mapped, by) == wide_layer)
            shared = shared + jnp.where(chosen, turn(reaction, by), 0.0)
        unclamped = lanes > 0
        for tile in range(2):
            here = slice(8 * tile, 8 * tile + 8)
            part = shared[here, :]
            for x in range(rows_x):
                factor = jnp.where(lanes >= depth - 3, time_step * inverse_mass(x, tile), 0.0)
                for c in range(3):
                    place = 3 * (rows_x * c + x)
                    moved = turn(part, place + 3 - depth)
                    speed = jnp.where(unclamped, out_v[0, c, x, here, :] + factor * moved, 0.0)
                    out_v[0, c, x, here, :] = speed
                    out_u[0, c, x, here, :] = jnp.where(
                        unclamped,
                        B[c, rim + x, low + 8 * tile : low + 8 * tile + 8, :] + time_step * speed,
                        0.0,
                    )

    for index in range(8):

        @pl.when(exists(*directions[index]))
        def _():
            send(field_parts, fs, fr, index).wait_send()
            send(modulus_parts, ms, mr, index).wait_send()
            if index in has_words:

                @pl.when(is_zone)
                def _():
                    send(word_parts, ws, wr, index).wait_send()

            @pl.when(is_slab)
            def _():
                send_coupled(index).wait_send()

    @pl.when(is_slab)
    def _():
        send_coupled(8).wait_send()

    @pl.when(is_zone)
    def _():
        link_down.wait_send()


def per_device(displacement, velocity, modulus, bond_words, coupling_map):
    _, _, rows_x, rows_y, depth = displacement.shape
    f32, i32 = jnp.float32, jnp.int32
    wide_x, wide_y = rows_x + 2 * rim, rows_y + 16
    packed = rim * rows_x
    dma = pltpu.SemaphoreType.DMA
    return pl.pallas_call(
        kernel,
        out_shape=(
            pltpu.VMEM(displacement.shape, f32),
            pltpu.VMEM(velocity.shape, f32),
        ),
        in_specs=[pl.BlockSpec(memory_space=pltpu.HBM)] * 5,
        out_specs=(pl.BlockSpec(memory_space=pltpu.VMEM),) * 2,
        scratch_shapes=[
            pltpu.VMEM((4, wide_x, wide_y, depth), f32),
            pltpu.VMEM((2, rim + rows_x, wide_y, depth), i32),
            pltpu.VMEM((3, rows_x, rows_y, depth), f32),
            pltpu.VMEM(coupling_map.shape, i32),
            pltpu.VMEM((2, 4, packed, depth), f32),
            pltpu.VMEM((2, 2, packed, depth), i32),
            pltpu.VMEM((2, 4, packed, depth), f32),
            pltpu.VMEM((2, 2, packed, depth), i32),
            pltpu.VMEM((4, 4, 8, depth), f32),
            pltpu.VMEM((2, 2, 8, depth), i32),
            pltpu.VMEM((4, 4, 8, depth), f32),
            pltpu.VMEM((2, 2, 8, depth), i32),
            pltpu.VMEM((rows_y, depth), f32),
            pltpu.VMEM((3, rows_y, depth), f32),
            pltpu.VMEM((2, 3, 8, depth), f32),
            pltpu.VMEM((rows_y, depth), f32),
            pltpu.VMEM((rows_y, depth), f32),
            pltpu.VMEM((5, 4, wide_x, wide_y, depth), f32),
            pltpu.VMEM((2, 2, rows_x, rows_y, depth), f32),
            pltpu.VMEM((4, 2, rim + rows_x, wide_y, depth), i32),
            pltpu.VMEM((rows_x, rows_y, depth), i32),
            pltpu.VMEM((len(bonds), rows_x, rows_y, depth), f32),
            pltpu.VMEM((3, rows_x, rows_y + 8, depth), f32),
            pltpu.VMEM((3, rows_x, rows_y + 8, depth), f32),
            dma((5,)), dma((8,)), dma((8,)), dma((8,)), dma((8,)), dma((8,)), dma((8,)),
            dma((9,)), dma((9,)), dma((1,)), dma((1,)),
        ],
        compiler_params=pltpu.CompilerParams(
            collective_id=0, has_side_effects=True, vmem_limit_bytes=24 * 1024 * 1024
        ),
    )(*[
        pltpu.with_memory_space_constraint(value, pltpu.HBM)
        for value in (displacement, velocity, modulus, bond_words, coupling_map)
    ])


def solution(mesh):
    return jax.shard_map(
        per_device,
        mesh=mesh,
        in_specs=(
            P("group", None, "gx", "gy", None),
            P("group", None, "gx", "gy", None),
            P("group", "gx", "gy", None),
            P(None, "gx", "gy", None),
            P(None, "gx", "gy"),
        ),
        out_specs=(P("group", None, "gx", "gy", None), P("group", None, "gx", "gy", None)),
        check_vma=False,
    )
```

```python
import math

import jax
import jax.numpy as jnp
import numpy as np
from jax import lax
from jax.experimental import pallas as pl
from jax.experimental.pallas import tpu as pltpu
from jax.sharding import PartitionSpec as P

time_step = 0.1
bond_scale = 1.0
rim = 3
low = 8
MESH = pl.DeviceIdType.MESH
directions = [(1, 0), (-1, 0), (0, 1), (0, -1), (1, 1), (1, -1), (-1, 1), (-1, -1)]
shifts = [1, -1, 2, -2]


def half_offsets():
    table = []
    for delta_x in range(-3, 4):
        for delta_y in range(-3, 4):
            for delta_z in range(-3, 4):
                radius = delta_x * delta_x + delta_y * delta_y + delta_z * delta_z
                if 0 < radius <= 9 and (delta_x, delta_y, delta_z) > (0, 0, 0):
                    table.append((delta_x, delta_y, delta_z))
    return table


def hex_stiffness():
    poisson = 0.3
    lame_first = poisson / ((1.0 + poisson) * (1.0 - 2.0 * poisson))
    shear_modulus = 0.5 / (1.0 + poisson)
    elastic = np.zeros((6, 6))
    elastic[:3, :3] = lame_first
    for axis_id in range(3):
        elastic[axis_id, axis_id] += 2.0 * shear_modulus
        elastic[3 + axis_id, 3 + axis_id] = shear_modulus
    points = [0.5 - 0.5 / math.sqrt(3.0), 0.5 + 0.5 / math.sqrt(3.0)]
    result = np.zeros((24, 24))
    shear_pairs = ((0, 1), (1, 2), (0, 2))
    for along_x in points:
        for along_y in points:
            for along_z in points:
                coords = (along_x, along_y, along_z)
                gradients = np.zeros((3, 8))
                for corner in range(8):
                    corner_bits = (corner >> 2 & 1, corner >> 1 & 1, corner & 1)
                    factors = [
                        coords[axis_id] if corner_bits[axis_id] else 1.0 - coords[axis_id]
                        for axis_id in range(3)
                    ]
                    slopes = [1.0 if corner_bits[axis_id] else -1.0 for axis_id in range(3)]
                    gradients[0, corner] = slopes[0] * factors[1] * factors[2]
                    gradients[1, corner] = factors[0] * slopes[1] * factors[2]
                    gradients[2, corner] = factors[0] * factors[1] * slopes[2]
                strain = np.zeros((6, 24))
                for axis_id in range(3):
                    strain[axis_id, axis_id * 8 : axis_id * 8 + 8] = gradients[axis_id]
                for shear_row, pair in enumerate(shear_pairs):
                    left_axis, right_axis = pair
                    strain[3 + shear_row, left_axis * 8 : left_axis * 8 + 8] = gradients[right_axis]
                    strain[3 + shear_row, right_axis * 8 : right_axis * 8 + 8] = gradients[
                        left_axis
                    ]
                result += strain.T @ elastic @ strain / 8.0
    return result


def modal_stiffness():
    one = np.array([[1.0, -1.0], [1.0, 1.0]])
    corners = np.kron(np.kron(one, one), one)
    basis = np.kron(np.eye(3), corners)
    modal = basis.T @ hex_stiffness() @ basis / 64.0
    modal[np.abs(modal) < 1e-12] = 0.0
    return modal


offsets = half_offsets()
numbers = {offset: number for number, offset in enumerate(offsets)}
sheets_of_bonds = [
    [
        (delta_y, delta_z)
        for delta_y in chosen
        for delta_z in range(-3, 4)
        if delta_y * delta_y + delta_z * delta_z <= 9
    ]
    for chosen in ((0, 3, -3), (1,), (-1,), (2,), (-2,))
]
bonds = offsets + [tuple(-delta for delta in offset) for offset in offsets]


def scaled(coefficient, value):
    return value if coefficient == 1 else coefficient * value


def combine(terms):
    total = None
    negative = None
    for coefficient, value in terms:
        if coefficient == 0:
            continue
        if coefficient < 0 and total is None:
            negative = scaled(-coefficient, value) if negative is None else (
                negative + scaled(-coefficient, value)
            )
        elif total is None:
            total = scaled(coefficient, value)
            if negative is not None:
                total = total - negative
                negative = None
        elif coefficient > 0:
            total = total + scaled(coefficient, value)
        else:
            total = total - scaled(-coefficient, value)
    if negative is not None:
        total = 0.0 - negative
    return total


def turn(value, by):
    return pltpu.roll(value, (-by) % 128, value.ndim - 1)


def kernel(
    disp, vel, mod, words, cmap,
    out_u, out_v,
    B, W, V, CM,
    YS, YSW, YR, YRW, CS, CSW, CR, CRW,
    PS, PT, PE, PX, PN, PY, RS, RR,
    R, R3, WR, WR3, K, FS, SL, SH,
    load_sem, fs, fr, ms, mr, ws, wr, cs, cr, ps, pr, link_s, link_r,
):
    group = lax.axis_index("group")
    gx = lax.axis_index("gx")
    gy = lax.axis_index("gy")
    size_x = lax.axis_size("gx")
    size_y = lax.axis_size("gy")
    is_zone = group == 0
    is_slab = group == 1
    rows_x, rows_y, depth = V.shape[1], V.shape[2], V.shape[3]
    own_x = slice(rim, rim + rows_x)
    own_y = slice(low, low + rows_y)

    def at(step_x, step_y):
        return (group, gx + step_x, gy + step_y)

    def both(first, second):
        if first is None:
            return second
        return first if second is None else jnp.logical_and(first, second)

    def exists(step_x, step_y):
        test = None
        if step_x:
            test = gx + step_x < size_x if step_x > 0 else gx > 0
        if step_y:
            test = both(test, gy + step_y < size_y if step_y > 0 else gy > 0)
        return test

    loads = [
        pltpu.make_async_copy(disp.at[0], B.at[0:3, own_x, own_y, :], load_sem.at[0]),
        pltpu.make_async_copy(mod.at[0], B.at[3, own_x, own_y, :], load_sem.at[1]),
        pltpu.make_async_copy(words, W.at[:, own_x, own_y, :], load_sem.at[2]),
        pltpu.make_async_copy(cmap, CM, load_sem.at[3]),
        pltpu.make_async_copy(vel.at[0], V, load_sem.at[4]),
    ]
    for load in loads:
        load.start()

    barrier = pltpu.get_barrier_semaphore()
    pl.semaphore_signal(barrier, inc=1, device_id=(1 - group, gx, gy), device_id_type=MESH)
    expected = jnp.int32(1)
    for step_x, step_y in directions:
        present = exists(step_x, step_y)
        expected = expected + jnp.where(is_slab, 2, 1) * present.astype(jnp.int32)

        @pl.when(present)
        def _():
            pl.semaphore_signal(
                barrier, inc=1, device_id=at(step_x, step_y), device_id_type=MESH
            )

            @pl.when(is_zone)
            def _():
                pl.semaphore_signal(
                    barrier,
                    inc=1,
                    device_id=(1 - group, gx + step_x, gy + step_y),
                    device_id_type=MESH,
                )

    def clear(ref):
        ref[...] = jnp.zeros(ref.shape, ref.dtype)

    @pl.when(gx == 0)
    def _():
        clear(B.at[:, 0:rim])
        clear(W.at[:, 0:rim])
        clear(PN.at[0])
        for side in range(2):
            clear(PY.at[side, 0])

    @pl.when(gx == size_x - 1)
    def _():
        clear(B.at[:, rim + rows_x :])
        clear(PN.at[1])
        for side in range(2):
            clear(PY.at[side, 2])

    for side, edge in ((0, gy == 0), (1, gy == size_y - 1)):

        @pl.when(edge)
        def _():
            clear(YR.at[side])
            clear(YRW.at[side])
            for index in range(3):
                clear(PY.at[side, index])

    for index, (step_x, step_y) in enumerate(directions[4:]):

        @pl.when(jnp.logical_not(exists(-step_x, -step_y)))
        def _():
            clear(CR.at[index])
            if step_x > 0:
                clear(CRW.at[index])

    for load in loads[:3]:
        load.wait()

    def rows_for(step_y):
        return slice(low + rows_y - rim, low + rows_y) if step_y > 0 else slice(low, low + rim)

    for step_y in (1, -1):
        side = 0 if step_y > 0 else 1
        for x in range(rows_x):
            for field in range(4):
                YS[side, field, rim * x : rim * x + rim, :] = B[
                    field, rim + x, rows_for(step_y), :
                ]

        @pl.when(is_zone)
        def _():
            for x in range(rows_x):
                for word in range(2):
                    YSW[side, word, rim * x : rim * x + rim, :] = W[
                        word, rim + x, rows_for(step_y), :
                    ]

    def corner_rows(step_y):
        if step_y > 0:
            return slice(low + rows_y - 2, low + rows_y)
        return slice(low, low + 2)

    def in_corner(field, count):
        first = 4 * (field % 2) + 2 * count
        return field // 2, slice(first, first + 2)

    for index, (step_x, step_y) in enumerate(directions[4:]):
        for count in range(2):
            x = rim + (rows_x - 2 + count if step_x > 0 else count)
            for field in range(4):
                tile, rows = in_corner(field, count)
                CS[index, tile, rows, :] = B[field, x, corner_rows(step_y), :]
        if step_x > 0:

            @pl.when(is_zone)
            def _():
                for count in range(2):
                    x = rim + rows_x - 2 + count
                    for word in range(2):
                        _, rows = in_corner(word, count)
                        CSW[index, rows, :] = W[word, x, corner_rows(step_y), :]

    lanes = lax.broadcasted_iota(jnp.int32, (8, depth), 1)
    wide_lanes = lax.broadcasted_iota(jnp.int32, (rows_y, depth), 1)
    wide_layer = lax.rem(wide_lanes, 3)
    loads[3].wait()

    def packed_map():
        source = lax.broadcasted_iota(jnp.int32, (3 * rows_x, depth), 0)
        target = lax.broadcasted_iota(jnp.int32, (3 * rows_x, depth), 1)
        chosen = jnp.logical_and(
            lax.div(source, rows_x) == lax.rem(target, 3),
            lax.rem(source, rows_x) == lax.rem(lax.div(target, 3), rows_x),
        )
        values = CM[...].reshape(3 * rows_x, rows_y).astype(jnp.float32)
        spread = lax.dot_general(
            values,
            chosen.astype(jnp.float32),
            (((0,), (0,)), ((), ())),
            preferred_element_type=jnp.float32,
        )
        return (spread + 0.5).astype(jnp.int32)

    @pl.when(is_slab)
    def _():
        for tile in range(2):
            rows = slice(low + 8 * tile, low + 8 * tile + 8)
            top = jnp.zeros((8, depth), jnp.float32)
            for c in range(3):
                for x in range(rows_x):
                    place = 3 * (rows_x * c + x)
                    moved = turn(B[c, rim + x, rows, :], depth - 3 - place)
                    top = jnp.where(
                        jnp.logical_and(lanes >= place, lanes < place + 3), moved, top
                    )
            RS[8 * tile : 8 * tile + 8, :] = top
        top = RS[...]
        away = packed_map() - wide_layer
        coupled = jnp.zeros((rows_y, depth), jnp.float32)
        for by in range(-2, 3):
            coupled = jnp.where(away == by, turn(top, by), coupled)
        PS[...] = coupled
        for row in range(rows_y):
            PT[row] = coupled[row : row + 1, :]
        for side, first in ((0, rows_x - rim), (1, 0)):
            kept = lax.rem(lanes, 3 * rows_x)
            kept = jnp.logical_and(kept >= 3 * first, kept < 3 * (first + rim))
            kept = jnp.logical_and(kept, lanes < 9 * rows_x)
            PE[side] = jnp.where(kept, coupled[0:8, :], pltpu.roll(coupled[8:16, :], 64, 1))

    pl.semaphore_wait(barrier, expected)

    def message(source, target, sends, recvs, index, device):
        return pltpu.make_async_remote_copy(
            src_ref=source, dst_ref=target,
            send_sem=sends.at[index], recv_sem=recvs.at[index],
            device_id=device, device_id_type=MESH,
        )

    def along_gx(ref, step_x, first, count, lead):
        source = rows_x + first if step_x > 0 else rim + first
        target = first if step_x > 0 else rim + rows_x + first
        return (
            ref.at[lead, source : source + count, own_y, :],
            ref.at[lead, target : target + count, own_y, :],
        )

    def modulus_messages(index):
        step_x, step_y = directions[index]
        if step_y == 0:
            return [(along_gx(B, step_x, 0, rim, 3), ms, mr, index)]
        side = 0 if step_y > 0 else 1
        return [((YS.at[side, 3], YR.at[side, 3]), ms, mr, index)]

    def field_messages(index):
        step_x, step_y = directions[index]
        if step_y == 0:
            near, far = (1, 0) if step_x > 0 else (0, rim - 1)
            return [
                (along_gx(B, step_x, near, 2, slice(0, 3)), fs, fr, index),
                (along_gx(B, step_x, far, 1, 0), fs, fr, 4 + index),
            ]
        side = 0 if step_y > 0 else 1
        return [((YS.at[side, 0:3], YR.at[side, 0:3]), fs, fr, index)]

    def word_messages(index):
        step_x, step_y = directions[index]
        if step_y == 0:
            return [
                (along_gx(W, step_x, 2, 1, slice(0, 2)), ws, wr, index),
                (along_gx(W, step_x, 0, 2, 1), ws, wr, 4 + index),
            ]
        side = 0 if step_y > 0 else 1
        return [((YSW.at[side], YRW.at[side]), ws, wr, index)]

    def corner_messages(index):
        return [((CS.at[index - 4], CR.at[index - 4]), cs, cr, index - 4)]

    def corner_word_messages(index):
        return [((CSW.at[index - 4], CRW.at[index - 4]), cs, cr, index)]

    def copies(messages, index):
        return [
            message(source, target, sends, recvs, spot, at(*directions[index]))
            for (source, target), sends, recvs, spot in messages(index)
        ]

    def coupled_copy(index):
        step_x, step_y = directions[index] if index < 8 else (0, 0)
        if index == 8:
            source, target = PS, PX
        elif step_y == 0:
            side = 0 if step_x > 0 else 1
            source, target = PE.at[side], PN.at[side]
        elif step_y > 0:
            source, target = PT.at[rows_y - rim : rows_y], PY.at[0, 1 - step_x]
        else:
            source, target = PT.at[0:rim], PY.at[1, 1 - step_x]
        device = (1 - group, gx + step_x, gy + step_y)
        return message(source, target, ps, pr, index, device)

    link_down = message(RS, RR, link_s, link_r, 0, (1 - group, gx, gy))
    straight, corners = (0, 1, 2, 3), (4, 5, 6, 7)
    plan = [(corner_messages, index, False) for index in corners]
    plan += [(corner_word_messages, index, True) for index in (4, 5)]
    plan += [(modulus_messages, index, False) for index in (0, 1)]
    plan += [(word_messages, 0, True)]
    plan += [(modulus_messages, index, False) for index in (2, 3)]
    plan += [(word_messages, index, True) for index in (2, 3)]
    plan += [(field_messages, index, False) for index in straight]

    def start_plan(zone):
        for messages, index, zone_only in plan:
            if zone_only and not zone:
                continue

            @pl.when(exists(*directions[index]))
            def _():
                for copy in copies(messages, index):
                    copy.start()

    @pl.when(is_slab)
    def _():
        for index in (4, 5, 6, 7, 0, 1, 8, 2, 3):
            if index == 8:
                coupled_copy(8).start()
            else:

                @pl.when(exists(*directions[index]))
                def _():
                    coupled_copy(index).start()

        start_plan(False)

    @pl.when(is_zone)
    def _():
        start_plan(True)

    loads[4].wait()

    def arrived(index):
        step_x, step_y = directions[index]
        return exists(-step_x, -step_y)

    def receive(messages, indices):
        for index in indices:

            @pl.when(arrived(index))
            def _():
                for copy in copies(messages, index):
                    copy.wait_recv()

    def unpack_rows(side):
        return slice(low - rim, low) if side == 0 else slice(low + rows_y, low + rows_y + rim)

    def unpack_sides(fields):
        for side in range(2):
            for x in range(rows_x):
                for field in fields:
                    B[field, rim + x, unpack_rows(side), :] = YR[
                        side, field, rim * x : rim * x + rim, :
                    ]

    def unpack_corners(first, last, source, target, fields):
        for index in range(first, last):
            step_x, step_y = directions[index]
            where = slice(low - 2, low) if step_y > 0 else slice(low + rows_y, low + rows_y + 2)
            for count in range(2):
                x = 1 + count if step_x > 0 else rim + rows_x + count
                for field in range(fields):
                    tile, rows = in_corner(field, count)
                    part = source[index - 4, rows, :] if fields == 2 else source[
                        index - 4, tile, rows, :
                    ]
                    target[field, x, where, :] = part

    @pl.when(is_zone)
    def _():
        tiles = [slice(8 * tile, 8 * tile + 8) for tile in range(4)]
        beside_x = (1, 2, rim + rows_x, rim + rows_x + 1)

        def turn_words(x, chosen, words_there=(0, 1)):
            for word in words_there:
                for rows in chosen:
                    value = W[word, x, rows, :]
                    for place, by in enumerate(shifts):
                        WR[place, word, x, rows, :] = turn(value, by)

        def turn_fields(x, chosen, fields):
            for field in fields:
                for rows in chosen:
                    value = B[field, x, rows, :]
                    for place, by in enumerate(shifts):
                        R[place, field, x, rows, :] = scaled(
                            by if field == 2 else 1, turn(value, by)
                        )

        def turn_own(x, carry):
            turn_words(rim + x, tiles[1:3])
            turn_fields(rim + x, tiles[1:3], range(4))
            for rows in tiles[1:3]:
                where = slice(rows.start - low, rows.stop - low)
                for spot, by in enumerate((3, -3)):
                    R3[spot, 0, x, where, :] = turn(B[3, rim + x, rows, :], by)
                    R3[spot, 1, x, where, :] = by * turn(B[2, rim + x, rows, :], by)
                WR3[x, where, :] = turn(W[0, rim + x, rows, :], -3)
            return carry

        lax.fori_loop(0, rows_x, turn_own, 0)

        receive(corner_messages, corners)
        receive(corner_word_messages, (4, 5))
        unpack_corners(4, 8, CR, B, 4)
        unpack_corners(4, 6, CRW, W, 2)
        receive(modulus_messages, straight)
        receive(word_messages, (0, 2, 3))
        unpack_sides((3,))
        for side in range(2):
            for x in range(rows_x):
                for word in range(2):
                    W[word, rim + x, unpack_rows(side), :] = YRW[
                        side, word, rim * x : rim * x + rim, :
                    ]

        def turn_beside(x, carry):
            turn_words(rim + x, (tiles[0], tiles[3]))
            turn_fields(rim + x, (tiles[0], tiles[3]), (3,))
            return carry

        lax.fori_loop(0, rows_x, turn_beside, 0)
        for x in beside_x:
            turn_fields(x, tiles, (3,))
            if x < rim:
                turn_words(x, tiles, (0, 1) if x == rim - 1 else (1,))

        group_of = 4
        blocks = sheets_of_bonds

        def factor_rows(step, carry):
            tile = lax.rem(step, 2)
            start = lax.div(step, 2) * group_of
            here = pl.ds(pl.multiple_of(8 * tile, 8), 8)

            def load_modulus(move_x, delta_y, delta_z):
                if abs(delta_z) == 3:
                    return R3[0 if delta_z > 0 else 1, 0, start + move_x, here, :]
                rows = pl.ds(low + 8 * tile + delta_y, 8)
                if delta_z == 0:
                    return B[3, start + rim + move_x, rows, :]
                return R[shifts.index(delta_z), 3, start + rim + move_x, rows, :]

            def load_word(word, move_x, delta_y, delta_z):
                if delta_z == -3:
                    return WR3[start + move_x, here, :]
                rows = pl.ds(low + 8 * tile + delta_y, 8)
                if delta_z == 0:
                    return W[word, start + rim + move_x, rows, :]
                return WR[shifts.index(delta_z), word, start + rim + move_x, rows, :]

            def block(lines):
                centre = [load_modulus(member, 0, 0) for member in range(group_of)]
                centre_words = [
                    [load_word(word, member, 0, 0) for word in range(2)]
                    for member in range(group_of)
                ]
                for delta_y, delta_z in lines:
                    reach = math.isqrt(9 - delta_y * delta_y - delta_z * delta_z)
                    for move_x in range(-reach, group_of + reach):
                        modulus_there, words_there = None, {}
                        for member in range(group_of):
                            delta = (move_x - member, delta_y, delta_z)
                            if abs(delta[0]) > reach or delta == (0, 0, 0):
                                continue
                            radius = sum(value * value for value in delta)
                            weight = 0.5 * bond_scale / float(radius) ** 1.5
                            ahead = delta > (0, 0, 0)
                            number = numbers[delta if ahead else tuple(-value for value in delta)]
                            word = number // 31
                            if modulus_there is None:
                                modulus_there = load_modulus(move_x, delta_y, delta_z)
                            if ahead:
                                flags = centre_words[member][word]
                            else:
                                if word not in words_there:
                                    words_there[word] = load_word(word, move_x, delta_y, delta_z)
                                flags = words_there[word]
                            intact = (flags & (1 << number % 31)) != 0
                            K[bonds.index(delta), start + member, here, :] = jnp.where(
                                intact, weight * (centre[member] + modulus_there), 0.0
                            )

            for lines in blocks:

                @pl.when(gx >= 0)
                def _():
                    block(lines)

            return carry

        lax.fori_loop(0, 2 * (rows_x // group_of), factor_rows, 0)

        receive(field_messages, straight)
        unpack_sides(range(3))

        def turn_around(x, carry):
            turn_fields(rim + x, (tiles[0], tiles[3]), range(3))
            return carry

        lax.fori_loop(0, rows_x, turn_around, 0)
        for x in beside_x:
            turn_fields(x, tiles, range(3))

        coupled_copy(8).wait_recv()
        for index in range(8):

            @pl.when(arrived(index))
            def _():
                coupled_copy(index).wait_recv()

        def merge(x):
            beside = 0 if x < rim else 1 if x < rim + rows_x else 2
            inner = (x - rim) % rows_x
            for tile, rows in enumerate(tiles):
                extra = 0
                if tile in (0, 3):
                    first = 8 - rim if tile == 0 else 0
                    rows = slice(rows.start + first, rows.start + first + rim)
                    side = 0 if tile == 0 else 1
                    packed = PY[side, beside, :, 0, :]
                elif beside == 1:
                    packed = PX[8 * tile - 8 : 8 * tile, :]
                else:
                    packed = PN[0 if beside == 0 else 1]
                    extra = 64 * (tile - 1)
                outer = x in (0, 2 * rim + rows_x - 1)
                if outer and tile in (0, 3):
                    continue
                lane = lanes if tile in (1, 2) else lanes[0:rim]
                for c in range(1 if outer else 3):
                    place = 3 * (rows_x * c + inner) + extra

                    def moved(by):
                        return turn(packed, place + by)

                    R[4, c, x, rows, :] = jnp.where(lane < 3, moved(0), B[c, x, rows, :])
                    if outer:
                        continue
                    for spot, by in enumerate(shifts):
                        inside = lane < 3 - by
                        if by < 0:
                            inside = jnp.logical_and(inside, lane >= -by)
                        R[spot, c, x, rows, :] = jnp.where(
                            inside, scaled(by if c == 2 else 1, moved(by)), R[spot, c, x, rows, :]
                        )
                    if c == 2 and beside == 1 and tile in (1, 2):
                        where = slice(rows.start - low, rows.stop - low)
                        inside = jnp.logical_and(lane >= 3, lane < 6)
                        R3[1, 1, inner, where, :] = jnp.where(
                            inside, -3 * moved(-3), R3[1, 1, inner, where, :]
                        )

        for x in range(2 * rim + rows_x):
            merge(x)


        def added(total, sign, value):
            if total is None:
                return value if sign > 0 else -value
            return total + value if sign > 0 else total - value

        def zone_rows(step, carry):
            tile = lax.rem(step, 2)
            start = lax.div(step, 2) * group_of
            here = pl.ds(pl.multiple_of(8 * tile, 8), 8)

            def load(field, move_x, delta_y, delta_z):
                if abs(delta_z) == 3:
                    return R3[0 if delta_z > 0 else 1, 1, start + move_x, here, :]
                first = low + 8 * tile + delta_y
                place = 4 if delta_z == 0 else shifts.index(delta_z)
                return R[place, field, start + rim + move_x, pl.ds(first, 8), :]

            def block(number, lines):
                centre = [
                    [load(c, member, 0, 0) for c in range(3)] for member in range(group_of)
                ]
                along_x = [[None] * 4 for _ in range(group_of)]
                along_z = [[None] * 4 for _ in range(group_of)]
                sheets = [{} for _ in range(group_of)]
                for delta_y, delta_z in lines:
                    reach = math.isqrt(9 - delta_y * delta_y - delta_z * delta_z)
                    base = [
                        combine([(delta_y, centre[member][1]), (delta_z, centre[member][2])])
                        for member in range(group_of)
                    ]
                    line = [None] * group_of
                    for move_x in range(-reach, group_of + reach):
                        members = [
                            member
                            for member in range(group_of)
                            if abs(move_x - member) <= reach
                            and (move_x - member, delta_y, delta_z) != (0, 0, 0)
                        ]
                        if not members:
                            continue
                        if any(move_x != member for member in members):
                            away = load(0, move_x, delta_y, delta_z)
                        side = combine(
                            [
                                (delta_y, load(1, move_x, delta_y, delta_z) if delta_y else None),
                                (
                                    1 if delta_z else 0,
                                    load(2, move_x, delta_y, delta_z) if delta_z else None,
                                ),
                            ]
                        )
                        for member in members:
                            delta_x = move_x - member
                            stretch = None
                            if side is not None:
                                stretch = side - base[member]
                            if delta_x:
                                gap = away - centre[member][0]
                                if stretch is None:
                                    stretch = scaled(delta_x, gap)
                                elif abs(delta_x) == 1:
                                    stretch = added(stretch, delta_x, gap)
                                else:
                                    stretch = stretch + delta_x * gap
                            index = bonds.index((delta_x, delta_y, delta_z))
                            pull = K[index, start + member, here, :] * stretch
                            line[member] = added(line[member], 1, pull)
                            if delta_x:
                                along_x[member][abs(delta_x)] = added(
                                    along_x[member][abs(delta_x)], delta_x, pull
                                )
                    for member in range(group_of):
                        if delta_y:
                            sheets[member][delta_y] = added(
                                sheets[member].get(delta_y), 1, line[member]
                            )
                        if delta_z:
                            along_z[member][abs(delta_z)] = added(
                                along_z[member][abs(delta_z)], delta_z, line[member]
                            )
                for member in range(group_of):
                    part = [
                        combine([(size, along_x[member][size]) for size in (1, 2, 3)
                                 if along_x[member][size] is not None]),
                        combine(list(sheets[member].items())),
                        combine([(size, along_z[member][size]) for size in (1, 2, 3)
                                 if along_z[member][size] is not None]),
                    ]
                    for c in range(3):
                        if part[c] is None:
                            part[c] = jnp.zeros((8, depth), jnp.float32)
                        if number:
                            part[c] = part[c] + FS[c, start + member, here, :]
                        FS[c, start + member, here, :] = part[c]

            for number, lines in enumerate(blocks):

                @pl.when(gx >= 0)
                def _():
                    block(number, lines)

            return carry

        lax.fori_loop(0, 2 * (rows_x // group_of), zone_rows, 0)

        moving = lanes >= 3
        for tile in range(2):
            here = slice(8 * tile, 8 * tile + 8)
            packed = jnp.zeros((8, depth), jnp.float32)
            for x in range(rows_x):
                for c in range(3):
                    place = 3 * (rows_x * c + x)
                    moved = pltpu.roll(FS[c, x, here, :], place, 1)
                    packed = jnp.where(
                        jnp.logical_and(lanes >= place, lanes < place + 3), moved, packed
                    )
            RS[here, :] = packed
        link_down.start()
        for x in range(rows_x):
            for tile in range(2):
                here = slice(8 * tile, 8 * tile + 8)
                for c in range(3):
                    old = V[c, x, here, :]
                    place = R[4, c, rim + x, low + 8 * tile : low + 8 * tile + 8, :]
                    speed = jnp.where(moving, old + time_step * FS[c, x, here, :], old)
                    out_v[0, c, x, here, :] = speed
                    out_u[0, c, x, here, :] = jnp.where(moving, place + time_step * speed, place)

    @pl.when(is_slab)
    def _():
        receive(corner_messages, corners)
        receive(modulus_messages, straight)
        receive(field_messages, straight)
        unpack_corners(4, 8, CR, B, 4)
        unpack_sides(range(4))
        modal = modal_stiffness()
        last_x = gx == size_x - 1
        last_y = gy == size_y - 1
        row_ids = lax.broadcasted_iota(jnp.int32, (8, depth), 0)
        for tile in range(3):
            rows = slice(8 * tile, 8 * tile + 8)
            next_rows = slice(8 * tile + 1, 8 * tile + 9)
            solid = lanes < depth - 1
            if tile == 2:
                solid = jnp.logical_and(
                    solid, jnp.logical_or(row_ids < 7, jnp.logical_not(last_y))
                )

            def nodes(x):
                result = []
                for c in range(3):
                    here, there = B[c, x, rows, :], B[c, x, next_rows, :]
                    for value in (here + there, there - here):
                        above = turn(value, 1)
                        result += [value + above, above - value]
                return result

            below = nodes(rim - 1)
            carried = None
            for element in range(rows_x + 1):
                above = nodes(rim + element)
                modes = {}
                for c in range(3):
                    for pair in range(4):
                        first, second = below[4 * c + pair], above[4 * c + pair]
                        if pair:
                            modes[8 * c + pair] = first + second
                        modes[8 * c + 4 + pair] = second - first
                below = above
                inside = solid
                if element == rows_x:
                    inside = jnp.logical_and(inside, jnp.logical_not(last_x))
                stiff = jnp.where(inside, B[3, rim - 1 + element, rows, :], 0.0)
                loads_of = {}
                for i in range(24):
                    total = None
                    for j in range(24):
                        if modal[i, j]:
                            term = float(modal[i, j]) * modes[j]
                            total = term if total is None else total + term
                    if total is not None:
                        loads_of[i] = total * stiff
                lows, highs = [], []
                for c in range(3):
                    for pair in range(4):
                        flat, steep = loads_of.get(8 * c + pair), loads_of[8 * c + 4 + pair]
                        lows.append(-steep if flat is None else flat - steep)
                        highs.append(steep if flat is None else flat + steep)
                if element:
                    for c in range(3):
                        halves = []
                        for pair in range(2):
                            flat = lows[4 * c + 2 * pair] + carried[4 * c + 2 * pair]
                            steep = lows[4 * c + 2 * pair + 1] + carried[4 * c + 2 * pair + 1]
                            halves.append((flat - steep) + turn(flat + steep, -1))
                        SL[c, element - 1, rows, :] = halves[0] - halves[1]
                        SH[c, element - 1, rows, :] = halves[0] + halves[1]
                carried = highs

        def inverse_mass(x, tile):
            spread = jnp.where(jnp.logical_or(lanes == 0, lanes == depth - 1), 2.0, 1.0)
            ends_y = jnp.logical_or(
                jnp.logical_and(gy == 0, row_ids + 8 * tile == 0),
                jnp.logical_and(last_y, row_ids + 8 * tile == rows_y - 1),
            )
            spread = spread * jnp.where(ends_y, 2.0, 1.0)
            if x == 0:
                spread = spread * jnp.where(gx == 0, 2.0, 1.0)
            if x == rows_x - 1:
                spread = spread * jnp.where(last_x, 2.0, 1.0)
            return spread

        for x in range(rows_x):
            for tile in range(2):
                here = slice(8 * tile, 8 * tile + 8)
                factor = time_step * inverse_mass(x, tile)
                for c in range(3):
                    force = (
                        SL[c, x, low + 8 * tile : low + 8 * tile + 8, :]
                        + SH[c, x, low + 8 * tile - 1 : low + 8 * tile + 7, :]
                    )
                    out_v[0, c, x, here, :] = V[c, x, here, :] - factor * force

        mapped = packed_map()
        link_down.wait_recv()
        reaction = RR[...]
        shared = jnp.zeros((rows_y, depth), jnp.float32)
        for by in range(-2, 3):
            source_layer = wide_layer + by
            fits = jnp.logical_and(source_layer >= 0, source_layer < 3)
            chosen = jnp.logical_and(fits, turn(mapped, by) == wide_layer)
            shared = shared + jnp.where(chosen, turn(reaction, by), 0.0)
        unclamped = lanes > 0
        for tile in range(2):
            here = slice(8 * tile, 8 * tile + 8)
            part = shared[here, :]
            for x in range(rows_x):
                factor = jnp.where(lanes >= depth - 3, time_step * inverse_mass(x, tile), 0.0)
                for c in range(3):
                    place = 3 * (rows_x * c + x)
                    moved = turn(part, place + 3 - depth)
                    speed = jnp.where(unclamped, out_v[0, c, x, here, :] + factor * moved, 0.0)
                    out_v[0, c, x, here, :] = speed
                    out_u[0, c, x, here, :] = jnp.where(
                        unclamped,
                        B[c, rim + x, low + 8 * tile : low + 8 * tile + 8, :] + time_step * speed,
                        0.0,
                    )

    def end_plan(zone):
        for messages, index, zone_only in plan:
            if zone_only and not zone:
                continue

            @pl.when(exists(*directions[index]))
            def _():
                for copy in copies(messages, index):
                    copy.wait_send()

    @pl.when(is_slab)
    def _():
        for index in range(8):

            @pl.when(exists(*directions[index]))
            def _():
                coupled_copy(index).wait_send()

        coupled_copy(8).wait_send()
        end_plan(False)

    @pl.when(is_zone)
    def _():
        end_plan(True)
        link_down.wait_send()


def store(first_in, second_in, first_out, second_out, sem):
    copies = [
        pltpu.make_async_copy(first_in, first_out, sem.at[0]),
        pltpu.make_async_copy(second_in, second_out, sem.at[1]),
    ]
    for copy in copies:
        copy.start()
    for copy in copies:
        copy.wait()


def per_device(displacement, velocity, modulus, bond_words, coupling_map):
    _, _, rows_x, rows_y, depth = displacement.shape
    f32, i32 = jnp.float32, jnp.int32
    wide_x, wide_y = rows_x + 2 * rim, rows_y + 16
    packed = rim * rows_x
    dma = pltpu.SemaphoreType.DMA
    field, speed = pl.pallas_call(
        kernel,
        out_shape=(
            pltpu.VMEM(displacement.shape, f32),
            pltpu.VMEM(velocity.shape, f32),
        ),
        in_specs=[pl.BlockSpec(memory_space=pltpu.HBM)] * 5,
        out_specs=(pl.BlockSpec(memory_space=pltpu.VMEM),) * 2,
        scratch_shapes=[
            pltpu.VMEM((4, wide_x, wide_y, depth), f32),
            pltpu.VMEM((2, rim + rows_x, wide_y, depth), i32),
            pltpu.VMEM((3, rows_x, rows_y, depth), f32),
            pltpu.VMEM(coupling_map.shape, i32),
            pltpu.VMEM((2, 4, packed, depth), f32),
            pltpu.VMEM((2, 2, packed, depth), i32),
            pltpu.VMEM((2, 4, packed, depth), f32),
            pltpu.VMEM((2, 2, packed, depth), i32),
            pltpu.VMEM((4, 2, 8, depth), f32),
            pltpu.VMEM((2, 8, depth), i32),
            pltpu.VMEM((4, 2, 8, depth), f32),
            pltpu.VMEM((2, 8, depth), i32),
            pltpu.VMEM((rows_y, depth), f32),
            pltpu.VMEM((rows_y, 1, depth), f32),
            pltpu.VMEM((2, 8, depth), f32),
            pltpu.VMEM((rows_y, depth), f32),
            pltpu.VMEM((2, 8, depth), f32),
            pltpu.VMEM((2, 3, rim, 1, depth), f32),
            pltpu.VMEM((rows_y, depth), f32),
            pltpu.VMEM((rows_y, depth), f32),
            pltpu.VMEM((5, 4, wide_x, wide_y, depth), f32),
            pltpu.VMEM((2, 2, rows_x, rows_y, depth), f32),
            pltpu.VMEM((4, 2, rim + rows_x, wide_y, depth), i32),
            pltpu.VMEM((rows_x, rows_y, depth), i32),
            pltpu.VMEM((len(bonds), rows_x, rows_y, depth), f32),
            pltpu.VMEM((3, rows_x, rows_y, depth), f32),
            pltpu.VMEM((3, rows_x, rows_y + 8, depth), f32),
            pltpu.VMEM((3, rows_x, rows_y + 8, depth), f32),
            dma((5,)), dma((6,)), dma((6,)), dma((4,)), dma((4,)), dma((6,)), dma((6,)),
            dma((6,)), dma((6,)), dma((9,)), dma((9,)), dma((1,)), dma((1,)),
        ],
        compiler_params=pltpu.CompilerParams(
            collective_id=0, has_side_effects=True, vmem_limit_bytes=24 * 1024 * 1024
        ),
    )(*[
        pltpu.with_memory_space_constraint(value, pltpu.HBM)
        for value in (displacement, velocity, modulus, bond_words, coupling_map)
    ])
    return pl.pallas_call(
        store,
        out_shape=(
            jax.ShapeDtypeStruct(displacement.shape, f32),
            jax.ShapeDtypeStruct(velocity.shape, f32),
        ),
        in_specs=[pl.BlockSpec(memory_space=pltpu.VMEM)] * 2,
        out_specs=(pl.BlockSpec(memory_space=pltpu.HBM),) * 2,
        scratch_shapes=[dma((2,))],
    )(*[pltpu.with_memory_space_constraint(value, pltpu.VMEM) for value in (field, speed)])


def solution(mesh):
    return jax.shard_map(
        per_device,
        mesh=mesh,
        in_specs=(
            P("group", None, "gx", "gy", None),
            P("group", None, "gx", "gy", None),
            P("group", "gx", "gy", None),
            P(None, "gx", "gy", None),
            P(None, "gx", "gy"),
        ),
        out_specs=(P("group", None, "gx", "gy", None), P("group", None, "gx", "gy", None)),
        check_vma=False,
    )
```

```python
import math

import jax
import jax.numpy as jnp
import numpy as np
from jax import lax
from jax.experimental import pallas as pl
from jax.experimental.pallas import tpu as pltpu
from jax.sharding import PartitionSpec as P

time_step = 0.1
bond_scale = 1.0
rim = 3
low = 8
MESH = pl.DeviceIdType.MESH
directions = [(1, 0), (-1, 0), (0, 1), (0, -1), (1, 1), (1, -1), (-1, 1), (-1, -1)]
shifts = [1, -1, 2, -2]


def half_offsets():
    table = []
    for delta_x in range(-3, 4):
        for delta_y in range(-3, 4):
            for delta_z in range(-3, 4):
                radius = delta_x * delta_x + delta_y * delta_y + delta_z * delta_z
                if 0 < radius <= 9 and (delta_x, delta_y, delta_z) > (0, 0, 0):
                    table.append((delta_x, delta_y, delta_z))
    return table


def hex_stiffness():
    poisson = 0.3
    lame_first = poisson / ((1.0 + poisson) * (1.0 - 2.0 * poisson))
    shear_modulus = 0.5 / (1.0 + poisson)
    elastic = np.zeros((6, 6))
    elastic[:3, :3] = lame_first
    for axis_id in range(3):
        elastic[axis_id, axis_id] += 2.0 * shear_modulus
        elastic[3 + axis_id, 3 + axis_id] = shear_modulus
    points = [0.5 - 0.5 / math.sqrt(3.0), 0.5 + 0.5 / math.sqrt(3.0)]
    result = np.zeros((24, 24))
    shear_pairs = ((0, 1), (1, 2), (0, 2))
    for along_x in points:
        for along_y in points:
            for along_z in points:
                coords = (along_x, along_y, along_z)
                gradients = np.zeros((3, 8))
                for corner in range(8):
                    corner_bits = (corner >> 2 & 1, corner >> 1 & 1, corner & 1)
                    factors = [
                        coords[axis_id] if corner_bits[axis_id] else 1.0 - coords[axis_id]
                        for axis_id in range(3)
                    ]
                    slopes = [1.0 if corner_bits[axis_id] else -1.0 for axis_id in range(3)]
                    gradients[0, corner] = slopes[0] * factors[1] * factors[2]
                    gradients[1, corner] = factors[0] * slopes[1] * factors[2]
                    gradients[2, corner] = factors[0] * factors[1] * slopes[2]
                strain = np.zeros((6, 24))
                for axis_id in range(3):
                    strain[axis_id, axis_id * 8 : axis_id * 8 + 8] = gradients[axis_id]
                for shear_row, pair in enumerate(shear_pairs):
                    left_axis, right_axis = pair
                    strain[3 + shear_row, left_axis * 8 : left_axis * 8 + 8] = gradients[right_axis]
                    strain[3 + shear_row, right_axis * 8 : right_axis * 8 + 8] = gradients[
                        left_axis
                    ]
                result += strain.T @ elastic @ strain / 8.0
    return result


def modal_stiffness():
    one = np.array([[1.0, -1.0], [1.0, 1.0]])
    corners = np.kron(np.kron(one, one), one)
    basis = np.kron(np.eye(3), corners)
    modal = basis.T @ hex_stiffness() @ basis / 64.0
    modal[np.abs(modal) < 1e-12] = 0.0
    return modal


offsets = half_offsets()
numbers = {offset: number for number, offset in enumerate(offsets)}
sheets_of_bonds = [
    [
        (delta_y, delta_z)
        for delta_y in chosen
        for delta_z in range(-3, 4)
        if delta_y * delta_y + delta_z * delta_z <= 9
    ]
    for chosen in ((0, 3, -3), (1,), (-1,), (2,), (-2,))
]
bonds = offsets + [tuple(-delta for delta in offset) for offset in offsets]


def scaled(coefficient, value):
    return value if coefficient == 1 else coefficient * value


def combine(terms):
    total = None
    negative = None
    for coefficient, value in terms:
        if coefficient == 0:
            continue
        if coefficient < 0 and total is None:
            negative = scaled(-coefficient, value) if negative is None else (
                negative + scaled(-coefficient, value)
            )
        elif total is None:
            total = scaled(coefficient, value)
            if negative is not None:
                total = total - negative
                negative = None
        elif coefficient > 0:
            total = total + scaled(coefficient, value)
        else:
            total = total - scaled(-coefficient, value)
    if negative is not None:
        total = 0.0 - negative
    return total


def turn(value, by):
    return pltpu.roll(value, (-by) % 128, value.ndim - 1)


def kernel(
    disp, vel, mod, words, cmap,
    out_u, out_v,
    B, W, V, CM,
    YS, YSW, YR, YRW, CS, CSW, CR, CRW,
    PS, PT, PE, PX, PN, PY, RS, RR,
    R, R3, WR, WR3, K, FS, SL, SH,
    load_sem, fs, fr, ms, mr, ws, wr, cs, cr, ps, pr, link_s, link_r,
):
    group = lax.axis_index("group")
    gx = lax.axis_index("gx")
    gy = lax.axis_index("gy")
    size_x = lax.axis_size("gx")
    size_y = lax.axis_size("gy")
    is_zone = group == 0
    is_slab = group == 1
    rows_x, rows_y, depth = V.shape[1], V.shape[2], V.shape[3]
    own_x = slice(rim, rim + rows_x)
    own_y = slice(low, low + rows_y)

    def at(step_x, step_y):
        return (group, gx + step_x, gy + step_y)

    def both(first, second):
        if first is None:
            return second
        return first if second is None else jnp.logical_and(first, second)

    def exists(step_x, step_y):
        test = None
        if step_x:
            test = gx + step_x < size_x if step_x > 0 else gx > 0
        if step_y:
            test = both(test, gy + step_y < size_y if step_y > 0 else gy > 0)
        return test

    loads = [
        pltpu.make_async_copy(disp.at[0], B.at[0:3, own_x, own_y, :], load_sem.at[0]),
        pltpu.make_async_copy(mod.at[0], B.at[3, own_x, own_y, :], load_sem.at[1]),
        pltpu.make_async_copy(words, W.at[:, own_x, own_y, :], load_sem.at[2]),
        pltpu.make_async_copy(cmap, CM, load_sem.at[3]),
        pltpu.make_async_copy(vel.at[0], V, load_sem.at[4]),
    ]
    for load in loads:
        load.start()

    barrier = pltpu.get_barrier_semaphore()
    pl.semaphore_signal(barrier, inc=1, device_id=(1 - group, gx, gy), device_id_type=MESH)
    expected = jnp.int32(1)
    for step_x, step_y in directions:
        present = exists(step_x, step_y)
        expected = expected + jnp.where(is_slab, 2, 1) * present.astype(jnp.int32)

        @pl.when(present)
        def _():
            pl.semaphore_signal(
                barrier, inc=1, device_id=at(step_x, step_y), device_id_type=MESH
            )

            @pl.when(is_zone)
            def _():
                pl.semaphore_signal(
                    barrier,
                    inc=1,
                    device_id=(1 - group, gx + step_x, gy + step_y),
                    device_id_type=MESH,
                )

    def clear(ref):
        ref[...] = jnp.zeros(ref.shape, ref.dtype)

    @pl.when(gx == 0)
    def _():
        clear(B.at[:, 0:rim])
        clear(W.at[:, 0:rim])
        clear(PN.at[0])
        for side in range(2):
            clear(PY.at[side, 0])

    @pl.when(gx == size_x - 1)
    def _():
        clear(B.at[:, rim + rows_x :])
        clear(PN.at[1])
        for side in range(2):
            clear(PY.at[side, 2])

    for side, edge in ((0, gy == 0), (1, gy == size_y - 1)):

        @pl.when(edge)
        def _():
            clear(YR.at[side])
            clear(YRW.at[side])
            for index in range(3):
                clear(PY.at[side, index])

    for index, (step_x, step_y) in enumerate(directions[4:]):

        @pl.when(jnp.logical_not(exists(-step_x, -step_y)))
        def _():
            clear(CR.at[index])
            if step_x > 0:
                clear(CRW.at[index])

    for load in loads[:3]:
        load.wait()

    def rows_for(step_y):
        return slice(low + rows_y - rim, low + rows_y) if step_y > 0 else slice(low, low + rim)

    for step_y in (1, -1):
        side = 0 if step_y > 0 else 1
        for x in range(rows_x):
            for field in range(4):
                YS[side, field, rim * x : rim * x + rim, :] = B[
                    field, rim + x, rows_for(step_y), :
                ]

        @pl.when(is_zone)
        def _():
            for x in range(rows_x):
                for word in range(2):
                    YSW[side, word, rim * x : rim * x + rim, :] = W[
                        word, rim + x, rows_for(step_y), :
                    ]

    def corner_rows(step_y):
        if step_y > 0:
            return slice(low + rows_y - 2, low + rows_y)
        return slice(low, low + 2)

    def in_corner(field, count):
        first = 4 * (field % 2) + 2 * count
        return field // 2, slice(first, first + 2)

    for index, (step_x, step_y) in enumerate(directions[4:]):
        for count in range(2):
            x = rim + (rows_x - 2 + count if step_x > 0 else count)
            for field in range(4):
                tile, rows = in_corner(field, count)
                CS[index, tile, rows, :] = B[field, x, corner_rows(step_y), :]
        if step_x > 0:

            @pl.when(is_zone)
            def _():
                for count in range(2):
                    x = rim + rows_x - 2 + count
                    for word in range(2):
                        _, rows = in_corner(word, count)
                        CSW[index, rows, :] = W[word, x, corner_rows(step_y), :]

    lanes = lax.broadcasted_iota(jnp.int32, (8, depth), 1)
    wide_lanes = lax.broadcasted_iota(jnp.int32, (rows_y, depth), 1)
    wide_layer = lax.rem(wide_lanes, 3)
    loads[3].wait()

    def packed_map():
        source = lax.broadcasted_iota(jnp.int32, (3 * rows_x, depth), 0)
        target = lax.broadcasted_iota(jnp.int32, (3 * rows_x, depth), 1)
        chosen = jnp.logical_and(
            lax.div(source, rows_x) == lax.rem(target, 3),
            lax.rem(source, rows_x) == lax.rem(lax.div(target, 3), rows_x),
        )
        values = CM[...].reshape(3 * rows_x, rows_y).astype(jnp.float32)
        spread = lax.dot_general(
            values,
            chosen.astype(jnp.float32),
            (((0,), (0,)), ((), ())),
            preferred_element_type=jnp.float32,
        )
        return (spread + 0.5).astype(jnp.int32)

    @pl.when(is_slab)
    def _():
        for tile in range(2):
            rows = slice(low + 8 * tile, low + 8 * tile + 8)
            top = jnp.zeros((8, depth), jnp.float32)
            for c in range(3):
                for x in range(rows_x):
                    place = 3 * (rows_x * c + x)
                    moved = turn(B[c, rim + x, rows, :], depth - 3 - place)
                    top = jnp.where(
                        jnp.logical_and(lanes >= place, lanes < place + 3), moved, top
                    )
            RS[8 * tile : 8 * tile + 8, :] = top
        top = RS[...]
        away = packed_map() - wide_layer
        coupled = jnp.zeros((rows_y, depth), jnp.float32)
        for by in range(-2, 3):
            coupled = jnp.where(away == by, turn(top, by), coupled)
        PS[...] = coupled
        for row in range(rows_y):
            PT[row] = coupled[row : row + 1, :]
        for side, first in ((0, rows_x - rim), (1, 0)):
            kept = lax.rem(lanes, 3 * rows_x)
            kept = jnp.logical_and(kept >= 3 * first, kept < 3 * (first + rim))
            kept = jnp.logical_and(kept, lanes < 9 * rows_x)
            PE[side] = jnp.where(kept, coupled[0:8, :], pltpu.roll(coupled[8:16, :], 64, 1))

    pl.semaphore_wait(barrier, expected)

    def message(source, target, sends, recvs, index, device):
        return pltpu.make_async_remote_copy(
            src_ref=source, dst_ref=target,
            send_sem=sends.at[index], recv_sem=recvs.at[index],
            device_id=device, device_id_type=MESH,
        )

    def along_gx(ref, step_x, first, count, lead):
        source = rows_x + first if step_x > 0 else rim + first
        target = first if step_x > 0 else rim + rows_x + first
        return (
            ref.at[lead, source : source + count, own_y, :],
            ref.at[lead, target : target + count, own_y, :],
        )

    def modulus_messages(index):
        step_x, step_y = directions[index]
        if step_y == 0:
            return [(along_gx(B, step_x, 0, rim, 3), ms, mr, index)]
        side = 0 if step_y > 0 else 1
        return [((YS.at[side, 3], YR.at[side, 3]), ms, mr, index)]

    def field_messages(index):
        step_x, step_y = directions[index]
        if step_y == 0:
            near, far = (1, 0) if step_x > 0 else (0, rim - 1)
            return [
                (along_gx(B, step_x, near, 2, slice(0, 3)), fs, fr, index),
                (along_gx(B, step_x, far, 1, 0), fs, fr, 4 + index),
            ]
        side = 0 if step_y > 0 else 1
        return [((YS.at[side, 0:3], YR.at[side, 0:3]), fs, fr, index)]

    def word_messages(index):
        step_x, step_y = directions[index]
        if step_y == 0:
            return [
                (along_gx(W, step_x, 2, 1, slice(0, 2)), ws, wr, index),
                (along_gx(W, step_x, 0, 2, 1), ws, wr, 4 + index),
            ]
        side = 0 if step_y > 0 else 1
        return [((YSW.at[side], YRW.at[side]), ws, wr, index)]

    def corner_messages(index):
        return [((CS.at[index - 4], CR.at[index - 4]), cs, cr, index - 4)]

    def corner_word_messages(index):
        return [((CSW.at[index - 4], CRW.at[index - 4]), cs, cr, index)]

    def copies(messages, index):
        return [
            message(source, target, sends, recvs, spot, at(*directions[index]))
            for (source, target), sends, recvs, spot in messages(index)
        ]

    def coupled_copy(index):
        step_x, step_y = directions[index] if index < 8 else (0, 0)
        if index == 8:
            source, target = PS, PX
        elif step_y == 0:
            side = 0 if step_x > 0 else 1
            source, target = PE.at[side], PN.at[side]
        elif step_y > 0:
            source, target = PT.at[rows_y - rim : rows_y], PY.at[0, 1 - step_x]
        else:
            source, target = PT.at[0:rim], PY.at[1, 1 - step_x]
        device = (1 - group, gx + step_x, gy + step_y)
        return message(source, target, ps, pr, index, device)

    link_down = message(RS, RR, link_s, link_r, 0, (1 - group, gx, gy))
    straight, corners = (0, 1, 2, 3), (4, 5, 6, 7)
    plan = [(corner_messages, index, False) for index in corners]
    plan += [(corner_word_messages, index, True) for index in (4, 5)]
    plan += [(modulus_messages, index, False) for index in (0, 1)]
    plan += [(word_messages, 0, True)]
    plan += [(modulus_messages, index, False) for index in (2, 3)]
    plan += [(word_messages, index, True) for index in (2, 3)]
    plan += [(field_messages, index, False) for index in straight]

    def start_plan(zone):
        for messages, index, zone_only in plan:
            if zone_only and not zone:
                continue

            @pl.when(exists(*directions[index]))
            def _():
                for copy in copies(messages, index):
                    copy.start()

    @pl.when(is_slab)
    def _():
        for index in (4, 5, 6, 7, 0, 1, 8, 2, 3):
            if index == 8:
                coupled_copy(8).start()
            else:

                @pl.when(exists(*directions[index]))
                def _():
                    coupled_copy(index).start()

        start_plan(False)

    @pl.when(is_zone)
    def _():
        start_plan(True)

    loads[4].wait()

    def arrived(index):
        step_x, step_y = directions[index]
        return exists(-step_x, -step_y)

    def receive(messages, indices):
        for index in indices:

            @pl.when(arrived(index))
            def _():
                for copy in copies(messages, index):
                    copy.wait_recv()

    def unpack_rows(side):
        return slice(low - rim, low) if side == 0 else slice(low + rows_y, low + rows_y + rim)

    def unpack_sides(fields):
        for side in range(2):
            for x in range(rows_x):
                for field in fields:
                    B[field, rim + x, unpack_rows(side), :] = YR[
                        side, field, rim * x : rim * x + rim, :
                    ]

    def unpack_corners(first, last, source, target, fields):
        for index in range(first, last):
            step_x, step_y = directions[index]
            where = slice(low - 2, low) if step_y > 0 else slice(low + rows_y, low + rows_y + 2)
            for count in range(2):
                x = 1 + count if step_x > 0 else rim + rows_x + count
                for field in range(fields):
                    tile, rows = in_corner(field, count)
                    part = source[index - 4, rows, :] if fields == 2 else source[
                        index - 4, tile, rows, :
                    ]
                    target[field, x, where, :] = part

    @pl.when(is_zone)
    def _():
        tiles = [slice(8 * tile, 8 * tile + 8) for tile in range(4)]
        beside_x = (1, 2, rim + rows_x, rim + rows_x + 1)

        def turn_words(x, chosen, words_there=(0, 1)):
            for word in words_there:
                for rows in chosen:
                    value = W[word, x, rows, :]
                    for place, by in enumerate(shifts):
                        WR[place, word, x, rows, :] = turn(value, by)

        def turn_fields(x, chosen, fields):
            for field in fields:
                for rows in chosen:
                    value = B[field, x, rows, :]
                    for place, by in enumerate(shifts):
                        R[place, field, x, rows, :] = scaled(
                            by if field == 2 else 1, turn(value, by)
                        )

        def turn_own(x, carry):
            turn_words(rim + x, tiles[1:3])
            turn_fields(rim + x, tiles[1:3], range(4))
            for rows in tiles[1:3]:
                where = slice(rows.start - low, rows.stop - low)
                for spot, by in enumerate((3, -3)):
                    R3[spot, 0, x, where, :] = turn(B[3, rim + x, rows, :], by)
                    R3[spot, 1, x, where, :] = by * turn(B[2, rim + x, rows, :], by)
                WR3[x, where, :] = turn(W[0, rim + x, rows, :], -3)
            return carry

        lax.fori_loop(0, rows_x, turn_own, 0)

        group_of = 4
        blocks = sheets_of_bonds

        def factor_rows(start, tile, part):
            here = slice(8 * tile, 8 * tile + 8)

            def load_modulus(move_x, delta_y, delta_z):
                if abs(delta_z) == 3:
                    return R3[0 if delta_z > 0 else 1, 0, start + move_x, here, :]
                rows = slice(low + 8 * tile + delta_y, low + 8 * tile + delta_y + 8)
                if delta_z == 0:
                    return B[3, start + rim + move_x, rows, :]
                return R[shifts.index(delta_z), 3, start + rim + move_x, rows, :]

            def load_word(word, move_x, delta_y, delta_z):
                if delta_z == -3:
                    return WR3[start + move_x, here, :]
                rows = slice(low + 8 * tile + delta_y, low + 8 * tile + delta_y + 8)
                if delta_z == 0:
                    return W[word, start + rim + move_x, rows, :]
                return WR[shifts.index(delta_z), word, start + rim + move_x, rows, :]

            def block(lines):
                centre = [load_modulus(member, 0, 0) for member in range(group_of)]
                centre_words = [
                    [load_word(word, member, 0, 0) for word in range(2)]
                    for member in range(group_of)
                ]
                for delta_y, delta_z in lines:
                    reach = math.isqrt(9 - delta_y * delta_y - delta_z * delta_z)
                    for move_x in range(-reach, group_of + reach):
                        modulus_there, words_there = None, {}
                        for member in range(group_of):
                            delta = (move_x - member, delta_y, delta_z)
                            if abs(delta[0]) > reach or delta == (0, 0, 0):
                                continue
                            beyond_x = not 0 <= start + move_x < rows_x
                            beyond_y = delta_y < 0 if tile == 0 else delta_y > 0
                            if part != (2 if beyond_x else 1 if beyond_y else 0):
                                continue
                            radius = sum(value * value for value in delta)
                            weight = 0.5 * bond_scale / float(radius) ** 1.5
                            ahead = delta > (0, 0, 0)
                            number = numbers[delta if ahead else tuple(-value for value in delta)]
                            word = number // 31
                            if modulus_there is None:
                                modulus_there = load_modulus(move_x, delta_y, delta_z)
                            if ahead:
                                flags = centre_words[member][word]
                            else:
                                if word not in words_there:
                                    words_there[word] = load_word(word, move_x, delta_y, delta_z)
                                flags = words_there[word]
                            intact = (flags & (1 << number % 31)) != 0
                            K[bonds.index(delta), start + member, here, :] = jnp.where(
                                intact, weight * (centre[member] + modulus_there), 0.0
                            )

            for lines in blocks:

                @pl.when(gx >= 0)
                def _():
                    block(lines)

        def factors(part):
            for start in range(0, rows_x, group_of):
                for tile in range(2):
                    factor_rows(start, tile, part)

        factors(0)

        receive(modulus_messages, (2, 3))
        receive(word_messages, (2, 3))
        unpack_sides((3,))
        for side in range(2):
            for x in range(rows_x):
                for word in range(2):
                    W[word, rim + x, unpack_rows(side), :] = YRW[
                        side, word, rim * x : rim * x + rim, :
                    ]

        def turn_beside(x, carry):
            turn_words(rim + x, (tiles[0], tiles[3]))
            turn_fields(rim + x, (tiles[0], tiles[3]), (3,))
            return carry

        lax.fori_loop(0, rows_x, turn_beside, 0)
        factors(1)

        receive(corner_messages, corners)
        receive(corner_word_messages, (4, 5))
        unpack_corners(4, 8, CR, B, 4)
        unpack_corners(4, 6, CRW, W, 2)
        receive(modulus_messages, (0, 1))
        receive(word_messages, (0,))
        for x in beside_x:
            turn_fields(x, tiles, (3,))
            if x < rim:
                turn_words(x, tiles, (0, 1) if x == rim - 1 else (1,))
        factors(2)

        receive(field_messages, straight)
        unpack_sides(range(3))

        def turn_around(x, carry):
            turn_fields(rim + x, (tiles[0], tiles[3]), range(3))
            return carry

        lax.fori_loop(0, rows_x, turn_around, 0)
        for x in beside_x:
            turn_fields(x, tiles, range(3))

        def merge(x, chosen):
            beside = 0 if x < rim else 1 if x < rim + rows_x else 2
            inner = (x - rim) % rows_x
            for tile in chosen:
                rows = tiles[tile]
                extra = 0
                if tile in (0, 3):
                    first = 8 - rim if tile == 0 else 0
                    rows = slice(rows.start + first, rows.start + first + rim)
                    side = 0 if tile == 0 else 1
                    packed = PY[side, beside, :, 0, :]
                elif beside == 1:
                    packed = PX[8 * tile - 8 : 8 * tile, :]
                else:
                    packed = PN[0 if beside == 0 else 1]
                    extra = 64 * (tile - 1)
                outer = x in (0, 2 * rim + rows_x - 1)
                if outer and tile in (0, 3):
                    continue
                lane = lanes if tile in (1, 2) else lanes[0:rim]
                for c in range(1 if outer else 3):
                    place = 3 * (rows_x * c + inner) + extra

                    def moved(by):
                        return turn(packed, place + by)

                    R[4, c, x, rows, :] = jnp.where(lane < 3, moved(0), B[c, x, rows, :])
                    if outer:
                        continue
                    for spot, by in enumerate(shifts):
                        inside = lane < 3 - by
                        if by < 0:
                            inside = jnp.logical_and(inside, lane >= -by)
                        R[spot, c, x, rows, :] = jnp.where(
                            inside, scaled(by if c == 2 else 1, moved(by)), R[spot, c, x, rows, :]
                        )
                    if c == 2 and beside == 1 and tile in (1, 2):
                        where = slice(rows.start - low, rows.stop - low)
                        inside = jnp.logical_and(lane >= 3, lane < 6)
                        R3[1, 1, inner, where, :] = jnp.where(
                            inside, -3 * moved(-3), R3[1, 1, inner, where, :]
                        )

        own = range(rim, rim + rows_x)
        coupled_copy(8).wait_recv()
        for x in own:
            merge(x, (1, 2))
        for indices in ((2, 3), (0, 1, 4, 5, 6, 7)):
            for index in indices:

                @pl.when(arrived(index))
                def _():
                    coupled_copy(index).wait_recv()

            for x in range(2 * rim + rows_x):
                if indices[0] == 2 and x in own:
                    merge(x, (0, 3))
                elif indices[0] == 0 and x not in own:
                    merge(x, range(4))


        def added(total, sign, value):
            if total is None:
                return value if sign > 0 else -value
            return total + value if sign > 0 else total - value

        def zone_rows(step, carry):
            tile = lax.rem(step, 2)
            start = lax.div(step, 2) * group_of
            here = pl.ds(pl.multiple_of(8 * tile, 8), 8)

            def load(field, move_x, delta_y, delta_z):
                if abs(delta_z) == 3:
                    return R3[0 if delta_z > 0 else 1, 1, start + move_x, here, :]
                first = low + 8 * tile + delta_y
                place = 4 if delta_z == 0 else shifts.index(delta_z)
                return R[place, field, start + rim + move_x, pl.ds(first, 8), :]

            def block(number, lines):
                centre = [
                    [load(c, member, 0, 0) for c in range(3)] for member in range(group_of)
                ]
                along_x = [[None] * 4 for _ in range(group_of)]
                along_z = [[None] * 4 for _ in range(group_of)]
                sheets = [{} for _ in range(group_of)]
                for delta_y, delta_z in lines:
                    reach = math.isqrt(9 - delta_y * delta_y - delta_z * delta_z)
                    base = [
                        combine([(delta_y, centre[member][1]), (delta_z, centre[member][2])])
                        for member in range(group_of)
                    ]
                    line = [None] * group_of
                    for move_x in range(-reach, group_of + reach):
                        members = [
                            member
                            for member in range(group_of)
                            if abs(move_x - member) <= reach
                            and (move_x - member, delta_y, delta_z) != (0, 0, 0)
                        ]
                        if not members:
                            continue
                        if any(move_x != member for member in members):
                            away = load(0, move_x, delta_y, delta_z)
                        side = combine(
                            [
                                (delta_y, load(1, move_x, delta_y, delta_z) if delta_y else None),
                                (
                                    1 if delta_z else 0,
                                    load(2, move_x, delta_y, delta_z) if delta_z else None,
                                ),
                            ]
                        )
                        for member in members:
                            delta_x = move_x - member
                            stretch = None
                            if side is not None:
                                stretch = side - base[member]
                            if delta_x:
                                gap = away - centre[member][0]
                                if stretch is None:
                                    stretch = scaled(delta_x, gap)
                                elif abs(delta_x) == 1:
                                    stretch = added(stretch, delta_x, gap)
                                else:
                                    stretch = stretch + delta_x * gap
                            index = bonds.index((delta_x, delta_y, delta_z))
                            pull = K[index, start + member, here, :] * stretch
                            line[member] = added(line[member], 1, pull)
                            if delta_x:
                                along_x[member][abs(delta_x)] = added(
                                    along_x[member][abs(delta_x)], delta_x, pull
                                )
                    for member in range(group_of):
                        if delta_y:
                            sheets[member][delta_y] = added(
                                sheets[member].get(delta_y), 1, line[member]
                            )
                        if delta_z:
                            along_z[member][abs(delta_z)] = added(
                                along_z[member][abs(delta_z)], delta_z, line[member]
                            )
                for member in range(group_of):
                    part = [
                        combine([(size, along_x[member][size]) for size in (1, 2, 3)
                                 if along_x[member][size] is not None]),
                        combine(list(sheets[member].items())),
                        combine([(size, along_z[member][size]) for size in (1, 2, 3)
                                 if along_z[member][size] is not None]),
                    ]
                    for c in range(3):
                        if part[c] is None:
                            part[c] = jnp.zeros((8, depth), jnp.float32)
                        if number:
                            part[c] = part[c] + FS[c, start + member, here, :]
                        FS[c, start + member, here, :] = part[c]

            for number, lines in enumerate(blocks):

                @pl.when(gx >= 0)
                def _():
                    block(number, lines)

            return carry

        lax.fori_loop(0, 2 * (rows_x // group_of), zone_rows, 0)

        moving = lanes >= 3
        for tile in range(2):
            here = slice(8 * tile, 8 * tile + 8)
            packed = jnp.zeros((8, depth), jnp.float32)
            for x in range(rows_x):
                for c in range(3):
                    place = 3 * (rows_x * c + x)
                    moved = pltpu.roll(FS[c, x, here, :], place, 1)
                    packed = jnp.where(
                        jnp.logical_and(lanes >= place, lanes < place + 3), moved, packed
                    )
            RS[here, :] = packed
        link_down.start()
        for x in range(rows_x):
            for tile in range(2):
                here = slice(8 * tile, 8 * tile + 8)
                for c in range(3):
                    old = V[c, x, here, :]
                    place = R[4, c, rim + x, low + 8 * tile : low + 8 * tile + 8, :]
                    speed = jnp.where(moving, old + time_step * FS[c, x, here, :], old)
                    out_v[0, c, x, here, :] = speed
                    out_u[0, c, x, here, :] = jnp.where(moving, place + time_step * speed, place)

    @pl.when(is_slab)
    def _():
        receive(corner_messages, corners)
        receive(modulus_messages, straight)
        receive(field_messages, straight)
        unpack_corners(4, 8, CR, B, 4)
        unpack_sides(range(4))
        modal = modal_stiffness()
        last_x = gx == size_x - 1
        last_y = gy == size_y - 1
        row_ids = lax.broadcasted_iota(jnp.int32, (8, depth), 0)
        for tile in range(3):
            rows = slice(8 * tile, 8 * tile + 8)
            next_rows = slice(8 * tile + 1, 8 * tile + 9)
            solid = lanes < depth - 1
            if tile == 2:
                solid = jnp.logical_and(
                    solid, jnp.logical_or(row_ids < 7, jnp.logical_not(last_y))
                )

            def nodes(x):
                result = []
                for c in range(3):
                    here, there = B[c, x, rows, :], B[c, x, next_rows, :]
                    for value in (here + there, there - here):
                        above = turn(value, 1)
                        result += [value + above, above - value]
                return result

            below = nodes(rim - 1)
            carried = None
            for element in range(rows_x + 1):
                above = nodes(rim + element)
                modes = {}
                for c in range(3):
                    for pair in range(4):
                        first, second = below[4 * c + pair], above[4 * c + pair]
                        if pair:
                            modes[8 * c + pair] = first + second
                        modes[8 * c + 4 + pair] = second - first
                below = above
                inside = solid
                if element == rows_x:
                    inside = jnp.logical_and(inside, jnp.logical_not(last_x))
                stiff = jnp.where(inside, B[3, rim - 1 + element, rows, :], 0.0)
                loads_of = {}
                for i in range(24):
                    total = None
                    for j in range(24):
                        if modal[i, j]:
                            term = float(modal[i, j]) * modes[j]
                            total = term if total is None else total + term
                    if total is not None:
                        loads_of[i] = total * stiff
                lows, highs = [], []
                for c in range(3):
                    for pair in range(4):
                        flat, steep = loads_of.get(8 * c + pair), loads_of[8 * c + 4 + pair]
                        lows.append(-steep if flat is None else flat - steep)
                        highs.append(steep if flat is None else flat + steep)
                if element:
                    for c in range(3):
                        halves = []
                        for pair in range(2):
                            flat = lows[4 * c + 2 * pair] + carried[4 * c + 2 * pair]
                            steep = lows[4 * c + 2 * pair + 1] + carried[4 * c + 2 * pair + 1]
                            halves.append((flat - steep) + turn(flat + steep, -1))
                        SL[c, element - 1, rows, :] = halves[0] - halves[1]
                        SH[c, element - 1, rows, :] = halves[0] + halves[1]
                carried = highs

        def inverse_mass(x, tile):
            spread = jnp.where(jnp.logical_or(lanes == 0, lanes == depth - 1), 2.0, 1.0)
            ends_y = jnp.logical_or(
                jnp.logical_and(gy == 0, row_ids + 8 * tile == 0),
                jnp.logical_and(last_y, row_ids + 8 * tile == rows_y - 1),
            )
            spread = spread * jnp.where(ends_y, 2.0, 1.0)
            if x == 0:
                spread = spread * jnp.where(gx == 0, 2.0, 1.0)
            if x == rows_x - 1:
                spread = spread * jnp.where(last_x, 2.0, 1.0)
            return spread

        for x in range(rows_x):
            for tile in range(2):
                here = slice(8 * tile, 8 * tile + 8)
                factor = time_step * inverse_mass(x, tile)
                for c in range(3):
                    force = (
                        SL[c, x, low + 8 * tile : low + 8 * tile + 8, :]
                        + SH[c, x, low + 8 * tile - 1 : low + 8 * tile + 7, :]
                    )
                    out_v[0, c, x, here, :] = V[c, x, here, :] - factor * force

        mapped = packed_map()
        link_down.wait_recv()
        reaction = RR[...]
        shared = jnp.zeros((rows_y, depth), jnp.float32)
        for by in range(-2, 3):
            source_layer = wide_layer + by
            fits = jnp.logical_and(source_layer >= 0, source_layer < 3)
            chosen = jnp.logical_and(fits, turn(mapped, by) == wide_layer)
            shared = shared + jnp.where(chosen, turn(reaction, by), 0.0)
        unclamped = lanes > 0
        for tile in range(2):
            here = slice(8 * tile, 8 * tile + 8)
            part = shared[here, :]
            for x in range(rows_x):
                factor = jnp.where(lanes >= depth - 3, time_step * inverse_mass(x, tile), 0.0)
                for c in range(3):
                    place = 3 * (rows_x * c + x)
                    moved = turn(part, place + 3 - depth)
                    speed = jnp.where(unclamped, out_v[0, c, x, here, :] + factor * moved, 0.0)
                    out_v[0, c, x, here, :] = speed
                    out_u[0, c, x, here, :] = jnp.where(
                        unclamped,
                        B[c, rim + x, low + 8 * tile : low + 8 * tile + 8, :] + time_step * speed,
                        0.0,
                    )

    def end_plan(zone):
        for messages, index, zone_only in plan:
            if zone_only and not zone:
                continue

            @pl.when(exists(*directions[index]))
            def _():
                for copy in copies(messages, index):
                    copy.wait_send()

    @pl.when(is_slab)
    def _():
        for index in range(8):

            @pl.when(exists(*directions[index]))
            def _():
                coupled_copy(index).wait_send()

        coupled_copy(8).wait_send()
        end_plan(False)

    @pl.when(is_zone)
    def _():
        end_plan(True)
        link_down.wait_send()


def store(first_in, second_in, first_out, second_out, sem):
    copies = [
        pltpu.make_async_copy(first_in, first_out, sem.at[0]),
        pltpu.make_async_copy(second_in, second_out, sem.at[1]),
    ]
    for copy in copies:
        copy.start()
    for copy in copies:
        copy.wait()


def per_device(displacement, velocity, modulus, bond_words, coupling_map):
    _, _, rows_x, rows_y, depth = displacement.shape
    f32, i32 = jnp.float32, jnp.int32
    wide_x, wide_y = rows_x + 2 * rim, rows_y + 16
    packed = rim * rows_x
    dma = pltpu.SemaphoreType.DMA
    field, speed = pl.pallas_call(
        kernel,
        out_shape=(
            pltpu.VMEM(displacement.shape, f32),
            pltpu.VMEM(velocity.shape, f32),
        ),
        in_specs=[pl.BlockSpec(memory_space=pltpu.HBM)] * 5,
        out_specs=(pl.BlockSpec(memory_space=pltpu.VMEM),) * 2,
        scratch_shapes=[
            pltpu.VMEM((4, wide_x, wide_y, depth), f32),
            pltpu.VMEM((2, rim + rows_x, wide_y, depth), i32),
            pltpu.VMEM((3, rows_x, rows_y, depth), f32),
            pltpu.VMEM(coupling_map.shape, i32),
            pltpu.VMEM((2, 4, packed, depth), f32),
            pltpu.VMEM((2, 2, packed, depth), i32),
            pltpu.VMEM((2, 4, packed, depth), f32),
            pltpu.VMEM((2, 2, packed, depth), i32),
            pltpu.VMEM((4, 2, 8, depth), f32),
            pltpu.VMEM((2, 8, depth), i32),
            pltpu.VMEM((4, 2, 8, depth), f32),
            pltpu.VMEM((2, 8, depth), i32),
            pltpu.VMEM((rows_y, depth), f32),
            pltpu.VMEM((rows_y, 1, depth), f32),
            pltpu.VMEM((2, 8, depth), f32),
            pltpu.VMEM((rows_y, depth), f32),
            pltpu.VMEM((2, 8, depth), f32),
            pltpu.VMEM((2, 3, rim, 1, depth), f32),
            pltpu.VMEM((rows_y, depth), f32),
            pltpu.VMEM((rows_y, depth), f32),
            pltpu.VMEM((5, 4, wide_x, wide_y, depth), f32),
            pltpu.VMEM((2, 2, rows_x, rows_y, depth), f32),
            pltpu.VMEM((4, 2, rim + rows_x, wide_y, depth), i32),
            pltpu.VMEM((rows_x, rows_y, depth), i32),
            pltpu.VMEM((len(bonds), rows_x, rows_y, depth), f32),
            pltpu.VMEM((3, rows_x, rows_y, depth), f32),
            pltpu.VMEM((3, rows_x, rows_y + 8, depth), f32),
            pltpu.VMEM((3, rows_x, rows_y + 8, depth), f32),
            dma((5,)), dma((6,)), dma((6,)), dma((4,)), dma((4,)), dma((6,)), dma((6,)),
            dma((6,)), dma((6,)), dma((9,)), dma((9,)), dma((1,)), dma((1,)),
        ],
        compiler_params=pltpu.CompilerParams(
            collective_id=0, has_side_effects=True, vmem_limit_bytes=24 * 1024 * 1024
        ),
    )(*[
        pltpu.with_memory_space_constraint(value, pltpu.HBM)
        for value in (displacement, velocity, modulus, bond_words, coupling_map)
    ])
    return pl.pallas_call(
        store,
        out_shape=(
            jax.ShapeDtypeStruct(displacement.shape, f32),
            jax.ShapeDtypeStruct(velocity.shape, f32),
        ),
        in_specs=[pl.BlockSpec(memory_space=pltpu.VMEM)] * 2,
        out_specs=(pl.BlockSpec(memory_space=pltpu.HBM),) * 2,
        scratch_shapes=[dma((2,))],
    )(*[pltpu.with_memory_space_constraint(value, pltpu.VMEM) for value in (field, speed)])


def solution(mesh):
    return jax.shard_map(
        per_device,
        mesh=mesh,
        in_specs=(
            P("group", None, "gx", "gy", None),
            P("group", None, "gx", "gy", None),
            P("group", "gx", "gy", None),
            P(None, "gx", "gy", None),
            P(None, "gx", "gy"),
        ),
        out_specs=(P("group", None, "gx", "gy", None), P("group", None, "gx", "gy", None)),
        check_vma=False,
    )
```

```python
import math

import jax
import jax.numpy as jnp
import numpy as np
from jax import lax
from jax.experimental import pallas as pl
from jax.experimental.pallas import tpu as pltpu
from jax.sharding import PartitionSpec as P

time_step = 0.1
bond_scale = 1.0
rim = 3
low = 8
MESH = pl.DeviceIdType.MESH
directions = [(1, 0), (-1, 0), (0, 1), (0, -1), (1, 1), (1, -1), (-1, 1), (-1, -1)]
shifts = [1, -1, 2, -2]


def half_offsets():
    table = []
    for delta_x in range(-3, 4):
        for delta_y in range(-3, 4):
            for delta_z in range(-3, 4):
                radius = delta_x * delta_x + delta_y * delta_y + delta_z * delta_z
                if 0 < radius <= 9 and (delta_x, delta_y, delta_z) > (0, 0, 0):
                    table.append((delta_x, delta_y, delta_z))
    return table


def hex_stiffness():
    poisson = 0.3
    lame_first = poisson / ((1.0 + poisson) * (1.0 - 2.0 * poisson))
    shear_modulus = 0.5 / (1.0 + poisson)
    elastic = np.zeros((6, 6))
    elastic[:3, :3] = lame_first
    for axis_id in range(3):
        elastic[axis_id, axis_id] += 2.0 * shear_modulus
        elastic[3 + axis_id, 3 + axis_id] = shear_modulus
    points = [0.5 - 0.5 / math.sqrt(3.0), 0.5 + 0.5 / math.sqrt(3.0)]
    result = np.zeros((24, 24))
    shear_pairs = ((0, 1), (1, 2), (0, 2))
    for along_x in points:
        for along_y in points:
            for along_z in points:
                coords = (along_x, along_y, along_z)
                gradients = np.zeros((3, 8))
                for corner in range(8):
                    corner_bits = (corner >> 2 & 1, corner >> 1 & 1, corner & 1)
                    factors = [
                        coords[axis_id] if corner_bits[axis_id] else 1.0 - coords[axis_id]
                        for axis_id in range(3)
                    ]
                    slopes = [1.0 if corner_bits[axis_id] else -1.0 for axis_id in range(3)]
                    gradients[0, corner] = slopes[0] * factors[1] * factors[2]
                    gradients[1, corner] = factors[0] * slopes[1] * factors[2]
                    gradients[2, corner] = factors[0] * factors[1] * slopes[2]
                strain = np.zeros((6, 24))
                for axis_id in range(3):
                    strain[axis_id, axis_id * 8 : axis_id * 8 + 8] = gradients[axis_id]
                for shear_row, pair in enumerate(shear_pairs):
                    left_axis, right_axis = pair
                    strain[3 + shear_row, left_axis * 8 : left_axis * 8 + 8] = gradients[right_axis]
                    strain[3 + shear_row, right_axis * 8 : right_axis * 8 + 8] = gradients[
                        left_axis
                    ]
                result += strain.T @ elastic @ strain / 8.0
    return result


def modal_stiffness():
    one = np.array([[1.0, -1.0], [1.0, 1.0]])
    corners = np.kron(np.kron(one, one), one)
    basis = np.kron(np.eye(3), corners)
    modal = basis.T @ hex_stiffness() @ basis / 64.0
    modal[np.abs(modal) < 1e-12] = 0.0
    return modal


offsets = half_offsets()
numbers = {offset: number for number, offset in enumerate(offsets)}
sheets_of_bonds = [
    [
        (delta_y, delta_z)
        for delta_y in chosen
        for delta_z in range(-3, 4)
        if delta_y * delta_y + delta_z * delta_z <= 9
    ]
    for chosen in ((0, 3, -3), (1,), (-1,), (2,), (-2,))
]
bonds = offsets + [tuple(-delta for delta in offset) for offset in offsets]


def scaled(coefficient, value):
    return value if coefficient == 1 else coefficient * value


def combine(terms):
    total = None
    negative = None
    for coefficient, value in terms:
        if coefficient == 0:
            continue
        if coefficient < 0 and total is None:
            negative = scaled(-coefficient, value) if negative is None else (
                negative + scaled(-coefficient, value)
            )
        elif total is None:
            total = scaled(coefficient, value)
            if negative is not None:
                total = total - negative
                negative = None
        elif coefficient > 0:
            total = total + scaled(coefficient, value)
        else:
            total = total - scaled(-coefficient, value)
    if negative is not None:
        total = 0.0 - negative
    return total


def turn(value, by):
    return pltpu.roll(value, (-by) % 128, value.ndim - 1)


def kernel(
    disp, vel, mod, words, cmap,
    out_u, out_v,
    B, W, V, CM,
    YS, YSW, YR, YRW, CS, CSW, CR, CRW,
    PS, PT, PE, PX, PN, PY, RS, RR,
    R, R3, WR, WR3, K, FS, SL, SH,
    load_sem, fs, fr, ms, mr, ws, wr, cs, cr, ps, pr, link_s, link_r,
):
    group = lax.axis_index("group")
    gx = lax.axis_index("gx")
    gy = lax.axis_index("gy")
    size_x = lax.axis_size("gx")
    size_y = lax.axis_size("gy")
    is_zone = group == 0
    is_slab = group == 1
    rows_x, rows_y, depth = V.shape[1], V.shape[2], V.shape[3]
    own_x = slice(rim, rim + rows_x)
    own_y = slice(low, low + rows_y)

    def at(step_x, step_y):
        return (group, gx + step_x, gy + step_y)

    def both(first, second):
        if first is None:
            return second
        return first if second is None else jnp.logical_and(first, second)

    def exists(step_x, step_y):
        test = None
        if step_x:
            test = gx + step_x < size_x if step_x > 0 else gx > 0
        if step_y:
            test = both(test, gy + step_y < size_y if step_y > 0 else gy > 0)
        return test

    barrier = pltpu.get_barrier_semaphore()
    pl.semaphore_signal(barrier, inc=1, device_id=(1 - group, gx, gy), device_id_type=MESH)
    expected = jnp.int32(1)
    for step_x, step_y in directions[::-1]:
        present = exists(step_x, step_y)
        expected = expected + jnp.where(is_slab, 2, 1) * present.astype(jnp.int32)

        @pl.when(present)
        def _():
            pl.semaphore_signal(
                barrier, inc=1, device_id=at(step_x, step_y), device_id_type=MESH
            )

            @pl.when(is_zone)
            def _():
                pl.semaphore_signal(
                    barrier,
                    inc=1,
                    device_id=(1 - group, gx + step_x, gy + step_y),
                    device_id_type=MESH,
                )

    loads = [
        pltpu.make_async_copy(disp.at[0], B.at[0:3, own_x, own_y, :], load_sem.at[0]),
        pltpu.make_async_copy(mod.at[0], B.at[3, own_x, own_y, :], load_sem.at[1]),
        pltpu.make_async_copy(words, W.at[:, own_x, own_y, :], load_sem.at[2]),
        pltpu.make_async_copy(cmap, CM, load_sem.at[3]),
        pltpu.make_async_copy(vel.at[0], V, load_sem.at[4]),
    ]
    for load in loads:
        load.start()

    def clear(ref):
        ref[...] = jnp.zeros(ref.shape, ref.dtype)

    @pl.when(gx == 0)
    def _():
        clear(B.at[:, 0:rim])
        clear(W.at[:, 0:rim])
        clear(PN.at[0])
        for side in range(2):
            clear(PY.at[side, 0])

    @pl.when(gx == size_x - 1)
    def _():
        clear(B.at[:, rim + rows_x :])
        clear(PN.at[1])
        for side in range(2):
            clear(PY.at[side, 2])

    for side, edge in ((0, gy == 0), (1, gy == size_y - 1)):

        @pl.when(edge)
        def _():
            clear(YR.at[side])
            clear(YRW.at[side])
            for index in range(3):
                clear(PY.at[side, index])

    for index, (step_x, step_y) in enumerate(directions[4:]):

        @pl.when(jnp.logical_not(exists(-step_x, -step_y)))
        def _():
            clear(CR.at[index])
            if step_x > 0:
                clear(CRW.at[index])

    for load in loads[:3]:
        load.wait()

    def rows_for(step_y):
        return slice(low + rows_y - rim, low + rows_y) if step_y > 0 else slice(low, low + rim)

    for step_y in (1, -1):
        side = 0 if step_y > 0 else 1
        for x in range(rows_x):
            for field in range(4):
                YS[side, field, rim * x : rim * x + rim, :] = B[
                    field, rim + x, rows_for(step_y), :
                ]

        @pl.when(is_zone)
        def _():
            for x in range(rows_x):
                for word in range(2):
                    YSW[side, word, rim * x : rim * x + rim, :] = W[
                        word, rim + x, rows_for(step_y), :
                    ]

    def corner_rows(step_y):
        if step_y > 0:
            return slice(low + rows_y - 2, low + rows_y)
        return slice(low, low + 2)

    def in_corner(field, count):
        first = 4 * (field % 2) + 2 * count
        return field // 2, slice(first, first + 2)

    for index, (step_x, step_y) in enumerate(directions[4:]):
        for count in range(2):
            x = rim + (rows_x - 2 + count if step_x > 0 else count)
            for field in range(4):
                tile, rows = in_corner(field, count)
                CS[index, tile, rows, :] = B[field, x, corner_rows(step_y), :]
        if step_x > 0:

            @pl.when(is_zone)
            def _():
                for count in range(2):
                    x = rim + rows_x - 2 + count
                    for word in range(2):
                        _, rows = in_corner(word, count)
                        CSW[index, rows, :] = W[word, x, corner_rows(step_y), :]

    lanes = lax.broadcasted_iota(jnp.int32, (8, depth), 1)
    wide_lanes = lax.broadcasted_iota(jnp.int32, (rows_y, depth), 1)
    wide_layer = lax.rem(wide_lanes, 3)
    loads[3].wait()

    def packed_map():
        source = lax.broadcasted_iota(jnp.int32, (3 * rows_x, depth), 0)
        target = lax.broadcasted_iota(jnp.int32, (3 * rows_x, depth), 1)
        chosen = jnp.logical_and(
            lax.div(source, rows_x) == lax.rem(target, 3),
            lax.rem(source, rows_x) == lax.rem(lax.div(target, 3), rows_x),
        )
        values = CM[...].reshape(3 * rows_x, rows_y).astype(jnp.float32)
        spread = lax.dot_general(
            values,
            chosen.astype(jnp.float32),
            (((0,), (0,)), ((), ())),
            preferred_element_type=jnp.float32,
        )
        return (spread + 0.5).astype(jnp.int32)

    @pl.when(is_slab)
    def _():
        for tile in range(2):
            rows = slice(low + 8 * tile, low + 8 * tile + 8)
            top = jnp.zeros((8, depth), jnp.float32)
            for c in range(3):
                for x in range(rows_x):
                    place = 3 * (rows_x * c + x)
                    moved = turn(B[c, rim + x, rows, :], depth - 3 - place)
                    top = jnp.where(
                        jnp.logical_and(lanes >= place, lanes < place + 3), moved, top
                    )
            RS[8 * tile : 8 * tile + 8, :] = top
        top = RS[...]
        away = packed_map() - wide_layer
        coupled = jnp.zeros((rows_y, depth), jnp.float32)
        for by in range(-2, 3):
            coupled = jnp.where(away == by, turn(top, by), coupled)
        PS[...] = coupled
        for row in range(rows_y):
            PT[row] = coupled[row : row + 1, :]
        for side, first in ((0, rows_x - rim), (1, 0)):
            kept = lax.rem(lanes, 3 * rows_x)
            kept = jnp.logical_and(kept >= 3 * first, kept < 3 * (first + rim))
            kept = jnp.logical_and(kept, lanes < 9 * rows_x)
            PE[side] = jnp.where(kept, coupled[0:8, :], pltpu.roll(coupled[8:16, :], 64, 1))

    tiles = [slice(8 * tile, 8 * tile + 8) for tile in range(4)]
    beside_x = (1, 2, rim + rows_x, rim + rows_x + 1)

    def turn_words(x, chosen, words_there=(0, 1)):
        for word in words_there:
            for rows in chosen:
                value = W[word, x, rows, :]
                for place, by in enumerate(shifts):
                    WR[place, word, x, rows, :] = turn(value, by)

    def turn_fields(x, chosen, fields):
        for field in fields:
            for rows in chosen:
                value = B[field, x, rows, :]
                for place, by in enumerate(shifts):
                    R[place, field, x, rows, :] = scaled(
                        by if field == 2 else 1, turn(value, by)
                    )

    def turn_own(x, carry):
        turn_words(rim + x, tiles[1:3])
        turn_fields(rim + x, tiles[1:3], range(4))
        for rows in tiles[1:3]:
            where = slice(rows.start - low, rows.stop - low)
            for spot, by in enumerate((3, -3)):
                R3[spot, 0, x, where, :] = turn(B[3, rim + x, rows, :], by)
                R3[spot, 1, x, where, :] = by * turn(B[2, rim + x, rows, :], by)
            WR3[x, where, :] = turn(W[0, rim + x, rows, :], -3)
        return carry


    group_of = 4
    blocks = sheets_of_bonds

    def factor_rows(start, tile, part):
        here = slice(8 * tile, 8 * tile + 8)

        def load_modulus(move_x, delta_y, delta_z):
            if abs(delta_z) == 3:
                return R3[0 if delta_z > 0 else 1, 0, start + move_x, here, :]
            rows = slice(low + 8 * tile + delta_y, low + 8 * tile + delta_y + 8)
            if delta_z == 0:
                return B[3, start + rim + move_x, rows, :]
            return R[shifts.index(delta_z), 3, start + rim + move_x, rows, :]

        def load_word(word, move_x, delta_y, delta_z):
            if delta_z == -3:
                return WR3[start + move_x, here, :]
            rows = slice(low + 8 * tile + delta_y, low + 8 * tile + delta_y + 8)
            if delta_z == 0:
                return W[word, start + rim + move_x, rows, :]
            return WR[shifts.index(delta_z), word, start + rim + move_x, rows, :]

        def block(lines):
            centre = [load_modulus(member, 0, 0) for member in range(group_of)]
            centre_words = [
                [load_word(word, member, 0, 0) for word in range(2)]
                for member in range(group_of)
            ]
            for delta_y, delta_z in lines:
                reach = math.isqrt(9 - delta_y * delta_y - delta_z * delta_z)
                for move_x in range(-reach, group_of + reach):
                    modulus_there, words_there = None, {}
                    for member in range(group_of):
                        delta = (move_x - member, delta_y, delta_z)
                        if abs(delta[0]) > reach or delta == (0, 0, 0):
                            continue
                        beyond_x = not 0 <= start + move_x < rows_x
                        beyond_y = delta_y < 0 if tile == 0 else delta_y > 0
                        if part != (2 if beyond_x else 1 if beyond_y else 0):
                            continue
                        radius = sum(value * value for value in delta)
                        weight = 0.5 * bond_scale / float(radius) ** 1.5
                        ahead = delta > (0, 0, 0)
                        number = numbers[delta if ahead else tuple(-value for value in delta)]
                        word = number // 31
                        if modulus_there is None:
                            modulus_there = load_modulus(move_x, delta_y, delta_z)
                        if ahead:
                            flags = centre_words[member][word]
                        else:
                            if word not in words_there:
                                words_there[word] = load_word(word, move_x, delta_y, delta_z)
                            flags = words_there[word]
                        intact = (flags & (1 << number % 31)) != 0
                        K[bonds.index(delta), start + member, here, :] = jnp.where(
                            intact, weight * (centre[member] + modulus_there), 0.0
                        )

        for lines in blocks:

            @pl.when(gx >= 0)
            def _():
                block(lines)

    def factors(part):
        for start in range(0, rows_x, group_of):
            for tile in range(2):
                factor_rows(start, tile, part)


    @pl.when(is_zone)
    def _():
        lax.fori_loop(0, rows_x, turn_own, 0)


    pl.semaphore_wait(barrier, expected)

    def message(source, target, sends, recvs, index, device):
        return pltpu.make_async_remote_copy(
            src_ref=source, dst_ref=target,
            send_sem=sends.at[index], recv_sem=recvs.at[index],
            device_id=device, device_id_type=MESH,
        )

    def along_gx(ref, step_x, first, count, lead):
        source = rows_x + first if step_x > 0 else rim + first
        target = first if step_x > 0 else rim + rows_x + first
        return (
            ref.at[lead, source : source + count, own_y, :],
            ref.at[lead, target : target + count, own_y, :],
        )

    def modulus_messages(index):
        step_x, step_y = directions[index]
        if step_y == 0:
            return [(along_gx(B, step_x, 0, rim, 3), ms, mr, index)]
        side = 0 if step_y > 0 else 1
        return [((YS.at[side, 3], YR.at[side, 3]), ms, mr, index)]

    def field_messages(index):
        step_x, step_y = directions[index]
        if step_y == 0:
            near, far = (1, 0) if step_x > 0 else (0, rim - 1)
            return [
                (along_gx(B, step_x, near, 2, slice(0, 3)), fs, fr, index),
                (along_gx(B, step_x, far, 1, 0), fs, fr, 4 + index),
            ]
        side = 0 if step_y > 0 else 1
        return [((YS.at[side, 0:3], YR.at[side, 0:3]), fs, fr, index)]

    def word_messages(index):
        step_x, step_y = directions[index]
        if step_y == 0:
            return [
                (along_gx(W, step_x, 2, 1, slice(0, 2)), ws, wr, index),
                (along_gx(W, step_x, 0, 2, 1), ws, wr, 4 + index),
            ]
        side = 0 if step_y > 0 else 1
        return [((YSW.at[side], YRW.at[side]), ws, wr, index)]

    def corner_messages(index):
        return [((CS.at[index - 4], CR.at[index - 4]), cs, cr, index - 4)]

    def corner_word_messages(index):
        return [((CSW.at[index - 4], CRW.at[index - 4]), cs, cr, index)]

    def copies(messages, index):
        return [
            message(source, target, sends, recvs, spot, at(*directions[index]))
            for (source, target), sends, recvs, spot in messages(index)
        ]

    def coupled_copy(index):
        step_x, step_y = directions[index] if index < 8 else (0, 0)
        if index == 8:
            source, target = PS, PX
        elif step_y == 0:
            side = 0 if step_x > 0 else 1
            source, target = PE.at[side], PN.at[side]
        elif step_y > 0:
            source, target = PT.at[rows_y - rim : rows_y], PY.at[0, 1 - step_x]
        else:
            source, target = PT.at[0:rim], PY.at[1, 1 - step_x]
        device = (1 - group, gx + step_x, gy + step_y)
        return message(source, target, ps, pr, index, device)

    link_down = message(RS, RR, link_s, link_r, 0, (1 - group, gx, gy))
    straight, corners = (0, 1, 2, 3), (4, 5, 6, 7)
    plan = [(corner_messages, index, False) for index in corners]
    plan += [(corner_word_messages, index, True) for index in (4, 5)]
    plan += [(modulus_messages, index, False) for index in (0, 1)]
    plan += [(word_messages, 0, True)]
    plan += [(modulus_messages, index, False) for index in (2, 3)]
    plan += [(word_messages, index, True) for index in (2, 3)]
    plan += [(field_messages, index, False) for index in straight]

    def start_plan(zone):
        for messages, index, zone_only in plan:
            if zone_only and not zone:
                continue

            @pl.when(exists(*directions[index]))
            def _():
                for copy in copies(messages, index):
                    copy.start()

    @pl.when(is_slab)
    def _():
        for index in (4, 5, 6, 7, 0, 1, 8, 2, 3):
            if index == 8:
                coupled_copy(8).start()
            else:

                @pl.when(exists(*directions[index]))
                def _():
                    coupled_copy(index).start()

        start_plan(False)

    @pl.when(is_zone)
    def _():
        start_plan(True)

    loads[4].wait()

    def arrived(index):
        step_x, step_y = directions[index]
        return exists(-step_x, -step_y)

    def receive(messages, indices):
        for index in indices:

            @pl.when(arrived(index))
            def _():
                for copy in copies(messages, index):
                    copy.wait_recv()

    def unpack_rows(side):
        return slice(low - rim, low) if side == 0 else slice(low + rows_y, low + rows_y + rim)

    def unpack_sides(fields):
        for side in range(2):
            for x in range(rows_x):
                for field in fields:
                    B[field, rim + x, unpack_rows(side), :] = YR[
                        side, field, rim * x : rim * x + rim, :
                    ]

    def unpack_corners(first, last, source, target, fields):
        for index in range(first, last):
            step_x, step_y = directions[index]
            where = slice(low - 2, low) if step_y > 0 else slice(low + rows_y, low + rows_y + 2)
            for count in range(2):
                x = 1 + count if step_x > 0 else rim + rows_x + count
                for field in range(fields):
                    tile, rows = in_corner(field, count)
                    part = source[index - 4, rows, :] if fields == 2 else source[
                        index - 4, tile, rows, :
                    ]
                    target[field, x, where, :] = part

    @pl.when(is_zone)
    def _():
        factors(0)

        receive(modulus_messages, (2, 3))
        receive(word_messages, (2, 3))
        unpack_sides((3,))
        for side in range(2):
            for x in range(rows_x):
                for word in range(2):
                    W[word, rim + x, unpack_rows(side), :] = YRW[
                        side, word, rim * x : rim * x + rim, :
                    ]

        def turn_beside(x, carry):
            turn_words(rim + x, (tiles[0], tiles[3]))
            turn_fields(rim + x, (tiles[0], tiles[3]), (3,))
            return carry

        lax.fori_loop(0, rows_x, turn_beside, 0)
        factors(1)

        receive(field_messages, (2, 3))
        unpack_sides(range(3))

        def turn_around(x, carry):
            turn_fields(rim + x, (tiles[0], tiles[3]), range(3))
            return carry

        lax.fori_loop(0, rows_x, turn_around, 0)

        def merge(x, chosen):
            beside = 0 if x < rim else 1 if x < rim + rows_x else 2
            inner = (x - rim) % rows_x
            for tile in chosen:
                rows = tiles[tile]
                extra = 0
                if tile in (0, 3):
                    first = 8 - rim if tile == 0 else 0
                    rows = slice(rows.start + first, rows.start + first + rim)
                    side = 0 if tile == 0 else 1
                    packed = PY[side, beside, :, 0, :]
                elif beside == 1:
                    packed = PX[8 * tile - 8 : 8 * tile, :]
                else:
                    packed = PN[0 if beside == 0 else 1]
                    extra = 64 * (tile - 1)
                outer = x in (0, 2 * rim + rows_x - 1)
                if outer and tile in (0, 3):
                    continue
                lane = lanes if tile in (1, 2) else lanes[0:rim]
                for c in range(1 if outer else 3):
                    place = 3 * (rows_x * c + inner) + extra

                    def moved(by):
                        return turn(packed, place + by)

                    R[4, c, x, rows, :] = jnp.where(lane < 3, moved(0), B[c, x, rows, :])
                    if outer:
                        continue
                    for spot, by in enumerate(shifts):
                        inside = lane < 3 - by
                        if by < 0:
                            inside = jnp.logical_and(inside, lane >= -by)
                        R[spot, c, x, rows, :] = jnp.where(
                            inside, scaled(by if c == 2 else 1, moved(by)), R[spot, c, x, rows, :]
                        )
                    if c == 2 and beside == 1 and tile in (1, 2):
                        where = slice(rows.start - low, rows.stop - low)
                        inside = jnp.logical_and(lane >= 3, lane < 6)
                        R3[1, 1, inner, where, :] = jnp.where(
                            inside, -3 * moved(-3), R3[1, 1, inner, where, :]
                        )


        def added(total, sign, value):
            if total is None:
                return value if sign > 0 else -value
            return total + value if sign > 0 else total - value

        def zone_rows(start, tile, part):
            here = slice(8 * tile, 8 * tile + 8)

            def load(field, move_x, delta_y, delta_z):
                if abs(delta_z) == 3:
                    return R3[0 if delta_z > 0 else 1, 1, start + move_x, here, :]
                first = low + 8 * tile + delta_y
                place = 4 if delta_z == 0 else shifts.index(delta_z)
                return R[place, field, start + rim + move_x, slice(first, first + 8), :]

            def block(lines):
                centre = [
                    [load(c, member, 0, 0) for c in range(3)] for member in range(group_of)
                ]
                along_x = [[None] * 4 for _ in range(group_of)]
                along_z = [[None] * 4 for _ in range(group_of)]
                sheets = [{} for _ in range(group_of)]
                for delta_y, delta_z in lines:
                    reach = math.isqrt(9 - delta_y * delta_y - delta_z * delta_z)
                    base = [
                        combine([(delta_y, centre[member][1]), (delta_z, centre[member][2])])
                        for member in range(group_of)
                    ]
                    line = [None] * group_of
                    for move_x in range(-reach, group_of + reach):
                        if part != (0 if 0 <= start + move_x < rows_x else 1):
                            continue
                        members = [
                            member
                            for member in range(group_of)
                            if abs(move_x - member) <= reach
                            and (move_x - member, delta_y, delta_z) != (0, 0, 0)
                        ]
                        if not members:
                            continue
                        if any(move_x != member for member in members):
                            away = load(0, move_x, delta_y, delta_z)
                        side = combine(
                            [
                                (delta_y, load(1, move_x, delta_y, delta_z) if delta_y else None),
                                (
                                    1 if delta_z else 0,
                                    load(2, move_x, delta_y, delta_z) if delta_z else None,
                                ),
                            ]
                        )
                        for member in members:
                            delta_x = move_x - member
                            stretch = None
                            if side is not None:
                                stretch = side - base[member]
                            if delta_x:
                                gap = away - centre[member][0]
                                if stretch is None:
                                    stretch = scaled(delta_x, gap)
                                elif abs(delta_x) == 1:
                                    stretch = added(stretch, delta_x, gap)
                                else:
                                    stretch = stretch + delta_x * gap
                            index = bonds.index((delta_x, delta_y, delta_z))
                            pull = K[index, start + member, here, :] * stretch
                            line[member] = added(line[member], 1, pull)
                            if delta_x:
                                along_x[member][abs(delta_x)] = added(
                                    along_x[member][abs(delta_x)], delta_x, pull
                                )
                    for member in range(group_of):
                        if line[member] is None:
                            continue
                        if delta_y:
                            sheets[member][delta_y] = added(
                                sheets[member].get(delta_y), 1, line[member]
                            )
                        if delta_z:
                            along_z[member][abs(delta_z)] = added(
                                along_z[member][abs(delta_z)], delta_z, line[member]
                            )
                for member in range(group_of):
                    sums = [
                        combine([(size, along_x[member][size]) for size in (1, 2, 3)
                                 if along_x[member][size] is not None]),
                        combine(list(sheets[member].items())),
                        combine([(size, along_z[member][size]) for size in (1, 2, 3)
                                 if along_z[member][size] is not None]),
                    ]
                    for c in range(3):
                        if sums[c] is not None:
                            FS[c, start + member, here, :] = FS[c, start + member, here, :] + sums[c]

            for lines in blocks:

                @pl.when(gx >= 0)
                def _():
                    block(lines)

        def forces(part):
            for start in range(0, rows_x, group_of):
                for tile in range(2):
                    zone_rows(start, tile, part)

        def receive_coupled(indices):
            for index in indices:

                @pl.when(arrived(index))
                def _():
                    coupled_copy(index).wait_recv()

        own = range(rim, rim + rows_x)
        FS[...] = jnp.zeros(FS.shape, FS.dtype)
        coupled_copy(8).wait_recv()
        for x in own:
            merge(x, (1, 2))
        receive_coupled((2, 3))
        for x in own:
            merge(x, (0, 3))
        forces(0)

        receive(corner_messages, corners)
        receive(corner_word_messages, (4, 5))
        unpack_corners(4, 8, CR, B, 4)
        unpack_corners(4, 6, CRW, W, 2)
        receive(modulus_messages, (0, 1))
        receive(word_messages, (0,))
        for x in beside_x:
            turn_fields(x, tiles, (3,))
            if x < rim:
                turn_words(x, tiles, (0, 1) if x == rim - 1 else (1,))
        factors(2)

        receive(field_messages, (0, 1))
        for x in beside_x:
            turn_fields(x, tiles, range(3))
        receive_coupled((0, 1, 4, 5, 6, 7))
        for x in range(2 * rim + rows_x):
            if x not in own:
                merge(x, range(4))
        forces(1)

        moving = lanes >= 3
        for tile in range(2):
            here = slice(8 * tile, 8 * tile + 8)
            packed = jnp.zeros((8, depth), jnp.float32)
            for x in range(rows_x):
                for c in range(3):
                    place = 3 * (rows_x * c + x)
                    moved = pltpu.roll(FS[c, x, here, :], place, 1)
                    packed = jnp.where(
                        jnp.logical_and(lanes >= place, lanes < place + 3), moved, packed
                    )
            RS[here, :] = packed
        link_down.start()
        for x in range(rows_x):
            for tile in range(2):
                here = slice(8 * tile, 8 * tile + 8)
                for c in range(3):
                    old = V[c, x, here, :]
                    place = R[4, c, rim + x, low + 8 * tile : low + 8 * tile + 8, :]
                    speed = jnp.where(moving, old + time_step * FS[c, x, here, :], old)
                    out_v[0, c, x, here, :] = speed
                    out_u[0, c, x, here, :] = jnp.where(moving, place + time_step * speed, place)

    @pl.when(is_slab)
    def _():
        receive(corner_messages, corners)
        receive(modulus_messages, straight)
        receive(field_messages, straight)
        unpack_corners(4, 8, CR, B, 4)
        unpack_sides(range(4))
        modal = modal_stiffness()
        last_x = gx == size_x - 1
        last_y = gy == size_y - 1
        row_ids = lax.broadcasted_iota(jnp.int32, (8, depth), 0)
        for tile in range(3):
            rows = slice(8 * tile, 8 * tile + 8)
            next_rows = slice(8 * tile + 1, 8 * tile + 9)
            solid = lanes < depth - 1
            if tile == 2:
                solid = jnp.logical_and(
                    solid, jnp.logical_or(row_ids < 7, jnp.logical_not(last_y))
                )

            def nodes(x):
                result = []
                for c in range(3):
                    here, there = B[c, x, rows, :], B[c, x, next_rows, :]
                    for value in (here + there, there - here):
                        above = turn(value, 1)
                        result += [value + above, above - value]
                return result

            below = nodes(rim - 1)
            carried = None
            for element in range(rows_x + 1):
                above = nodes(rim + element)
                modes = {}
                for c in range(3):
                    for pair in range(4):
                        first, second = below[4 * c + pair], above[4 * c + pair]
                        if pair:
                            modes[8 * c + pair] = first + second
                        modes[8 * c + 4 + pair] = second - first
                below = above
                inside = solid
                if element == rows_x:
                    inside = jnp.logical_and(inside, jnp.logical_not(last_x))
                stiff = jnp.where(inside, B[3, rim - 1 + element, rows, :], 0.0)
                loads_of = {}
                for i in range(24):
                    total = None
                    for j in range(24):
                        if modal[i, j]:
                            term = float(modal[i, j]) * modes[j]
                            total = term if total is None else total + term
                    if total is not None:
                        loads_of[i] = total * stiff
                lows, highs = [], []
                for c in range(3):
                    for pair in range(4):
                        flat, steep = loads_of.get(8 * c + pair), loads_of[8 * c + 4 + pair]
                        lows.append(-steep if flat is None else flat - steep)
                        highs.append(steep if flat is None else flat + steep)
                if element:
                    for c in range(3):
                        halves = []
                        for pair in range(2):
                            flat = lows[4 * c + 2 * pair] + carried[4 * c + 2 * pair]
                            steep = lows[4 * c + 2 * pair + 1] + carried[4 * c + 2 * pair + 1]
                            halves.append((flat - steep) + turn(flat + steep, -1))
                        SL[c, element - 1, rows, :] = halves[0] - halves[1]
                        SH[c, element - 1, rows, :] = halves[0] + halves[1]
                carried = highs

        def inverse_mass(x, tile):
            spread = jnp.where(jnp.logical_or(lanes == 0, lanes == depth - 1), 2.0, 1.0)
            ends_y = jnp.logical_or(
                jnp.logical_and(gy == 0, row_ids + 8 * tile == 0),
                jnp.logical_and(last_y, row_ids + 8 * tile == rows_y - 1),
            )
            spread = spread * jnp.where(ends_y, 2.0, 1.0)
            if x == 0:
                spread = spread * jnp.where(gx == 0, 2.0, 1.0)
            if x == rows_x - 1:
                spread = spread * jnp.where(last_x, 2.0, 1.0)
            return spread

        for x in range(rows_x):
            for tile in range(2):
                here = slice(8 * tile, 8 * tile + 8)
                factor = time_step * inverse_mass(x, tile)
                for c in range(3):
                    force = (
                        SL[c, x, low + 8 * tile : low + 8 * tile + 8, :]
                        + SH[c, x, low + 8 * tile - 1 : low + 8 * tile + 7, :]
                    )
                    out_v[0, c, x, here, :] = V[c, x, here, :] - factor * force

        mapped = packed_map()
        link_down.wait_recv()
        reaction = RR[...]
        shared = jnp.zeros((rows_y, depth), jnp.float32)
        for by in range(-2, 3):
            source_layer = wide_layer + by
            fits = jnp.logical_and(source_layer >= 0, source_layer < 3)
            chosen = jnp.logical_and(fits, turn(mapped, by) == wide_layer)
            shared = shared + jnp.where(chosen, turn(reaction, by), 0.0)
        unclamped = lanes > 0
        for tile in range(2):
            here = slice(8 * tile, 8 * tile + 8)
            part = shared[here, :]
            for x in range(rows_x):
                factor = jnp.where(lanes >= depth - 3, time_step * inverse_mass(x, tile), 0.0)
                for c in range(3):
                    place = 3 * (rows_x * c + x)
                    moved = turn(part, place + 3 - depth)
                    speed = jnp.where(unclamped, out_v[0, c, x, here, :] + factor * moved, 0.0)
                    out_v[0, c, x, here, :] = speed
                    out_u[0, c, x, here, :] = jnp.where(
                        unclamped,
                        B[c, rim + x, low + 8 * tile : low + 8 * tile + 8, :] + time_step * speed,
                        0.0,
                    )

    def end_plan(zone):
        for messages, index, zone_only in plan:
            if zone_only and not zone:
                continue

            @pl.when(exists(*directions[index]))
            def _():
                for copy in copies(messages, index):
                    copy.wait_send()

    @pl.when(is_slab)
    def _():
        for index in range(8):

            @pl.when(exists(*directions[index]))
            def _():
                coupled_copy(index).wait_send()

        coupled_copy(8).wait_send()
        end_plan(False)

    @pl.when(is_zone)
    def _():
        end_plan(True)
        link_down.wait_send()


def store(first_in, second_in, first_out, second_out, sem):
    copies = [
        pltpu.make_async_copy(first_in, first_out, sem.at[0]),
        pltpu.make_async_copy(second_in, second_out, sem.at[1]),
    ]
    for copy in copies:
        copy.start()
    for copy in copies:
        copy.wait()


def per_device(displacement, velocity, modulus, bond_words, coupling_map):
    _, _, rows_x, rows_y, depth = displacement.shape
    f32, i32 = jnp.float32, jnp.int32
    wide_x, wide_y = rows_x + 2 * rim, rows_y + 16
    packed = rim * rows_x
    dma = pltpu.SemaphoreType.DMA
    field, speed = pl.pallas_call(
        kernel,
        out_shape=(
            pltpu.VMEM(displacement.shape, f32),
            pltpu.VMEM(velocity.shape, f32),
        ),
        in_specs=[pl.BlockSpec(memory_space=pltpu.HBM)] * 5,
        out_specs=(pl.BlockSpec(memory_space=pltpu.VMEM),) * 2,
        scratch_shapes=[
            pltpu.VMEM((4, wide_x, wide_y, depth), f32),
            pltpu.VMEM((2, rim + rows_x, wide_y, depth), i32),
            pltpu.VMEM((3, rows_x, rows_y, depth), f32),
            pltpu.VMEM(coupling_map.shape, i32),
            pltpu.VMEM((2, 4, packed, depth), f32),
            pltpu.VMEM((2, 2, packed, depth), i32),
            pltpu.VMEM((2, 4, packed, depth), f32),
            pltpu.VMEM((2, 2, packed, depth), i32),
            pltpu.VMEM((4, 2, 8, depth), f32),
            pltpu.VMEM((2, 8, depth), i32),
            pltpu.VMEM((4, 2, 8, depth), f32),
            pltpu.VMEM((2, 8, depth), i32),
            pltpu.VMEM((rows_y, depth), f32),
            pltpu.VMEM((rows_y, 1, depth), f32),
            pltpu.VMEM((2, 8, depth), f32),
            pltpu.VMEM((rows_y, depth), f32),
            pltpu.VMEM((2, 8, depth), f32),
            pltpu.VMEM((2, 3, rim, 1, depth), f32),
            pltpu.VMEM((rows_y, depth), f32),
            pltpu.VMEM((rows_y, depth), f32),
            pltpu.VMEM((5, 4, wide_x, wide_y, depth), f32),
            pltpu.VMEM((2, 2, rows_x, rows_y, depth), f32),
            pltpu.VMEM((4, 2, rim + rows_x, wide_y, depth), i32),
            pltpu.VMEM((rows_x, rows_y, depth), i32),
            pltpu.VMEM((len(bonds), rows_x, rows_y, depth), f32),
            pltpu.VMEM((3, rows_x, rows_y, depth), f32),
            pltpu.VMEM((3, rows_x, rows_y + 8, depth), f32),
            pltpu.VMEM((3, rows_x, rows_y + 8, depth), f32),
            dma((5,)), dma((6,)), dma((6,)), dma((4,)), dma((4,)), dma((6,)), dma((6,)),
            dma((6,)), dma((6,)), dma((9,)), dma((9,)), dma((1,)), dma((1,)),
        ],
        compiler_params=pltpu.CompilerParams(
            collective_id=0, has_side_effects=True, vmem_limit_bytes=24 * 1024 * 1024
        ),
    )(*[
        pltpu.with_memory_space_constraint(value, pltpu.HBM)
        for value in (displacement, velocity, modulus, bond_words, coupling_map)
    ])
    return pl.pallas_call(
        store,
        out_shape=(
            jax.ShapeDtypeStruct(displacement.shape, f32),
            jax.ShapeDtypeStruct(velocity.shape, f32),
        ),
        in_specs=[pl.BlockSpec(memory_space=pltpu.VMEM)] * 2,
        out_specs=(pl.BlockSpec(memory_space=pltpu.HBM),) * 2,
        scratch_shapes=[dma((2,))],
    )(*[pltpu.with_memory_space_constraint(value, pltpu.VMEM) for value in (field, speed)])


def solution(mesh):
    return jax.shard_map(
        per_device,
        mesh=mesh,
        in_specs=(
            P("group", None, "gx", "gy", None),
            P("group", None, "gx", "gy", None),
            P("group", "gx", "gy", None),
            P(None, "gx", "gy", None),
            P(None, "gx", "gy"),
        ),
        out_specs=(P("group", None, "gx", "gy", None), P("group", None, "gx", "gy", None)),
        check_vma=False,
    )
```

```python
import math

import jax
import jax.numpy as jnp
import numpy as np
from jax import lax
from jax.experimental import pallas as pl
from jax.experimental.pallas import tpu as pltpu
from jax.sharding import PartitionSpec as P

time_step = 0.1
bond_scale = 1.0
rim = 3
low = 8
MESH = pl.DeviceIdType.MESH
directions = [(1, 0), (-1, 0), (0, 1), (0, -1), (1, 1), (1, -1), (-1, 1), (-1, -1)]
shifts = [1, -1, 2, -2]


def half_offsets():
    table = []
    for delta_x in range(-3, 4):
        for delta_y in range(-3, 4):
            for delta_z in range(-3, 4):
                radius = delta_x * delta_x + delta_y * delta_y + delta_z * delta_z
                if 0 < radius <= 9 and (delta_x, delta_y, delta_z) > (0, 0, 0):
                    table.append((delta_x, delta_y, delta_z))
    return table


def hex_stiffness():
    poisson = 0.3
    lame_first = poisson / ((1.0 + poisson) * (1.0 - 2.0 * poisson))
    shear_modulus = 0.5 / (1.0 + poisson)
    elastic = np.zeros((6, 6))
    elastic[:3, :3] = lame_first
    for axis_id in range(3):
        elastic[axis_id, axis_id] += 2.0 * shear_modulus
        elastic[3 + axis_id, 3 + axis_id] = shear_modulus
    points = [0.5 - 0.5 / math.sqrt(3.0), 0.5 + 0.5 / math.sqrt(3.0)]
    result = np.zeros((24, 24))
    shear_pairs = ((0, 1), (1, 2), (0, 2))
    for along_x in points:
        for along_y in points:
            for along_z in points:
                coords = (along_x, along_y, along_z)
                gradients = np.zeros((3, 8))
                for corner in range(8):
                    corner_bits = (corner >> 2 & 1, corner >> 1 & 1, corner & 1)
                    factors = [
                        coords[axis_id] if corner_bits[axis_id] else 1.0 - coords[axis_id]
                        for axis_id in range(3)
                    ]
                    slopes = [1.0 if corner_bits[axis_id] else -1.0 for axis_id in range(3)]
                    gradients[0, corner] = slopes[0] * factors[1] * factors[2]
                    gradients[1, corner] = factors[0] * slopes[1] * factors[2]
                    gradients[2, corner] = factors[0] * factors[1] * slopes[2]
                strain = np.zeros((6, 24))
                for axis_id in range(3):
                    strain[axis_id, axis_id * 8 : axis_id * 8 + 8] = gradients[axis_id]
                for shear_row, pair in enumerate(shear_pairs):
                    left_axis, right_axis = pair
                    strain[3 + shear_row, left_axis * 8 : left_axis * 8 + 8] = gradients[right_axis]
                    strain[3 + shear_row, right_axis * 8 : right_axis * 8 + 8] = gradients[
                        left_axis
                    ]
                result += strain.T @ elastic @ strain / 8.0
    return result


def modal_stiffness():
    one = np.array([[1.0, -1.0], [1.0, 1.0]])
    corners = np.kron(np.kron(one, one), one)
    basis = np.kron(np.eye(3), corners)
    modal = basis.T @ hex_stiffness() @ basis / 64.0
    modal[np.abs(modal) < 1e-12] = 0.0
    return modal


offsets = half_offsets()
numbers = {offset: number for number, offset in enumerate(offsets)}
sheets_of_bonds = [
    [
        (delta_y, delta_z)
        for delta_y in chosen
        for delta_z in range(-3, 4)
        if delta_y * delta_y + delta_z * delta_z <= 9
    ]
    for chosen in ((0, 3, -3), (1,), (-1,), (2,), (-2,))
]
bonds = offsets + [tuple(-delta for delta in offset) for offset in offsets]


def scaled(coefficient, value):
    return value if coefficient == 1 else coefficient * value


def combine(terms):
    total = None
    negative = None
    for coefficient, value in terms:
        if coefficient == 0:
            continue
        if coefficient < 0 and total is None:
            negative = scaled(-coefficient, value) if negative is None else (
                negative + scaled(-coefficient, value)
            )
        elif total is None:
            total = scaled(coefficient, value)
            if negative is not None:
                total = total - negative
                negative = None
        elif coefficient > 0:
            total = total + scaled(coefficient, value)
        else:
            total = total - scaled(-coefficient, value)
    if negative is not None:
        total = 0.0 - negative
    return total


def turn(value, by):
    return pltpu.roll(value, (-by) % 128, value.ndim - 1)


def kernel(
    disp, vel, mod, words, cmap,
    out_u, out_v,
    B, W, V, CM,
    YS, YSW, YR, YRW, CS, CSW, CR, CRW,
    PS, PT, PE, PX, PN, PY, RS, RR,
    R, R3, WR, WR3, K, FS, SL, SH,
    load_sem, fs, fr, ms, mr, ws, wr, cs, cr, ps, pr, link_s, link_r,
):
    group = lax.axis_index("group")
    gx = lax.axis_index("gx")
    gy = lax.axis_index("gy")
    size_x = lax.axis_size("gx")
    size_y = lax.axis_size("gy")
    is_zone = group == 0
    is_slab = group == 1
    rows_x, rows_y, depth = V.shape[1], V.shape[2], V.shape[3]
    own_x = slice(rim, rim + rows_x)
    own_y = slice(low, low + rows_y)

    def at(step_x, step_y):
        return (group, gx + step_x, gy + step_y)

    def both(first, second):
        if first is None:
            return second
        return first if second is None else jnp.logical_and(first, second)

    def exists(step_x, step_y):
        test = None
        if step_x:
            test = gx + step_x < size_x if step_x > 0 else gx > 0
        if step_y:
            test = both(test, gy + step_y < size_y if step_y > 0 else gy > 0)
        return test

    barrier = pltpu.get_barrier_semaphore()
    pl.semaphore_signal(barrier, inc=1, device_id=(1 - group, gx, gy), device_id_type=MESH)
    expected = jnp.int32(1)
    for step_x, step_y in directions[::-1]:
        present = exists(step_x, step_y)
        expected = expected + jnp.where(is_slab, 2, 1) * present.astype(jnp.int32)

        @pl.when(present)
        def _():
            pl.semaphore_signal(
                barrier, inc=1, device_id=at(step_x, step_y), device_id_type=MESH
            )

            @pl.when(is_zone)
            def _():
                pl.semaphore_signal(
                    barrier,
                    inc=1,
                    device_id=(1 - group, gx + step_x, gy + step_y),
                    device_id_type=MESH,
                )

    loads = [
        pltpu.make_async_copy(disp.at[0], B.at[0:3, own_x, own_y, :], load_sem.at[0]),
        pltpu.make_async_copy(mod.at[0], B.at[3, own_x, own_y, :], load_sem.at[1]),
        pltpu.make_async_copy(words, W.at[:, own_x, own_y, :], load_sem.at[2]),
        pltpu.make_async_copy(cmap, CM, load_sem.at[3]),
        pltpu.make_async_copy(vel.at[0], V, load_sem.at[4]),
    ]
    for load in loads:
        load.start()

    def clear(ref):
        ref[...] = jnp.zeros(ref.shape, ref.dtype)

    @pl.when(gx == 0)
    def _():
        clear(B.at[:, 0:rim])
        clear(W.at[:, 0:rim])
        clear(PN.at[0])
        for side in range(2):
            clear(PY.at[side, 0])

    @pl.when(gx == size_x - 1)
    def _():
        clear(B.at[:, rim + rows_x :])
        clear(PN.at[1])
        for side in range(2):
            clear(PY.at[side, 2])

    for side, edge in ((0, gy == 0), (1, gy == size_y - 1)):

        @pl.when(edge)
        def _():
            clear(YR.at[side])
            clear(YRW.at[side])
            for index in range(3):
                clear(PY.at[side, index])

    for index, (step_x, step_y) in enumerate(directions[4:]):

        @pl.when(jnp.logical_not(exists(-step_x, -step_y)))
        def _():
            clear(CR.at[index])
            if step_x > 0:
                clear(CRW.at[index])

    for load in loads[:3]:
        load.wait()

    def rows_for(step_y):
        return slice(low + rows_y - rim, low + rows_y) if step_y > 0 else slice(low, low + rim)

    for step_y in (1, -1):
        side = 0 if step_y > 0 else 1
        for x in range(rows_x):
            for field in range(4):
                YS[side, field, rim * x : rim * x + rim, :] = B[
                    field, rim + x, rows_for(step_y), :
                ]

        @pl.when(is_zone)
        def _():
            for x in range(rows_x):
                for word in range(2):
                    YSW[side, word, rim * x : rim * x + rim, :] = W[
                        word, rim + x, rows_for(step_y), :
                    ]

    def corner_rows(step_y):
        if step_y > 0:
            return slice(low + rows_y - 2, low + rows_y)
        return slice(low, low + 2)

    def in_corner(field, count):
        first = 4 * (field % 2) + 2 * count
        return field // 2, slice(first, first + 2)

    for index, (step_x, step_y) in enumerate(directions[4:]):
        for count in range(2):
            x = rim + (rows_x - 2 + count if step_x > 0 else count)
            for field in range(4):
                tile, rows = in_corner(field, count)
                CS[index, tile, rows, :] = B[field, x, corner_rows(step_y), :]
        if step_x > 0:

            @pl.when(is_zone)
            def _():
                for count in range(2):
                    x = rim + rows_x - 2 + count
                    for word in range(2):
                        _, rows = in_corner(word, count)
                        CSW[index, rows, :] = W[word, x, corner_rows(step_y), :]

    lanes = lax.broadcasted_iota(jnp.int32, (8, depth), 1)
    wide_lanes = lax.broadcasted_iota(jnp.int32, (rows_y, depth), 1)
    wide_layer = lax.rem(wide_lanes, 3)
    loads[3].wait()

    def packed_map():
        source = lax.broadcasted_iota(jnp.int32, (3 * rows_x, depth), 0)
        target = lax.broadcasted_iota(jnp.int32, (3 * rows_x, depth), 1)
        chosen = jnp.logical_and(
            lax.div(source, rows_x) == lax.rem(target, 3),
            lax.rem(source, rows_x) == lax.rem(lax.div(target, 3), rows_x),
        )
        values = CM[...].reshape(3 * rows_x, rows_y).astype(jnp.float32)
        spread = lax.dot_general(
            values,
            chosen.astype(jnp.float32),
            (((0,), (0,)), ((), ())),
            preferred_element_type=jnp.float32,
        )
        return (spread + 0.5).astype(jnp.int32)

    @pl.when(is_slab)
    def _():
        for tile in range(2):
            rows = slice(low + 8 * tile, low + 8 * tile + 8)
            top = jnp.zeros((8, depth), jnp.float32)
            for c in range(3):
                for x in range(rows_x):
                    place = 3 * (rows_x * c + x)
                    moved = turn(B[c, rim + x, rows, :], depth - 3 - place)
                    top = jnp.where(
                        jnp.logical_and(lanes >= place, lanes < place + 3), moved, top
                    )
            RS[8 * tile : 8 * tile + 8, :] = top
        top = RS[...]
        away = packed_map() - wide_layer
        coupled = jnp.zeros((rows_y, depth), jnp.float32)
        for by in range(-2, 3):
            coupled = jnp.where(away == by, turn(top, by), coupled)
        PS[...] = coupled
        for row in range(rows_y):
            PT[row] = coupled[row : row + 1, :]
        for side, first in ((0, rows_x - rim), (1, 0)):
            kept = lax.rem(lanes, 3 * rows_x)
            kept = jnp.logical_and(kept >= 3 * first, kept < 3 * (first + rim))
            kept = jnp.logical_and(kept, lanes < 9 * rows_x)
            PE[side] = jnp.where(kept, coupled[0:8, :], pltpu.roll(coupled[8:16, :], 64, 1))

    tiles = [slice(8 * tile, 8 * tile + 8) for tile in range(4)]
    beside_x = (1, 2, rim + rows_x, rim + rows_x + 1)

    def turn_words(x, chosen, words_there=(0, 1)):
        for word in words_there:
            for rows in chosen:
                value = W[word, x, rows, :]
                for place, by in enumerate(shifts):
                    WR[place, word, x, rows, :] = turn(value, by)

    def turn_fields(x, chosen, fields):
        for field in fields:
            for rows in chosen:
                value = B[field, x, rows, :]
                for place, by in enumerate(shifts):
                    R[place, field, x, rows, :] = scaled(
                        by if field == 2 else 1, turn(value, by)
                    )

    def turn_own(x, carry):
        turn_words(rim + x, tiles[1:3])
        turn_fields(rim + x, tiles[1:3], range(4))
        for rows in tiles[1:3]:
            where = slice(rows.start - low, rows.stop - low)
            for spot, by in enumerate((3, -3)):
                R3[spot, 0, x, where, :] = turn(B[3, rim + x, rows, :], by)
                R3[spot, 1, x, where, :] = by * turn(B[2, rim + x, rows, :], by)
            WR3[x, where, :] = turn(W[0, rim + x, rows, :], -3)
        return carry


    group_of = 4
    blocks = sheets_of_bonds

    def factor_rows(start, tile, part):
        here = slice(8 * tile, 8 * tile + 8)

        def load_modulus(move_x, delta_y, delta_z):
            if abs(delta_z) == 3:
                return R3[0 if delta_z > 0 else 1, 0, start + move_x, here, :]
            rows = slice(low + 8 * tile + delta_y, low + 8 * tile + delta_y + 8)
            if delta_z == 0:
                return B[3, start + rim + move_x, rows, :]
            return R[shifts.index(delta_z), 3, start + rim + move_x, rows, :]

        def load_word(word, move_x, delta_y, delta_z):
            if delta_z == -3:
                return WR3[start + move_x, here, :]
            rows = slice(low + 8 * tile + delta_y, low + 8 * tile + delta_y + 8)
            if delta_z == 0:
                return W[word, start + rim + move_x, rows, :]
            return WR[shifts.index(delta_z), word, start + rim + move_x, rows, :]

        def block(lines):
            centre = [load_modulus(member, 0, 0) for member in range(group_of)]
            centre_words = [
                [load_word(word, member, 0, 0) for word in range(2)]
                for member in range(group_of)
            ]
            for delta_y, delta_z in lines:
                reach = math.isqrt(9 - delta_y * delta_y - delta_z * delta_z)
                for move_x in range(-reach, group_of + reach):
                    modulus_there, words_there = None, {}
                    for member in range(group_of):
                        delta = (move_x - member, delta_y, delta_z)
                        if abs(delta[0]) > reach or delta == (0, 0, 0):
                            continue
                        beyond_x = not 0 <= start + move_x < rows_x
                        beyond_y = delta_y < 0 if tile == 0 else delta_y > 0
                        if part != (2 if beyond_x else 1 if beyond_y else 0):
                            continue
                        radius = sum(value * value for value in delta)
                        weight = 0.5 * bond_scale / float(radius) ** 1.5
                        ahead = delta > (0, 0, 0)
                        number = numbers[delta if ahead else tuple(-value for value in delta)]
                        word = number // 31
                        if modulus_there is None:
                            modulus_there = load_modulus(move_x, delta_y, delta_z)
                        if ahead:
                            flags = centre_words[member][word]
                        else:
                            if word not in words_there:
                                words_there[word] = load_word(word, move_x, delta_y, delta_z)
                            flags = words_there[word]
                        intact = (flags & (1 << number % 31)) != 0
                        K[bonds.index(delta), start + member, here, :] = jnp.where(
                            intact, weight * (centre[member] + modulus_there), 0.0
                        )

        for lines in blocks:

            @pl.when(gx >= 0)
            def _():
                block(lines)

    def factors(part):
        for start in range(0, rows_x, group_of):
            for tile in range(2):
                factor_rows(start, tile, part)


    @pl.when(is_zone)
    def _():
        lax.fori_loop(0, rows_x, turn_own, 0)


    pl.semaphore_wait(barrier, expected)

    def message(source, target, sends, recvs, index, device):
        return pltpu.make_async_remote_copy(
            src_ref=source, dst_ref=target,
            send_sem=sends.at[index], recv_sem=recvs.at[index],
            device_id=device, device_id_type=MESH,
        )

    def along_gx(ref, step_x, first, count, lead):
        source = rows_x + first if step_x > 0 else rim + first
        target = first if step_x > 0 else rim + rows_x + first
        return (
            ref.at[lead, source : source + count, own_y, :],
            ref.at[lead, target : target + count, own_y, :],
        )

    def modulus_messages(index):
        step_x, step_y = directions[index]
        if step_y == 0:
            return [(along_gx(B, step_x, 0, rim, 3), ms, mr, index)]
        side = 0 if step_y > 0 else 1
        return [((YS.at[side, 3], YR.at[side, 3]), ms, mr, index)]

    def field_messages(index):
        step_x, step_y = directions[index]
        if step_y == 0:
            near, far = (1, 0) if step_x > 0 else (0, rim - 1)
            return [
                (along_gx(B, step_x, near, 2, slice(0, 3)), fs, fr, index),
                (along_gx(B, step_x, far, 1, 0), fs, fr, 4 + index),
            ]
        side = 0 if step_y > 0 else 1
        return [((YS.at[side, 0:3], YR.at[side, 0:3]), fs, fr, index)]

    def word_messages(index):
        step_x, step_y = directions[index]
        if step_y == 0:
            return [
                (along_gx(W, step_x, 2, 1, slice(0, 2)), ws, wr, index),
                (along_gx(W, step_x, 0, 2, 1), ws, wr, 4 + index),
            ]
        side = 0 if step_y > 0 else 1
        return [((YSW.at[side], YRW.at[side]), ws, wr, index)]

    def corner_messages(index):
        return [((CS.at[index - 4], CR.at[index - 4]), cs, cr, index - 4)]

    def corner_word_messages(index):
        return [((CSW.at[index - 4], CRW.at[index - 4]), cs, cr, index)]

    def copies(messages, index):
        return [
            message(source, target, sends, recvs, spot, at(*directions[index]))
            for (source, target), sends, recvs, spot in messages(index)
        ]

    def coupled_copy(index):
        step_x, step_y = directions[index] if index < 8 else (0, 0)
        if index == 8:
            source, target = PS, PX
        elif step_y == 0:
            side = 0 if step_x > 0 else 1
            source, target = PE.at[side], PN.at[side]
        elif step_y > 0:
            source, target = PT.at[rows_y - rim : rows_y], PY.at[0, 1 - step_x]
        else:
            source, target = PT.at[0:rim], PY.at[1, 1 - step_x]
        device = (1 - group, gx + step_x, gy + step_y)
        return message(source, target, ps, pr, index, device)

    link_down = message(RS, RR, link_s, link_r, 0, (1 - group, gx, gy))
    straight, corners = (0, 1, 2, 3), (4, 5, 6, 7)
    plan = [(modulus_messages, index, False) for index in (2, 3)]
    plan += [(word_messages, index, True) for index in (2, 3)]
    plan += [(field_messages, index, False) for index in (2, 3)]
    plan += [(corner_messages, index, False) for index in corners]
    plan += [(corner_word_messages, index, True) for index in (4, 5)]
    plan += [(modulus_messages, index, False) for index in (0, 1)]
    plan += [(word_messages, 0, True)]
    plan += [(field_messages, index, False) for index in (0, 1)]

    def start_plan(zone):
        for messages, index, zone_only in plan:
            if zone_only and not zone:
                continue

            @pl.when(exists(*directions[index]))
            def _():
                for copy in copies(messages, index):
                    copy.start()

    @pl.when(is_slab)
    def _():
        for index in (8, 2, 3, 4, 5, 6, 7, 0, 1):
            if index == 8:
                coupled_copy(8).start()
            else:

                @pl.when(exists(*directions[index]))
                def _():
                    coupled_copy(index).start()

        start_plan(False)

    @pl.when(is_zone)
    def _():
        start_plan(True)

    loads[4].wait()

    def arrived(index):
        step_x, step_y = directions[index]
        return exists(-step_x, -step_y)

    def receive(messages, indices):
        for index in indices:

            @pl.when(arrived(index))
            def _():
                for copy in copies(messages, index):
                    copy.wait_recv()

    def unpack_rows(side):
        return slice(low - rim, low) if side == 0 else slice(low + rows_y, low + rows_y + rim)

    def unpack_sides(fields):
        for side in range(2):
            for x in range(rows_x):
                for field in fields:
                    B[field, rim + x, unpack_rows(side), :] = YR[
                        side, field, rim * x : rim * x + rim, :
                    ]

    def unpack_corners(first, last, source, target, fields):
        for index in range(first, last):
            step_x, step_y = directions[index]
            where = slice(low - 2, low) if step_y > 0 else slice(low + rows_y, low + rows_y + 2)
            for count in range(2):
                x = 1 + count if step_x > 0 else rim + rows_x + count
                for field in range(fields):
                    tile, rows = in_corner(field, count)
                    part = source[index - 4, rows, :] if fields == 2 else source[
                        index - 4, tile, rows, :
                    ]
                    target[field, x, where, :] = part

    @pl.when(is_zone)
    def _():
        factors(0)

        receive(modulus_messages, (2, 3))
        receive(word_messages, (2, 3))
        unpack_sides((3,))
        for side in range(2):
            for x in range(rows_x):
                for word in range(2):
                    W[word, rim + x, unpack_rows(side), :] = YRW[
                        side, word, rim * x : rim * x + rim, :
                    ]

        def turn_beside(x, carry):
            turn_words(rim + x, (tiles[0], tiles[3]))
            turn_fields(rim + x, (tiles[0], tiles[3]), (3,))
            return carry

        lax.fori_loop(0, rows_x, turn_beside, 0)
        factors(1)

        receive(field_messages, (2, 3))
        unpack_sides(range(3))

        def turn_around(x, carry):
            turn_fields(rim + x, (tiles[0], tiles[3]), range(3))
            return carry

        lax.fori_loop(0, rows_x, turn_around, 0)

        def merge(x, chosen):
            beside = 0 if x < rim else 1 if x < rim + rows_x else 2
            inner = (x - rim) % rows_x
            for tile in chosen:
                rows = tiles[tile]
                extra = 0
                if tile in (0, 3):
                    first = 8 - rim if tile == 0 else 0
                    rows = slice(rows.start + first, rows.start + first + rim)
                    side = 0 if tile == 0 else 1
                    packed = PY[side, beside, :, 0, :]
                elif beside == 1:
                    packed = PX[8 * tile - 8 : 8 * tile, :]
                else:
                    packed = PN[0 if beside == 0 else 1]
                    extra = 64 * (tile - 1)
                outer = x in (0, 2 * rim + rows_x - 1)
                if outer and tile in (0, 3):
                    continue
                lane = lanes if tile in (1, 2) else lanes[0:rim]
                for c in range(1 if outer else 3):
                    place = 3 * (rows_x * c + inner) + extra

                    def moved(by):
                        return turn(packed, place + by)

                    R[4, c, x, rows, :] = jnp.where(lane < 3, moved(0), B[c, x, rows, :])
                    if outer:
                        continue
                    for spot, by in enumerate(shifts):
                        inside = lane < 3 - by
                        if by < 0:
                            inside = jnp.logical_and(inside, lane >= -by)
                        R[spot, c, x, rows, :] = jnp.where(
                            inside, scaled(by if c == 2 else 1, moved(by)), R[spot, c, x, rows, :]
                        )
                    if c == 2 and beside == 1 and tile in (1, 2):
                        where = slice(rows.start - low, rows.stop - low)
                        inside = jnp.logical_and(lane >= 3, lane < 6)
                        R3[1, 1, inner, where, :] = jnp.where(
                            inside, -3 * moved(-3), R3[1, 1, inner, where, :]
                        )


        def added(total, sign, value):
            if total is None:
                return value if sign > 0 else -value
            return total + value if sign > 0 else total - value

        def zone_rows(start, tile, part):
            here = slice(8 * tile, 8 * tile + 8)

            def load(field, move_x, delta_y, delta_z):
                if abs(delta_z) == 3:
                    return R3[0 if delta_z > 0 else 1, 1, start + move_x, here, :]
                first = low + 8 * tile + delta_y
                place = 4 if delta_z == 0 else shifts.index(delta_z)
                return R[place, field, start + rim + move_x, slice(first, first + 8), :]

            def block(lines):
                centre = [
                    [load(c, member, 0, 0) for c in range(3)] for member in range(group_of)
                ]
                along_x = [[None] * 4 for _ in range(group_of)]
                along_z = [[None] * 4 for _ in range(group_of)]
                sheets = [{} for _ in range(group_of)]
                for delta_y, delta_z in lines:
                    reach = math.isqrt(9 - delta_y * delta_y - delta_z * delta_z)
                    base = [
                        combine([(delta_y, centre[member][1]), (delta_z, centre[member][2])])
                        for member in range(group_of)
                    ]
                    line = [None] * group_of
                    for move_x in range(-reach, group_of + reach):
                        if part != (0 if 0 <= start + move_x < rows_x else 1):
                            continue
                        members = [
                            member
                            for member in range(group_of)
                            if abs(move_x - member) <= reach
                            and (move_x - member, delta_y, delta_z) != (0, 0, 0)
                        ]
                        if not members:
                            continue
                        if any(move_x != member for member in members):
                            away = load(0, move_x, delta_y, delta_z)
                        side = combine(
                            [
                                (delta_y, load(1, move_x, delta_y, delta_z) if delta_y else None),
                                (
                                    1 if delta_z else 0,
                                    load(2, move_x, delta_y, delta_z) if delta_z else None,
                                ),
                            ]
                        )
                        for member in members:
                            delta_x = move_x - member
                            stretch = None
                            if side is not None:
                                stretch = side - base[member]
                            if delta_x:
                                gap = away - centre[member][0]
                                if stretch is None:
                                    stretch = scaled(delta_x, gap)
                                elif abs(delta_x) == 1:
                                    stretch = added(stretch, delta_x, gap)
                                else:
                                    stretch = stretch + delta_x * gap
                            index = bonds.index((delta_x, delta_y, delta_z))
                            pull = K[index, start + member, here, :] * stretch
                            line[member] = added(line[member], 1, pull)
                            if delta_x:
                                along_x[member][abs(delta_x)] = added(
                                    along_x[member][abs(delta_x)], delta_x, pull
                                )
                    for member in range(group_of):
                        if line[member] is None:
                            continue
                        if delta_y:
                            sheets[member][delta_y] = added(
                                sheets[member].get(delta_y), 1, line[member]
                            )
                        if delta_z:
                            along_z[member][abs(delta_z)] = added(
                                along_z[member][abs(delta_z)], delta_z, line[member]
                            )
                for member in range(group_of):
                    sums = [
                        combine([(size, along_x[member][size]) for size in (1, 2, 3)
                                 if along_x[member][size] is not None]),
                        combine(list(sheets[member].items())),
                        combine([(size, along_z[member][size]) for size in (1, 2, 3)
                                 if along_z[member][size] is not None]),
                    ]
                    for c in range(3):
                        if sums[c] is not None:
                            FS[c, start + member, here, :] = FS[c, start + member, here, :] + sums[c]

            for lines in blocks:

                @pl.when(gx >= 0)
                def _():
                    block(lines)

        def forces(part):
            for start in range(0, rows_x, group_of):
                for tile in range(2):
                    zone_rows(start, tile, part)

        def receive_coupled(indices):
            for index in indices:

                @pl.when(arrived(index))
                def _():
                    coupled_copy(index).wait_recv()

        own = range(rim, rim + rows_x)
        FS[...] = jnp.zeros(FS.shape, FS.dtype)
        coupled_copy(8).wait_recv()
        for x in own:
            merge(x, (1, 2))
        receive_coupled((2, 3))
        for x in own:
            merge(x, (0, 3))
        forces(0)

        receive(corner_messages, corners)
        receive(corner_word_messages, (4, 5))
        unpack_corners(4, 8, CR, B, 4)
        unpack_corners(4, 6, CRW, W, 2)
        receive(modulus_messages, (0, 1))
        receive(word_messages, (0,))
        for x in beside_x:
            turn_fields(x, tiles, (3,))
            if x < rim:
                turn_words(x, tiles, (0, 1) if x == rim - 1 else (1,))
        factors(2)

        receive(field_messages, (0, 1))
        for x in beside_x:
            turn_fields(x, tiles, range(3))
        receive_coupled((0, 1, 4, 5, 6, 7))
        for x in range(2 * rim + rows_x):
            if x not in own:
                merge(x, range(4))
        forces(1)

        moving = lanes >= 3
        for tile in range(2):
            here = slice(8 * tile, 8 * tile + 8)
            packed = jnp.zeros((8, depth), jnp.float32)
            for x in range(rows_x):
                for c in range(3):
                    place = 3 * (rows_x * c + x)
                    moved = pltpu.roll(FS[c, x, here, :], place, 1)
                    packed = jnp.where(
                        jnp.logical_and(lanes >= place, lanes < place + 3), moved, packed
                    )
            RS[here, :] = packed
        link_down.start()
        for x in range(rows_x):
            for tile in range(2):
                here = slice(8 * tile, 8 * tile + 8)
                for c in range(3):
                    old = V[c, x, here, :]
                    place = R[4, c, rim + x, low + 8 * tile : low + 8 * tile + 8, :]
                    speed = jnp.where(moving, old + time_step * FS[c, x, here, :], old)
                    out_v[0, c, x, here, :] = speed
                    out_u[0, c, x, here, :] = jnp.where(moving, place + time_step * speed, place)

    @pl.when(is_slab)
    def _():
        receive(corner_messages, corners)
        receive(modulus_messages, straight)
        receive(field_messages, straight)
        unpack_corners(4, 8, CR, B, 4)
        unpack_sides(range(4))
        modal = modal_stiffness()
        last_x = gx == size_x - 1
        last_y = gy == size_y - 1
        row_ids = lax.broadcasted_iota(jnp.int32, (8, depth), 0)
        for tile in range(3):
            rows = slice(8 * tile, 8 * tile + 8)
            next_rows = slice(8 * tile + 1, 8 * tile + 9)
            solid = lanes < depth - 1
            if tile == 2:
                solid = jnp.logical_and(
                    solid, jnp.logical_or(row_ids < 7, jnp.logical_not(last_y))
                )

            def nodes(x):
                result = []
                for c in range(3):
                    here, there = B[c, x, rows, :], B[c, x, next_rows, :]
                    for value in (here + there, there - here):
                        above = turn(value, 1)
                        result += [value + above, above - value]
                return result

            below = nodes(rim - 1)
            carried = None
            for element in range(rows_x + 1):
                above = nodes(rim + element)
                modes = {}
                for c in range(3):
                    for pair in range(4):
                        first, second = below[4 * c + pair], above[4 * c + pair]
                        if pair:
                            modes[8 * c + pair] = first + second
                        modes[8 * c + 4 + pair] = second - first
                below = above
                inside = solid
                if element == rows_x:
                    inside = jnp.logical_and(inside, jnp.logical_not(last_x))
                stiff = jnp.where(inside, B[3, rim - 1 + element, rows, :], 0.0)
                loads_of = {}
                for i in range(24):
                    total = None
                    for j in range(24):
                        if modal[i, j]:
                            term = float(modal[i, j]) * modes[j]
                            total = term if total is None else total + term
                    if total is not None:
                        loads_of[i] = total * stiff
                lows, highs = [], []
                for c in range(3):
                    for pair in range(4):
                        flat, steep = loads_of.get(8 * c + pair), loads_of[8 * c + 4 + pair]
                        lows.append(-steep if flat is None else flat - steep)
                        highs.append(steep if flat is None else flat + steep)
                if element:
                    for c in range(3):
                        halves = []
                        for pair in range(2):
                            flat = lows[4 * c + 2 * pair] + carried[4 * c + 2 * pair]
                            steep = lows[4 * c + 2 * pair + 1] + carried[4 * c + 2 * pair + 1]
                            halves.append((flat - steep) + turn(flat + steep, -1))
                        SL[c, element - 1, rows, :] = halves[0] - halves[1]
                        SH[c, element - 1, rows, :] = halves[0] + halves[1]
                carried = highs

        def inverse_mass(x, tile):
            spread = jnp.where(jnp.logical_or(lanes == 0, lanes == depth - 1), 2.0, 1.0)
            ends_y = jnp.logical_or(
                jnp.logical_and(gy == 0, row_ids + 8 * tile == 0),
                jnp.logical_and(last_y, row_ids + 8 * tile == rows_y - 1),
            )
            spread = spread * jnp.where(ends_y, 2.0, 1.0)
            if x == 0:
                spread = spread * jnp.where(gx == 0, 2.0, 1.0)
            if x == rows_x - 1:
                spread = spread * jnp.where(last_x, 2.0, 1.0)
            return spread

        for x in range(rows_x):
            for tile in range(2):
                here = slice(8 * tile, 8 * tile + 8)
                factor = time_step * inverse_mass(x, tile)
                for c in range(3):
                    force = (
                        SL[c, x, low + 8 * tile : low + 8 * tile + 8, :]
                        + SH[c, x, low + 8 * tile - 1 : low + 8 * tile + 7, :]
                    )
                    out_v[0, c, x, here, :] = V[c, x, here, :] - factor * force

        mapped = packed_map()
        link_down.wait_recv()
        reaction = RR[...]
        shared = jnp.zeros((rows_y, depth), jnp.float32)
        for by in range(-2, 3):
            source_layer = wide_layer + by
            fits = jnp.logical_and(source_layer >= 0, source_layer < 3)
            chosen = jnp.logical_and(fits, turn(mapped, by) == wide_layer)
            shared = shared + jnp.where(chosen, turn(reaction, by), 0.0)
        unclamped = lanes > 0
        for tile in range(2):
            here = slice(8 * tile, 8 * tile + 8)
            part = shared[here, :]
            for x in range(rows_x):
                factor = jnp.where(lanes >= depth - 3, time_step * inverse_mass(x, tile), 0.0)
                for c in range(3):
                    place = 3 * (rows_x * c + x)
                    moved = turn(part, place + 3 - depth)
                    speed = jnp.where(unclamped, out_v[0, c, x, here, :] + factor * moved, 0.0)
                    out_v[0, c, x, here, :] = speed
                    out_u[0, c, x, here, :] = jnp.where(
                        unclamped,
                        B[c, rim + x, low + 8 * tile : low + 8 * tile + 8, :] + time_step * speed,
                        0.0,
                    )

    def end_plan(zone):
        for messages, index, zone_only in plan:
            if zone_only and not zone:
                continue

            @pl.when(exists(*directions[index]))
            def _():
                for copy in copies(messages, index):
                    copy.wait_send()

    @pl.when(is_slab)
    def _():
        for index in range(8):

            @pl.when(exists(*directions[index]))
            def _():
                coupled_copy(index).wait_send()

        coupled_copy(8).wait_send()
        end_plan(False)

    @pl.when(is_zone)
    def _():
        end_plan(True)
        link_down.wait_send()


def store(first_in, second_in, first_out, second_out, sem):
    copies = [
        pltpu.make_async_copy(first_in, first_out, sem.at[0]),
        pltpu.make_async_copy(second_in, second_out, sem.at[1]),
    ]
    for copy in copies:
        copy.start()
    for copy in copies:
        copy.wait()


def per_device(displacement, velocity, modulus, bond_words, coupling_map):
    _, _, rows_x, rows_y, depth = displacement.shape
    f32, i32 = jnp.float32, jnp.int32
    wide_x, wide_y = rows_x + 2 * rim, rows_y + 16
    packed = rim * rows_x
    dma = pltpu.SemaphoreType.DMA
    field, speed = pl.pallas_call(
        kernel,
        out_shape=(
            pltpu.VMEM(displacement.shape, f32),
            pltpu.VMEM(velocity.shape, f32),
        ),
        in_specs=[pl.BlockSpec(memory_space=pltpu.HBM)] * 5,
        out_specs=(pl.BlockSpec(memory_space=pltpu.VMEM),) * 2,
        scratch_shapes=[
            pltpu.VMEM((4, wide_x, wide_y, depth), f32),
            pltpu.VMEM((2, rim + rows_x, wide_y, depth), i32),
            pltpu.VMEM((3, rows_x, rows_y, depth), f32),
            pltpu.VMEM(coupling_map.shape, i32),
            pltpu.VMEM((2, 4, packed, depth), f32),
            pltpu.VMEM((2, 2, packed, depth), i32),
            pltpu.VMEM((2, 4, packed, depth), f32),
            pltpu.VMEM((2, 2, packed, depth), i32),
            pltpu.VMEM((4, 2, 8, depth), f32),
            pltpu.VMEM((2, 8, depth), i32),
            pltpu.VMEM((4, 2, 8, depth), f32),
            pltpu.VMEM((2, 8, depth), i32),
            pltpu.VMEM((rows_y, depth), f32),
            pltpu.VMEM((rows_y, 1, depth), f32),
            pltpu.VMEM((2, 8, depth), f32),
            pltpu.VMEM((rows_y, depth), f32),
            pltpu.VMEM((2, 8, depth), f32),
            pltpu.VMEM((2, 3, rim, 1, depth), f32),
            pltpu.VMEM((rows_y, depth), f32),
            pltpu.VMEM((rows_y, depth), f32),
            pltpu.VMEM((5, 4, wide_x, wide_y, depth), f32),
            pltpu.VMEM((2, 2, rows_x, rows_y, depth), f32),
            pltpu.VMEM((4, 2, rim + rows_x, wide_y, depth), i32),
            pltpu.VMEM((rows_x, rows_y, depth), i32),
            pltpu.VMEM((len(bonds), rows_x, rows_y, depth), f32),
            pltpu.VMEM((3, rows_x, rows_y, depth), f32),
            pltpu.VMEM((3, rows_x, rows_y + 8, depth), f32),
            pltpu.VMEM((3, rows_x, rows_y + 8, depth), f32),
            dma((5,)), dma((6,)), dma((6,)), dma((4,)), dma((4,)), dma((6,)), dma((6,)),
            dma((6,)), dma((6,)), dma((9,)), dma((9,)), dma((1,)), dma((1,)),
        ],
        compiler_params=pltpu.CompilerParams(
            collective_id=0, has_side_effects=True, vmem_limit_bytes=24 * 1024 * 1024
        ),
    )(*[
        pltpu.with_memory_space_constraint(value, pltpu.HBM)
        for value in (displacement, velocity, modulus, bond_words, coupling_map)
    ])
    return pl.pallas_call(
        store,
        out_shape=(
            jax.ShapeDtypeStruct(displacement.shape, f32),
            jax.ShapeDtypeStruct(velocity.shape, f32),
        ),
        in_specs=[pl.BlockSpec(memory_space=pltpu.VMEM)] * 2,
        out_specs=(pl.BlockSpec(memory_space=pltpu.HBM),) * 2,
        scratch_shapes=[dma((2,))],
    )(*[pltpu.with_memory_space_constraint(value, pltpu.VMEM) for value in (field, speed)])


def solution(mesh):
    return jax.shard_map(
        per_device,
        mesh=mesh,
        in_specs=(
            P("group", None, "gx", "gy", None),
            P("group", None, "gx", "gy", None),
            P("group", "gx", "gy", None),
            P(None, "gx", "gy", None),
            P(None, "gx", "gy"),
        ),
        out_specs=(P("group", None, "gx", "gy", None), P("group", None, "gx", "gy", None)),
        check_vma=False,
    )
```
